32 devices in a mesh: term: 4 (over y, x), sector: 8 (over z, core).
Axes of the slice: x: 2, y: 2, z: 4, core: 2. Of those that a mesh axis runs over, the one named last changes fastest.
Arguments:
- wavefunction: float32 [8, 512, 512], P('sector'), may hold values from -120 to 120
- precond: float32 [8, 512, 512], P('sector', 'term'), may hold values from 0.05 to 4
- left_ops: float32 [8, 16, 512, 512], P('sector', 'term'), may hold values from -0.5 to 4.5
- right_ops: float32 [8, 16, 512, 512], P('sector', 'term'), may hold values from -1 to 2
- out_sector: int32 [8, 16], P('sector', 'term'), may hold values from 0 to 7, as said below
- live_counts: int32 [8, 4], P('sector', 'term'), may hold values from 1 to 4, as said below
Outputs:
- first_image: float32 [8, 512, 512], P('sector', 'term')
- correction: float32 [8, 512, 512], P('sector', 'term')
- second_image: float32 [8, 512, 512], P('sector', 'term')
The draws below stay inside these ranges and needn't reach their ends.
Inputs may be any that keep to these rules, and one draw needn't show every extreme that they name: Each term moves the charge by at most one sector: out_sector[s, j] differs from s by at most 1. `live_counts`: in every sector some device has all 4 slots live.
All inputs are finite; a program needn't handle non-finite values.
Results may differ from the reference program's by a relative error of at most 0.0003.
Values sent between devices are 32-bit elements; how exact they have to be, the bound alone decides.
A program may use at most 64 MiB of HBM per device.

```python
import jax
import jax.numpy as jnp
from jax import lax

B = 512
CAP = 4
NSEC = 8
N_TERM = 4


def draw_wavefunction(key, part):
    key_values, key_rows, key_columns = jax.random.split(jax.random.fold_in(key, 11), 3)
    row_index = jnp.arange(B, dtype=jnp.float32)
    jitter = jax.random.uniform(key_rows, (B,), jnp.float32)
    row_scale = 10.0 ** ((row_index + jitter) / B)
    column_scale = 10.0 ** jax.random.uniform(key_columns, (B,), jnp.float32)
    sector_scale = 3.0 ** (jnp.arange(NSEC, dtype=jnp.float32) / max(NSEC - 1, 1))
    values = jax.random.truncated_normal(key_values, -4.0, 4.0, (NSEC, B, B), jnp.float32)
    return 0.1 * values * sector_scale[:, None, None] * row_scale[None, :, None] * column_scale[None, None, :]


def draw_out_sector(key, part):
    change = jax.random.randint(jax.random.fold_in(key, 23), (NSEC, N_TERM * CAP), -1, 2)
    sector_ids = jnp.arange(NSEC, dtype=jnp.int32)[:, None]
    target = sector_ids + change
    target = jnp.where(target < 0, sector_ids + 1, target)
    target = jnp.where(target > NSEC - 1, sector_ids - 1, target)
    return target.astype(jnp.int32)


def draw_live_counts(key, part):
    key_busy, key_pick = jax.random.split(jax.random.fold_in(key, 37), 2)
    busy = jax.random.randint(key_busy, (NSEC, N_TERM), 0, 10) < 3
    counts = jnp.where(busy, CAP, 1)
    chosen = jax.random.randint(key_pick, (NSEC,), 0, N_TERM)
    columns = jnp.arange(N_TERM, dtype=jnp.int32)[None, :]
    counts = jnp.where(columns == chosen[:, None], CAP, counts)
    return counts.astype(jnp.int32)


def sector_strengths(key):
    key_order, key_jitter = jax.random.split(jax.random.fold_in(key, 53), 2)
    order = jax.random.permutation(key_order, NSEC).astype(jnp.float32)
    jitter = jax.random.uniform(key_jitter, (NSEC,), jnp.float32)
    return 4.0 ** ((order + jitter) / NSEC)


def diagonal_weights(key, part):
    targets = draw_out_sector(key, part)
    counts = draw_live_counts(key, part)
    slot_ids = jnp.arange(N_TERM * CAP, dtype=jnp.int32) % CAP
    alive = slot_ids[None, :] < jnp.repeat(counts, CAP, axis=1)
    sector_ids = jnp.arange(NSEC, dtype=jnp.int32)[:, None]
    on_diagonal = jnp.logical_and(alive, targets == sector_ids)
    how_many = jnp.sum(on_diagonal.astype(jnp.float32), axis=1)
    strength = sector_strengths(key)
    effective = jnp.where(how_many > 0.5, strength, 0.0)
    per_slot = jnp.where(on_diagonal, (strength / jnp.maximum(how_many, 1.0))[:, None], 0.0)
    return (per_slot.astype(jnp.float32), effective.astype(jnp.float32))


def draw_left_ops(key, part):
    per_slot, effective = diagonal_weights(key, part)
    noise = jax.random.truncated_normal(jax.random.fold_in(key, 61), -4.0, 4.0, (NSEC, N_TERM * CAP, B, B), jnp.float32)
    noise = noise / jnp.sqrt(jnp.float32(B * N_TERM * CAP))
    identity = jnp.eye(B, dtype=jnp.float32)
    return noise + per_slot[:, :, None, None] * identity[None, None, :, :]


def draw_right_ops(key, part):
    noise = jax.random.truncated_normal(jax.random.fold_in(key, 67), -4.0, 4.0, (NSEC, N_TERM * CAP, B, B), jnp.float32)
    noise = noise / jnp.sqrt(jnp.float32(B))
    identity = jnp.eye(B, dtype=jnp.float32)
    return noise + identity[None, None, :, :]


def draw_precond(key, part):
    per_slot, effective = diagonal_weights(key, part)
    spread = jax.random.uniform(jax.random.fold_in(key, 71), (NSEC, B, B), jnp.float32, 0.0, 1.0)
    entries = 0.25 * 8.0 ** spread
    return entries / (effective + 0.5)[:, None, None]


def setup_inputs(seed: int = 0) -> dict:
    arg_keys = jax.random.split(jax.random.key(seed), 7)
    return {
        "wavefunction": draw_wavefunction(jax.random.fold_in(arg_keys[6], 71), 0),
        "precond": draw_precond(jax.random.fold_in(arg_keys[6], 71), 0),
        "left_ops": draw_left_ops(jax.random.fold_in(arg_keys[6], 71), 0),
        "right_ops": draw_right_ops(jax.random.fold_in(arg_keys[6], 71), 0),
        "out_sector": draw_out_sector(jax.random.fold_in(arg_keys[6], 71), 0),
        "live_counts": draw_live_counts(jax.random.fold_in(arg_keys[6], 71), 0),
    }


def matmul(first_op, second_op):
    return jnp.dot(first_op, second_op, precision=lax.Precision.HIGHEST, preferred_element_type=jnp.float32)


def apply_hamiltonian(field, left_ops, right_ops, out_sector, alive):
    def sector_step(totals, inputs):
        center, left_stack, right_stack, destinations, flags = inputs

        def slot_step(running, slot_data):
            left_one, right_one, destination, alive_flag = slot_data
            product = matmul(matmul(left_one, center), right_one)
            return running.at[destination].add(product * alive_flag), None

        totals, _ = lax.scan(slot_step, totals, (left_stack, right_stack, destinations, flags))
        return totals, None

    totals, _ = lax.scan(sector_step, jnp.zeros_like(field), (field, left_ops, right_ops, out_sector, alive))
    return totals


def reference(wavefunction, precond, left_ops, right_ops, out_sector, live_counts):
    slot_ids = jnp.arange(N_TERM * CAP, dtype=jnp.int32) % CAP
    alive = (slot_ids[None, :] < jnp.repeat(live_counts, CAP, axis=1)).astype(jnp.float32)
    first_image = apply_hamiltonian(wavefunction, left_ops, right_ops, out_sector, alive)
    norm_sq = jnp.sum(wavefunction * wavefunction)
    rayleigh = jnp.sum(wavefunction * first_image) / norm_sq
    raw = precond * (first_image - rayleigh * wavefunction)
    correction = raw - (jnp.sum(wavefunction * raw) / norm_sq) * wavefunction
    second_image = apply_hamiltonian(correction, left_ops, right_ops, out_sector, alive)
    return first_image, correction, second_image
```

```python
import functools
import math

import jax
import jax.numpy as jnp
from jax import lax
from jax.experimental import pallas as pl
from jax.experimental.pallas import tpu as pltpu
from jax.sharding import PartitionSpec as P

F32, BF16 = jnp.float32, jnp.bfloat16
MESH = pl.DeviceIdType.MESH
VMEM = pl.BlockSpec(memory_space=pltpu.VMEM)
SMEM = pl.BlockSpec(memory_space=pltpu.SMEM)
ANY = pl.BlockSpec(memory_space=pl.ANY)
SLICES = 4


def split(x):
    high = x.astype(BF16)
    return high, (x - high.astype(F32)).astype(BF16)


def product(a_high, a_low, b_high, b_low):
    dot = functools.partial(jnp.dot, preferred_element_type=F32)
    return dot(a_high, b_high) + dot(a_high, b_low) + dot(a_low, b_high)


def send(source, target, send_sem, recv_sem, **where):
    return pltpu.make_async_remote_copy(
        src_ref=source, dst_ref=target, send_sem=send_sem, recv_sem=recv_sem,
        device_id=where, device_id_type=MESH,
    )


def grid_of(terms):
    columns = max(d for d in range(1, math.isqrt(terms) + 1) if terms % d == 0)
    return terms // columns, columns


class Place:
    def __init__(self):
        self.terms, self.sectors = lax.axis_size("term"), lax.axis_size("sector")
        self.t, self.s = lax.axis_index("term"), lax.axis_index("sector")
        self.gy, self.gx = grid_of(self.terms)
        self.y, self.x = self.t // self.gx, lax.rem(self.t, self.gx)

    def at(self, dy, dx):
        return lax.rem(self.y + dy, self.gy) * self.gx + lax.rem(self.x + dx, self.gx)

    def order(self):
        both = [(dy, dx) for dy in range(1, self.gy) for dx in range(1, self.gx)]
        return both + [(dy, 0) for dy in range(1, self.gy)] + [(0, dx) for dx in range(1, self.gx)] + [(0, 0)]


def barrier(here):
    sem = pltpu.get_barrier_semaphore()
    for k in range(1, here.terms):
        pl.semaphore_signal(sem, inc=1, device_id={"term": lax.rem(here.t + k, here.terms)}, device_id_type=MESH)
    for k in range(1, here.sectors):
        pl.semaphore_signal(sem, inc=1, device_id={"sector": lax.rem(here.s + k, here.sectors)}, device_id_type=MESH)
    return lambda: pl.semaphore_wait(sem, here.terms + here.sectors - 2)


class Exchange:
    def __init__(self, here, refs):
        self.here = here
        (self.whole, self.up_in, self.down_in, self.acc, self.da_in, self.db_in, self.x_in, self.y_in,
         self.up_s, self.up_r, self.down_s, self.down_r, self.da_s, self.da_r, self.db_s, self.db_r,
         self.x_s, self.x_r, self.y_s, self.y_r) = refs
        self.rows, self.width = self.acc.shape[1], self.acc.shape[2]
        self.sub, self.half = self.rows // SLICES, self.width // 2

    @staticmethod
    def scratch(width, terms):
        rows, half = width // terms, width // 2
        gy, gx = grid_of(terms)
        dma = pltpu.SemaphoreType.DMA
        whole = pltpu.VMEM((terms, rows, width), F32)
        return [
            pltpu.VMEM((3, terms, rows, width), F32), whole, whole, whole,
            pltpu.VMEM((gy, gx, rows, half), F32), pltpu.VMEM((gy, gx, rows, half), F32),
            pltpu.VMEM((gx, rows, width), F32), pltpu.VMEM((gy, rows, width), F32),
        ] + [dma((SLICES, terms))] * 4 + [dma((SLICES, gy, gx))] * 4 + [dma((SLICES, gx))] * 2 + [dma((SLICES, gy))] * 2

    def part(self, i):
        return pl.ds(pl.multiple_of(i * self.sub, self.sub), self.sub)

    def upward(self, r, i):
        h = self.here
        return send(self.whole.at[2, r, self.part(i)], self.up_in.at[r, self.part(i)], self.up_s.at[i, r],
                    self.up_r.at[i, r], sector=lax.rem(h.s + 1, h.sectors))

    def downward(self, r, i):
        h = self.here
        return send(self.whole.at[0, r, self.part(i)], self.down_in.at[r, self.part(i)], self.down_s.at[i, r],
                    self.down_r.at[i, r], sector=lax.rem(h.s + h.sectors - 1, h.sectors))

    def corner_a(self, dy, dx, i):
        h, part = self.here, self.part(i)
        return send(self.acc.at[h.at(dy, dx), part, : self.half], self.da_in.at[dy, dx, part],
                    self.da_s.at[i, dy, dx], self.da_r.at[i, dy, dx], term=h.at(0, dx))

    def corner_b(self, dy, dx, i):
        h, part = self.here, self.part(i)
        return send(self.acc.at[h.at(dy, dx), part, self.half :], self.db_in.at[dy, dx, part],
                    self.db_s.at[i, dy, dx], self.db_r.at[i, dy, dx], term=h.at(dy, 0))

    def along_x(self, dx, i):
        h, part = self.here, self.part(i)
        return send(self.acc.at[h.at(0, dx), part], self.x_in.at[dx, part], self.x_s.at[i, dx], self.x_r.at[i, dx],
                    term=h.at(0, dx))

    def along_y(self, dy, i):
        h, part = self.here, self.part(i)
        return send(self.acc.at[h.at(dy, 0), part], self.y_in.at[dy, part], self.y_s.at[i, dy], self.y_r.at[i, dy],
                    term=h.at(dy, 0))

    def sectors_out(self, i):
        h = self.here
        for dy, dx in h.order():
            r = h.at(dy, dx)

            @pl.when(h.s + 1 < h.sectors)
            def _():
                self.upward(r, i).start()

            @pl.when(h.s > 0)
            def _():
                self.downward(r, i).start()

    def merge(self, r, i):
        h, part = self.here, self.part(i)
        self.acc[r, part] = self.whole[1, r, part]

        @pl.when(h.s > 0)
        def _():
            self.upward(r, i).wait_recv()
            self.acc[r, part] += self.up_in[r, part]

        @pl.when(h.s + 1 < h.sectors)
        def _():
            self.downward(r, i).wait_recv()
            self.acc[r, part] += self.down_in[r, part]

    def corners(self, i):
        h = self.here
        for dy in range(1, h.gy):
            for dx in range(1, h.gx):
                self.merge(h.at(dy, dx), i)
                self.corner_a(dy, dx, i).start()
                self.corner_b(dy, dx, i).start()

    def sides(self, i):
        h, part = self.here, self.part(i)
        for dy in range(1, h.gy):
            r = h.at(dy, 0)
            self.merge(r, i)
            for dx in range(1, h.gx):
                self.corner_a(dy, dx, i).wait_recv()
                self.acc[r, part, : self.half] += self.da_in[dy, dx, part]
            self.along_y(dy, i).start()
        for dx in range(1, h.gx):
            r = h.at(0, dx)
            self.merge(r, i)
            for dy in range(1, h.gy):
                self.corner_b(dy, dx, i).wait_recv()
                self.acc[r, part, self.half :] += self.db_in[dy, dx, part]
            self.along_x(dx, i).start()

    def own(self, i):
        h, part = self.here, self.part(i)
        self.merge(h.t, i)
        total = self.acc[h.t, part]
        for dy in range(1, h.gy):
            self.along_y(dy, i).wait_recv()
            total += self.y_in[dy, part]
        for dx in range(1, h.gx):
            self.along_x(dx, i).wait_recv()
            total += self.x_in[dx, part]
        return total

    def drain(self):
        h = self.here

        @pl.loop(0, SLICES)
        def _(i):
            for dy, dx in h.order():
                r = h.at(dy, dx)

                @pl.when(h.s + 1 < h.sectors)
                def _():
                    self.upward(r, i).wait_send()

                @pl.when(h.s > 0)
                def _():
                    self.downward(r, i).wait_send()

                if dy and dx:
                    self.corner_a(dy, dx, i).wait_send()
                    self.corner_b(dy, dx, i).wait_send()
                elif dy:
                    self.along_y(dy, i).wait_send()
                elif dx:
                    self.along_x(dx, i).wait_send()


class Gather:
    def __init__(self, here, full, refs, pieces):
        self.here, self.full = here, full
        self.x_s, self.x_r, self.y_s, self.y_r, self.a_s, self.a_r, self.b_s, self.b_r = refs
        self.sub, self.half = full.shape[1] // pieces, full.shape[2] // 2
        self.pieces = pieces

    @staticmethod
    def scratch(terms, pieces):
        gy, gx = grid_of(terms)
        dma = pltpu.SemaphoreType.DMA
        return [dma((pieces, gx))] * 2 + [dma((pieces, gy))] * 2 + [dma((pieces, gy, gx))] * 4

    def part(self, i):
        return pl.ds(pl.multiple_of(i * self.sub, self.sub), self.sub)

    def to_x(self, r, dx, i):
        ref = self.full.at[r, self.part(i)]
        return send(ref, ref, self.x_s.at[i, dx], self.x_r.at[i, dx], term=self.here.at(0, dx))

    def to_y(self, r, dy, i):
        ref = self.full.at[r, self.part(i)]
        return send(ref, ref, self.y_s.at[i, dy], self.y_r.at[i, dy], term=self.here.at(dy, 0))

    def relay_a(self, r, dy, dx, i):
        ref = self.full.at[r, self.part(i), : self.half]
        return send(ref, ref, self.a_s.at[i, dy, dx], self.a_r.at[i, dy, dx], term=self.here.at(0, dx))

    def relay_b(self, r, dy, dx, i):
        ref = self.full.at[r, self.part(i), self.half :]
        return send(ref, ref, self.b_s.at[i, dy, dx], self.b_r.at[i, dy, dx], term=self.here.at(dy, 0))

    def begin(self, i):
        h = self.here
        for dx in range(1, h.gx):
            self.to_x(h.t, dx, i).start()
        for dy in range(1, h.gy):
            self.to_y(h.t, dy, i).start()

    def relay(self, i):
        h = self.here
        for dx in range(1, h.gx):
            r = h.at(0, dx)
            self.to_x(r, h.gx - dx, i).wait_recv()
            for dy in range(1, h.gy):
                self.relay_b(r, dy, dx, i).start()
        for dy in range(1, h.gy):
            r = h.at(dy, 0)
            self.to_y(r, h.gy - dy, i).wait_recv()
            for dx in range(1, h.gx):
                self.relay_a(r, dy, dx, i).start()

    def finish(self, i):
        h = self.here
        for dy in range(1, h.gy):
            for dx in range(1, h.gx):
                self.relay_a(h.at(dy, h.gx - dx), dy, dx, i).wait_recv()
                self.relay_b(h.at(h.gy - dy, dx), dy, dx, i).wait_recv()

    def drain(self):
        h = self.here

        @pl.loop(0, self.pieces)
        def _(i):
            for dx in range(1, h.gx):
                self.to_x(h.t, dx, i).wait_send()
            for dy in range(1, h.gy):
                self.to_y(h.t, dy, i).wait_send()
            for dy in range(1, h.gy):
                for dx in range(1, h.gx):
                    self.relay_a(h.at(dy, 0), dy, dx, i).wait_send()
                    self.relay_b(h.at(0, dx), dy, dx, i).wait_send()


EXCHANGE_REFS, GATHER_REFS = 20, 8


def kernel(target, count, wave_hbm, precond_hbm, left_hbm, right_hbm, first_out, correction_out, second_out, *scratch):
    scratch = list(scratch)

    def take(n):
        refs = scratch[:n]
        del scratch[:n]
        return refs

    here = Place()
    first, second = Exchange(here, take(EXCHANGE_REFS)), Exchange(here, take(EXCHANGE_REFS))
    wave, precond, image, left, right, r_high, r_low, v_high, v_low = take(9)
    p_gather, f_gather = Gather(here, precond, take(GATHER_REFS), 1), Gather(here, image, take(GATHER_REFS), SLICES)
    mine, mid, term_in, sector_in, ts_s, ts_r, ss_s, ss_r, load = take(9)
    terms, sectors, t, s = here.terms, here.sectors, here.t, here.s
    slots, _, rows, width = left.shape
    sub = rows // SLICES

    loads = [pltpu.make_async_copy(precond_hbm, precond.at[t], load.at[0]),
             pltpu.make_async_copy(wave_hbm, wave, load.at[1])]
    for j in range(slots):
        loads.append(pltpu.make_async_copy(right_hbm.at[j], right.at[j], load.at[2 + 2 * j]))
        loads.append(pltpu.make_async_copy(left_hbm.at[j], left.at[j], load.at[3 + 2 * j]))
    arrived = barrier(here)
    for copy in loads:
        copy.start()
    loads[0].wait()
    arrived()
    p_gather.begin(0)
    loads[1].wait()
    for r in range(terms):
        v_high[r * rows : (r + 1) * rows], v_low[r * rows : (r + 1) * rows] = split(wave[r])
    for j in range(slots):
        loads[2 + 2 * j].wait()
        r_high[j], r_low[j] = split(right[j])
    for j in range(slots):
        loads[3 + 2 * j].wait()

    def compute(exchange, i):
        part = pl.ds(pl.multiple_of(i * sub, sub), sub)
        for j in range(slots):
            place = target[0, j] - s + 1
            alive = j < count[0, 0]
            left_high, left_low = split(left[j, :, part, :].reshape(terms * sub, width))
            inner = product(left_high, left_low, v_high[...], v_low[...])
            in_high, in_low = split(inner)
            tile = product(in_high, in_low, r_high[j], r_low[j]).reshape(terms, sub, width)
            for p in range(3):
                chosen = jnp.where(jnp.logical_and(alive, place == p), tile, 0.0)
                if j == 0:
                    exchange.whole[p, :, part, :] = chosen
                else:
                    exchange.whole[p, :, part, :] += chosen

    def apply(exchange, finished, relayed):
        @pl.loop(0, SLICES + 3)
        def _(i):
            @pl.when(i < SLICES)
            def _():
                compute(exchange, i)
                exchange.sectors_out(i)

            @pl.when(jnp.logical_and(i >= 1, i < SLICES + 1))
            def _():
                exchange.corners(i - 1)

            @pl.when(jnp.logical_and(i >= 2, i < SLICES + 2))
            def _():
                exchange.sides(i - 2)

            @pl.when(i >= 3)
            def _():
                finished(i - 3, exchange.own(i - 3))

            relayed(i)

    def first_done(i, total):
        part = first.part(i)
        image[t, part] = total
        first_out[part] = total
        f_gather.begin(i)

    def relays(i):
        @pl.when(i == 2)
        def _():
            p_gather.relay(0)

        @pl.when(i >= 5)
        def _():
            f_gather.relay(i - 5)

    apply(first, first_done, relays)

    w, f, p = wave[t], image[t], precond[t]
    wf, ww = w * f, w * w

    def lanes(x):
        line = jnp.sum(x, axis=0, keepdims=True)
        return sum(line[:, c : c + 128] for c in range(0, line.shape[1], 128))

    mine[...] = jnp.zeros_like(mine)
    for i, x in enumerate((wf, ww, wf * p, ww * p)):
        mine[i : i + 1] = lanes(x)

    def to_term(k):
        return send(mine, term_in.at[k - 1], ts_s.at[k - 1], ts_r.at[k - 1], term=lax.rem(t + k, terms))

    def to_sector(k):
        return send(mid, sector_in.at[k - 1], ss_s.at[k - 1], ss_r.at[k - 1], sector=lax.rem(s + k, sectors))

    for k in range(1, terms):
        to_term(k).start()
    f_gather.relay(2)
    total = mine[...]
    for k in range(1, terms):
        to_term(k).wait_recv()
        total += term_in[k - 1]
    mid[...] = total
    for k in range(1, sectors):
        to_sector(k).start()
    f_gather.relay(3)
    p_gather.finish(0)
    for k in range(1, sectors):
        to_sector(k).wait_recv()
        total += sector_in[k - 1]
    cross, norm, a, b = (jnp.sum(total[i : i + 1], axis=1, keepdims=True) for i in range(4))
    rayleigh = cross / norm
    share = (a - rayleigh * b) / norm
    for i in range(SLICES):
        f_gather.finish(i)

    def corrected(r):
        return precond[r] * (image[r] - rayleigh * wave[r]) - share * wave[r]

    for r in range(terms):
        v_high[r * rows : (r + 1) * rows], v_low[r * rows : (r + 1) * rows] = split(corrected(r))
    correction_out[...] = corrected(t)

    def second_done(i, total):
        second_out[second.part(i)] = total

    apply(second, second_done, lambda i: None)

    first.drain()
    second.drain()
    p_gather.drain()
    f_gather.drain()
    for k in range(1, terms):
        to_term(k).wait_send()
    for k in range(1, sectors):
        to_sector(k).wait_send()


def per_device(wavefunction, precond, left_ops, right_ops, out_sector, live_counts):
    terms, sectors = lax.axis_size("term"), lax.axis_size("sector")
    width, slots = wavefunction.shape[1], left_ops.shape[1]
    rows = width // terms
    dma = pltpu.SemaphoreType.DMA
    slab = jax.ShapeDtypeStruct((rows, width), F32)
    block = pltpu.VMEM((terms, rows, width), F32)
    half = pltpu.VMEM((width, width), BF16)
    operators = pltpu.VMEM((slots, terms, rows, width), F32)
    halves = pltpu.VMEM((slots, width, width), BF16)
    tile = pltpu.VMEM((8, 128), F32)
    outs = pl.pallas_call(
        kernel,
        out_shape=(slab,) * 3,
        in_specs=[SMEM] * 2 + [ANY] * 4,
        out_specs=(VMEM,) * 3,
        scratch_shapes=Exchange.scratch(width, terms) * 2
        + [block, block, block, operators, pltpu.VMEM((slots, width, width), F32), halves, halves, half, half]
        + Gather.scratch(terms, 1) + Gather.scratch(terms, SLICES)
        + [tile, tile, pltpu.VMEM((terms - 1, 8, 128), F32), pltpu.VMEM((sectors - 1, 8, 128), F32),
           dma((terms - 1,)), dma((terms - 1,)), dma((sectors - 1,)), dma((sectors - 1,)), dma((2 + 2 * slots,))],
        compiler_params=pltpu.CompilerParams(collective_id=0, has_side_effects=True, vmem_limit_bytes=60 << 20),
    )(out_sector, live_counts, wavefunction.reshape(terms, rows, width), precond[0],
      left_ops.reshape(slots, terms, rows, width), right_ops[0])
    return tuple(x[None] for x in outs)


def solution(mesh):
    placed = (
        P("sector", None, None),
        P("sector", "term", None),
        P("sector", "term", None, None),
        P("sector", "term", None, None),
        P("sector", "term"),
        P("sector", "term"),
    )
    return jax.shard_map(
        per_device,
        mesh=mesh,
        in_specs=placed,
        out_specs=(P("sector", "term", None), P("sector", "term", None), P("sector", "term", None)),
        check_vma=False,
    )
```

```python
import functools
import math

import jax
import jax.numpy as jnp
from jax import lax
from jax.experimental import pallas as pl
from jax.experimental.pallas import tpu as pltpu
from jax.sharding import PartitionSpec as P

F32, BF16 = jnp.float32, jnp.bfloat16
MESH = pl.DeviceIdType.MESH
VMEM = pl.BlockSpec(memory_space=pltpu.VMEM)
HBM = pl.BlockSpec(memory_space=pltpu.HBM)
SLICES = 4
VMEM_BYTES = 67043328


def split(x):
    high = x.astype(BF16)
    return high, (x - high.astype(F32)).astype(BF16)


def product(a_high, a_low, b_high, b_low):
    dot = functools.partial(jnp.dot, preferred_element_type=F32)
    return dot(a_high, b_high) + dot(a_high, b_low) + dot(a_low, b_high)


def send(source, target, send_sem, recv_sem, **where):
    return pltpu.make_async_remote_copy(
        src_ref=source, dst_ref=target, send_sem=send_sem, recv_sem=recv_sem,
        device_id=where, device_id_type=MESH,
    )


def grid_of(terms):
    columns = max(d for d in range(1, math.isqrt(terms) + 1) if terms % d == 0)
    return terms // columns, columns


class Place:
    def __init__(self):
        self.terms, self.sectors = lax.axis_size("term"), lax.axis_size("sector")
        self.t, self.s = lax.axis_index("term"), lax.axis_index("sector")
        self.gy, self.gx = grid_of(self.terms)
        self.y, self.x = self.t // self.gx, lax.rem(self.t, self.gx)
        self.corners = [(dy, dx) for dy in range(1, self.gy) for dx in range(1, self.gx)]
        self.sides = [(dy, 0) for dy in range(1, self.gy)] + [(0, dx) for dx in range(1, self.gx)] + [(0, 0)]

    def at(self, dy, dx):
        return lax.rem(self.y + dy, self.gy) * self.gx + lax.rem(self.x + dx, self.gx)

    def peer(self, k):
        return {"term": lax.rem(self.t + k // self.sectors, self.terms),
                "sector": lax.rem(self.s + lax.rem(k, self.sectors), self.sectors)}


def barrier(here):
    sem = pltpu.get_barrier_semaphore()
    peers = here.terms * here.sectors - 1

    @pl.loop(1, peers + 1)
    def _(k):
        pl.semaphore_signal(sem, inc=1, device_id=here.peer(k), device_id_type=MESH)

    return lambda: pl.semaphore_wait(sem, peers)


class Exchange:
    def __init__(self, here, refs):
        self.here = here
        (self.whole, self.up_in, self.down_in, self.acc, self.da_in, self.db_in, self.x_in, self.y_in,
         self.up_s, self.up_r, self.down_s, self.down_r, self.da_s, self.da_r, self.db_s, self.db_r,
         self.x_s, self.x_r, self.y_s, self.y_r) = refs
        self.rows, self.width = self.acc.shape[1], self.acc.shape[2]
        self.sub, self.half = self.rows // SLICES, self.width // 2

    @staticmethod
    def scratch(width, terms):
        rows, half = width // terms, width // 2
        gy, gx = grid_of(terms)
        dma = pltpu.SemaphoreType.DMA
        whole = pltpu.VMEM((terms, rows, width), F32)
        return [
            pltpu.VMEM((3, terms, rows, width), F32), whole, whole, whole,
            pltpu.VMEM((gy, gx, rows, half), F32), pltpu.VMEM((gy, gx, rows, half), F32),
            pltpu.VMEM((gx, rows, width), F32), pltpu.VMEM((gy, rows, width), F32),
        ] + [dma((SLICES, terms))] * 4 + [dma((SLICES, gy, gx))] * 4 + [dma((SLICES, gx))] * 2 + [dma((SLICES, gy))] * 2

    def part(self, i):
        return pl.ds(pl.multiple_of(i * self.sub, self.sub), self.sub)

    def upward(self, r, i):
        h = self.here
        return send(self.whole.at[2, r, self.part(i)], self.up_in.at[r, self.part(i)], self.up_s.at[i, r],
                    self.up_r.at[i, r], sector=lax.rem(h.s + 1, h.sectors))

    def downward(self, r, i):
        h = self.here
        return send(self.whole.at[0, r, self.part(i)], self.down_in.at[r, self.part(i)], self.down_s.at[i, r],
                    self.down_r.at[i, r], sector=lax.rem(h.s + h.sectors - 1, h.sectors))

    def corner_a(self, dy, dx, i):
        h, part = self.here, self.part(i)
        return send(self.acc.at[h.at(dy, dx), part, : self.half], self.da_in.at[dy, dx, part],
                    self.da_s.at[i, dy, dx], self.da_r.at[i, dy, dx], term=h.at(0, dx))

    def corner_b(self, dy, dx, i):
        h, part = self.here, self.part(i)
        return send(self.acc.at[h.at(dy, dx), part, self.half :], self.db_in.at[dy, dx, part],
                    self.db_s.at[i, dy, dx], self.db_r.at[i, dy, dx], term=h.at(dy, 0))

    def along_x(self, dx, i):
        h, part = self.here, self.part(i)
        return send(self.acc.at[h.at(0, dx), part], self.x_in.at[dx, part], self.x_s.at[i, dx], self.x_r.at[i, dx],
                    term=h.at(0, dx))

    def along_y(self, dy, i):
        h, part = self.here, self.part(i)
        return send(self.acc.at[h.at(dy, 0), part], self.y_in.at[dy, part], self.y_s.at[i, dy], self.y_r.at[i, dy],
                    term=h.at(dy, 0))

    def sectors_out(self, slabs, i):
        h = self.here
        for dy, dx in slabs:
            r = h.at(dy, dx)

            @pl.when(h.s + 1 < h.sectors)
            def _():
                self.upward(r, i).start()

            @pl.when(h.s > 0)
            def _():
                self.downward(r, i).start()

    def merge(self, r, i):
        h, part = self.here, self.part(i)
        self.acc[r, part] = self.whole[1, r, part]

        @pl.when(h.s > 0)
        def _():
            self.upward(r, i).wait_recv()
            self.acc[r, part] += self.up_in[r, part]

        @pl.when(h.s + 1 < h.sectors)
        def _():
            self.downward(r, i).wait_recv()
            self.acc[r, part] += self.down_in[r, part]

    def corners(self, i):
        h = self.here
        for dy in range(1, h.gy):
            for dx in range(1, h.gx):
                self.merge(h.at(dy, dx), i)
                self.corner_a(dy, dx, i).start()
                self.corner_b(dy, dx, i).start()

    def sides(self, i):
        h, part = self.here, self.part(i)
        for dy in range(1, h.gy):
            r = h.at(dy, 0)
            self.merge(r, i)
            for dx in range(1, h.gx):
                self.corner_a(dy, dx, i).wait_recv()
                self.acc[r, part, : self.half] += self.da_in[dy, dx, part]
            self.along_y(dy, i).start()
        for dx in range(1, h.gx):
            r = h.at(0, dx)
            self.merge(r, i)
            for dy in range(1, h.gy):
                self.corner_b(dy, dx, i).wait_recv()
                self.acc[r, part, self.half :] += self.db_in[dy, dx, part]
            self.along_x(dx, i).start()

    def own(self, i):
        h, part = self.here, self.part(i)
        self.merge(h.t, i)
        total = self.acc[h.t, part]
        for dy in range(1, h.gy):
            self.along_y(dy, i).wait_recv()
            total += self.y_in[dy, part]
        for dx in range(1, h.gx):
            self.along_x(dx, i).wait_recv()
            total += self.x_in[dx, part]
        return total

    def drain(self):
        h = self.here

        @pl.loop(0, SLICES)
        def _(i):
            for dy, dx in h.corners + h.sides:
                r = h.at(dy, dx)

                @pl.when(h.s + 1 < h.sectors)
                def _():
                    self.upward(r, i).wait_send()

                @pl.when(h.s > 0)
                def _():
                    self.downward(r, i).wait_send()

                if dy and dx:
                    self.corner_a(dy, dx, i).wait_send()
                    self.corner_b(dy, dx, i).wait_send()
                elif dy:
                    self.along_y(dy, i).wait_send()
                elif dx:
                    self.along_x(dx, i).wait_send()


class Gather:
    def __init__(self, here, full, refs, pieces):
        self.here, self.full = here, full
        self.x_s, self.x_r, self.y_s, self.y_r, self.a_s, self.a_r, self.b_s, self.b_r = refs
        self.sub, self.half = full.shape[1] // pieces, full.shape[2] // 2
        self.pieces = pieces

    @staticmethod
    def scratch(terms, pieces):
        gy, gx = grid_of(terms)
        dma = pltpu.SemaphoreType.DMA
        return [dma((pieces, gx))] * 2 + [dma((pieces, gy))] * 2 + [dma((pieces, gy, gx))] * 4

    def part(self, i):
        return pl.ds(pl.multiple_of(i * self.sub, self.sub), self.sub)

    def to_x(self, r, dx, i):
        ref = self.full.at[r, self.part(i)]
        return send(ref, ref, self.x_s.at[i, dx], self.x_r.at[i, dx], term=self.here.at(0, dx))

    def to_y(self, r, dy, i):
        ref = self.full.at[r, self.part(i)]
        return send(ref, ref, self.y_s.at[i, dy], self.y_r.at[i, dy], term=self.here.at(dy, 0))

    def relay_a(self, r, dy, dx, i):
        ref = self.full.at[r, self.part(i), : self.half]
        return send(ref, ref, self.a_s.at[i, dy, dx], self.a_r.at[i, dy, dx], term=self.here.at(0, dx))

    def relay_b(self, r, dy, dx, i):
        ref = self.full.at[r, self.part(i), self.half :]
        return send(ref, ref, self.b_s.at[i, dy, dx], self.b_r.at[i, dy, dx], term=self.here.at(dy, 0))

    def begin(self, i):
        h = self.here
        for dx in range(1, h.gx):
            self.to_x(h.t, dx, i).start()
        for dy in range(1, h.gy):
            self.to_y(h.t, dy, i).start()

    def relay(self, i):
        h = self.here
        for dx in range(1, h.gx):
            r = h.at(0, dx)
            self.to_x(r, h.gx - dx, i).wait_recv()
            for dy in range(1, h.gy):
                self.relay_b(r, dy, dx, i).start()
        for dy in range(1, h.gy):
            r = h.at(dy, 0)
            self.to_y(r, h.gy - dy, i).wait_recv()
            for dx in range(1, h.gx):
                self.relay_a(r, dy, dx, i).start()

    def finish(self, i):
        h = self.here
        for dy in range(1, h.gy):
            for dx in range(1, h.gx):
                self.relay_a(h.at(dy, h.gx - dx), dy, dx, i).wait_recv()
                self.relay_b(h.at(h.gy - dy, dx), dy, dx, i).wait_recv()

    def drain(self):
        h = self.here

        @pl.loop(0, self.pieces)
        def _(i):
            for dx in range(1, h.gx):
                self.to_x(h.t, dx, i).wait_send()
            for dy in range(1, h.gy):
                self.to_y(h.t, dy, i).wait_send()
            for dy in range(1, h.gy):
                for dx in range(1, h.gx):
                    self.relay_a(h.at(dy, 0), dy, dx, i).wait_send()
                    self.relay_b(h.at(0, dx), dy, dx, i).wait_send()


EXCHANGE_REFS, GATHER_REFS = 20, 8


def kernel(target_hbm, count_hbm, wave_hbm, precond_hbm, left_hbm, right_hbm, first_out, correction_out, second_out, *scratch):
    scratch = list(scratch)

    def take(n):
        refs = scratch[:n]
        del scratch[:n]
        return refs

    here = Place()
    first, second = Exchange(here, take(EXCHANGE_REFS)), Exchange(here, take(EXCHANGE_REFS))
    wave, precond, image, left, right, r_high, r_low, v_high, v_low, in_high, in_low, target, count = take(13)
    p_gather, f_gather = Gather(here, precond, take(GATHER_REFS), 1), Gather(here, image, take(GATHER_REFS), SLICES)
    sums, mine, theirs, all_s, all_r, load = take(6)
    terms, sectors, t, s = here.terms, here.sectors, here.t, here.s
    slots, _, rows, width = left.shape
    sub = rows // SLICES
    peers = terms * sectors - 1

    order = here.corners + here.sides
    load_precond = pltpu.make_async_copy(precond_hbm, precond.at[t], load.at[0])
    load_wave = pltpu.make_async_copy(wave_hbm, wave, load.at[1])
    load_target = pltpu.make_async_copy(target_hbm, target, load.at[2])
    load_count = pltpu.make_async_copy(count_hbm, count, load.at[3])
    load_right = [pltpu.make_async_copy(right_hbm.at[j], right.at[j], load.at[4 + j]) for j in range(slots)]
    load_left = [pltpu.make_async_copy(left_hbm.at[:, here.at(*o)], left.at[:, here.at(*o)], load.at[4 + slots + n])
                 for n, o in enumerate(order)]
    corners = len(here.corners)
    arrived = barrier(here)
    for copy in [load_precond, load_wave, load_target, load_count] + load_left[:corners] + load_right + load_left[corners:]:
        copy.start()

    def split_rows(value):
        for r in range(terms):
            v_high[r * rows : (r + 1) * rows], v_low[r * rows : (r + 1) * rows] = split(value(r))

    def inner(slabs, part):
        stack = jnp.concatenate([left[j, here.at(*o), part] for j in range(slots) for o in slabs], axis=0)
        return split(product(*split(stack), v_high[...], v_low[...]))

    def chosen(j, p, tile):
        hit = jnp.logical_and(j < count[0, 0], target[0, j] - s + 1 == p)
        return jnp.where(hit, tile, 0.0)

    def compute(exchange, slabs, part, size):
        high, low = inner(slabs, part)
        m = len(slabs) * size
        tiles = [product(high[j * m : (j + 1) * m], low[j * m : (j + 1) * m], r_high[j], r_low[j]) for j in range(slots)]
        for n, o in enumerate(slabs):
            for p in range(3):
                exchange.whole[p, here.at(*o), part] = sum(
                    chosen(j, p, tiles[j][n * size : (n + 1) * size]) for j in range(slots))

    every = pl.ds(0, rows)

    def corners_first(exchange):
        m = corners * rows
        with jax.named_scope("startv"):
            load_wave.wait()
            split_rows(lambda r: wave[r])
        with jax.named_scope("startl"):
            for copy in load_left[:corners]:
                copy.wait()
            in_high[...], in_low[...] = inner(here.corners, every)
        load_target.wait()
        load_count.wait()
        for j in range(slots):
            with jax.named_scope("startr"):
                load_right[j].wait()
                r_high[j], r_low[j] = split(right[j])
            tile = product(in_high[j * m : (j + 1) * m], in_low[j * m : (j + 1) * m], r_high[j], r_low[j])
            for n, o in enumerate(here.corners):
                for p in range(3):
                    part = chosen(j, p, tile[n * rows : (n + 1) * rows])
                    exchange.whole[p, here.at(*o)] = part if j == 0 else exchange.whole[p, here.at(*o)] + part

    def apply(exchange, begin, finished, relayed):
        with jax.named_scope("CD"):
            begin()
        for i in range(SLICES):
            exchange.sectors_out(here.corners, i)

        @pl.loop(0, SLICES + 4)
        def _(i):
            @pl.when(i < SLICES)
            def _():
                with jax.named_scope("C"):
                    compute(exchange, here.sides, exchange.part(i), sub)
                with jax.named_scope("S"):
                    exchange.sectors_out(here.sides, i)

            @pl.when(jnp.logical_and(i >= 1, i < 1 + SLICES // 2))
            def _():
                with jax.named_scope("Fd"):
                    exchange.corners(2 * i - 2)
                    exchange.corners(2 * i - 1)

            @pl.when(i >= 4)
            def _():
                with jax.named_scope("Fo"):
                    finished(i - 4, exchange.own(i - 4))

            @pl.when(jnp.logical_and(i >= 2, i < SLICES + 2))
            def _():
                with jax.named_scope("Fxy"):
                    exchange.sides(i - 2)

            relayed(i)

    def fold(x):
        x = jnp.sum(x.reshape(sub // 8, 8, width), axis=0)
        return sum(x[:, c : c + 128] for c in range(0, width, 128))

    def first_begin():
        corners_first(first)
        for copy in load_left[corners:]:
            copy.wait()

    def first_done(i, f):
        part = first.part(i)
        image[t, part] = f
        f_gather.begin(i)
        first_out[part] = f
        w, p = wave[t, part], precond[t, part]
        wf, ww = w * f, w * w
        for n, x in enumerate((wf, ww, wf * p, ww * p)):
            sums[n] += fold(x)

    def relays(i):
        @pl.when(i == 3)
        def _():
            with jax.named_scope("Gp"):
                p_gather.relay(0)

        @pl.when(i >= 6)
        def _():
            with jax.named_scope("Gf"):
                f_gather.relay(i - 6)

    with jax.named_scope("enter"):
        load_precond.wait()
        arrived()
        p_gather.begin(0)
    sums[...] = jnp.zeros_like(sums)
    apply(first, first_begin, first_done, relays)

    def to_peer(k):
        return send(mine, theirs.at[k - 1], all_s.at[k - 1], all_r.at[k - 1], **here.peer(k))

    lane = lax.broadcasted_iota(jnp.int32, (1, 128), 1)
    row = jnp.zeros((1, 128), F32)
    for n in range(4):
        row = jnp.where(lane == n, jnp.sum(sums[n], keepdims=True), row)
    mine[...] = row

    @pl.loop(1, peers + 1)
    def _(k):
        to_peer(k).start()

    with jax.named_scope("relay2"):
        f_gather.relay(2)
        f_gather.relay(3)
        p_gather.finish(0)
    with jax.named_scope("peers"):
        @pl.loop(1, peers + 1)
        def _(k):
            to_peer(k).wait_recv()

    total = mine[...] + jnp.sum(theirs[...], axis=0)
    cross, norm, a, b = (total[:, n : n + 1] for n in range(4))
    rayleigh = cross / norm
    share = (a - rayleigh * b) / norm
    with jax.named_scope("gfin"):
        for i in range(SLICES):
            f_gather.finish(i)

    def corrected(r):
        return precond[r] * (image[r] - rayleigh * wave[r]) - share * wave[r]

    with jax.named_scope("corr"):
        split_rows(corrected)
        correction_out[...] = corrected(t)

    def second_done(i, total):
        second_out[second.part(i)] = total

    apply(second, lambda: compute(second, here.corners, every, rows), second_done, lambda i: None)

    with jax.named_scope("drain"):
        first.drain()
        second.drain()
        p_gather.drain()
        f_gather.drain()

        @pl.loop(1, peers + 1)
        def _(k):
            to_peer(k).wait_send()


def publish_kernel(*refs):
    ins, outs, sems = refs[:3], refs[3:6], refs[6]
    copies = [pltpu.make_async_copy(a, b, sems.at[n]) for n, (a, b) in enumerate(zip(ins, outs))]
    for copy in copies:
        copy.start()
    for copy in copies:
        copy.wait()


def per_device(wavefunction, precond, left_ops, right_ops, out_sector, live_counts):
    terms, sectors = lax.axis_size("term"), lax.axis_size("sector")
    width, slots = wavefunction.shape[1], left_ops.shape[1]
    rows = width // terms
    gy, gx = grid_of(terms)
    dma = pltpu.SemaphoreType.DMA
    slab = jax.ShapeDtypeStruct((rows, width), F32)
    block = pltpu.VMEM((terms, rows, width), F32)
    half = pltpu.VMEM((width, width), BF16)
    operators = pltpu.VMEM((slots, terms, rows, width), F32)
    halves = pltpu.VMEM((slots, width, width), BF16)
    inner = pltpu.VMEM((slots * (gy - 1) * (gx - 1) * rows, width), BF16)
    peers = terms * sectors - 1
    outs = pl.pallas_call(
        kernel,
        out_shape=(pltpu.VMEM((rows, width), F32),) * 3,
        in_specs=[HBM] * 6,
        out_specs=(VMEM,) * 3,
        scratch_shapes=Exchange.scratch(width, terms) * 2
        + [block, block, block, operators, pltpu.VMEM((slots, width, width), F32), halves, halves, half, half, inner, inner,
           pltpu.SMEM(out_sector.shape, jnp.int32), pltpu.SMEM(live_counts.shape, jnp.int32)]
        + Gather.scratch(terms, 1) + Gather.scratch(terms, SLICES)
        + [pltpu.VMEM((4, 8, 128), F32), pltpu.VMEM((1, 128), F32), pltpu.VMEM((peers, 1, 128), F32),
           dma((peers,)), dma((peers,)), dma((4 + slots + terms,))],
        compiler_params=pltpu.CompilerParams(collective_id=0, has_side_effects=True, vmem_limit_bytes=VMEM_BYTES - 3 * 4 * rows * width - (192 << 10)),
    )(out_sector, live_counts, wavefunction.reshape(terms, rows, width), precond[0],
      left_ops.reshape(slots, terms, rows, width), right_ops[0])
    outs = pl.pallas_call(
        publish_kernel,
        out_shape=(slab,) * 3,
        in_specs=[VMEM] * 3,
        out_specs=(HBM,) * 3,
        scratch_shapes=[dma((3,))],
        compiler_params=pltpu.CompilerParams(vmem_limit_bytes=1 << 20),
    )(*outs)
    return tuple(x[None] for x in outs)


def solution(mesh):
    placed = (
        P("sector", None, None),
        P("sector", "term", None),
        P("sector", "term", None, None),
        P("sector", "term", None, None),
        P("sector", "term"),
        P("sector", "term"),
    )
    return jax.shard_map(
        per_device,
        mesh=mesh,
        in_specs=placed,
        out_specs=(P("sector", "term", None), P("sector", "term", None), P("sector", "term", None)),
        check_vma=False,
    )
```

```python
import functools
import math

import jax
import jax.numpy as jnp
from jax import lax
from jax.experimental import pallas as pl
from jax.experimental.pallas import tpu as pltpu
from jax.sharding import PartitionSpec as P

F32, BF16 = jnp.float32, jnp.bfloat16
MESH = pl.DeviceIdType.MESH
VMEM = pl.BlockSpec(memory_space=pltpu.VMEM)
HBM = pl.BlockSpec(memory_space=pltpu.HBM)
SLICES = 4
VMEM_BYTES = 67043328


def split(x):
    high = x.astype(BF16)
    return high, (x - high.astype(F32)).astype(BF16)


def product(a_high, a_low, b_high, b_low):
    dot = functools.partial(jnp.dot, preferred_element_type=F32)
    return dot(a_high, b_high) + dot(a_high, b_low) + dot(a_low, b_high)


def send(source, target, send_sem, recv_sem, **where):
    return pltpu.make_async_remote_copy(
        src_ref=source, dst_ref=target, send_sem=send_sem, recv_sem=recv_sem,
        device_id=where, device_id_type=MESH,
    )


def grid_of(terms):
    columns = max(d for d in range(1, math.isqrt(terms) + 1) if terms % d == 0)
    return terms // columns, columns


class Place:
    def __init__(self):
        self.terms, self.sectors = lax.axis_size("term"), lax.axis_size("sector")
        self.t, self.s = lax.axis_index("term"), lax.axis_index("sector")
        self.gy, self.gx = grid_of(self.terms)
        self.y, self.x = self.t // self.gx, lax.rem(self.t, self.gx)
        self.corners = [(dy, dx) for dy in range(1, self.gy) for dx in range(1, self.gx)]
        self.sides = [(dy, 0) for dy in range(1, self.gy)] + [(0, dx) for dx in range(1, self.gx)] + [(0, 0)]

    def at(self, dy, dx):
        return lax.rem(self.y + dy, self.gy) * self.gx + lax.rem(self.x + dx, self.gx)

    def corner(self, dy, dx):
        return (dy - 1) * (self.gx - 1) + dx - 1

    def peer(self, k):
        return {"term": lax.rem(self.t + k // self.sectors, self.terms),
                "sector": lax.rem(self.s + lax.rem(k, self.sectors), self.sectors)}


def barrier(here):
    sem = pltpu.get_barrier_semaphore()
    peers = here.terms * here.sectors - 1

    @pl.loop(1, peers + 1)
    def _(k):
        pl.semaphore_signal(sem, inc=1, device_id=here.peer(k), device_id_type=MESH)

    return lambda: pl.semaphore_wait(sem, peers)


class Exchange:
    def __init__(self, here, refs, sems):
        self.here = here
        self.whole, self.up_in, self.down_in, self.acc, self.da_in, self.db_in, self.x_in, self.y_in = refs
        (self.z_s, self.up_r, self.down_r, self.da_s, self.da_r, self.db_s, self.db_r,
         self.x_s, self.x_r, self.y_s, self.y_r) = sems
        self.rows, self.width = self.acc.shape[1], self.acc.shape[2]
        self.sub, self.half = self.rows // SLICES, self.width // 2

    @staticmethod
    def buffers(width, terms):
        rows, half = width // terms, width // 2
        gy, gx = grid_of(terms)
        whole = pltpu.VMEM((terms, rows, width), F32)
        corner = pltpu.VMEM(((gy - 1) * (gx - 1), rows, half), F32)
        return [pltpu.VMEM((3, terms, rows, width), F32), whole, whole, whole, corner, corner,
                pltpu.VMEM((gx - 1, rows, width), F32), pltpu.VMEM((gy - 1, rows, width), F32)]

    @staticmethod
    def semaphores(terms):
        gy, gx = grid_of(terms)
        dma, corners = pltpu.SemaphoreType.DMA, (gy - 1) * (gx - 1)
        return [dma((2,)), dma((SLICES, terms)), dma((SLICES, terms))] + [dma((corners,)), dma((SLICES, corners))] * 2 + [
            dma((gx - 1,)), dma((SLICES, gx - 1)), dma((gy - 1,)), dma((SLICES, gy - 1))]

    def part(self, i):
        return pl.ds(pl.multiple_of(i * self.sub, self.sub), self.sub)

    def upward(self, r, i):
        h = self.here
        return send(self.whole.at[2, r, self.part(i)], self.up_in.at[r, self.part(i)], self.z_s.at[1],
                    self.up_r.at[i, r], sector=lax.rem(h.s + 1, h.sectors))

    def downward(self, r, i):
        h = self.here
        return send(self.whole.at[0, r, self.part(i)], self.down_in.at[r, self.part(i)], self.z_s.at[0],
                    self.down_r.at[i, r], sector=lax.rem(h.s + h.sectors - 1, h.sectors))

    def corner_a(self, dy, dx, i):
        h, part, c = self.here, self.part(i), self.here.corner(dy, dx)
        return send(self.acc.at[h.at(dy, dx), part, : self.half], self.da_in.at[c, part],
                    self.da_s.at[c], self.da_r.at[i, c], term=h.at(0, dx))

    def corner_b(self, dy, dx, i):
        h, part, c = self.here, self.part(i), self.here.corner(dy, dx)
        return send(self.acc.at[h.at(dy, dx), part, self.half :], self.db_in.at[c, part],
                    self.db_s.at[c], self.db_r.at[i, c], term=h.at(dy, 0))

    def along_x(self, dx, i):
        h, part = self.here, self.part(i)
        return send(self.acc.at[h.at(0, dx), part], self.x_in.at[dx - 1, part], self.x_s.at[dx - 1], self.x_r.at[i, dx - 1],
                    term=h.at(0, dx))

    def along_y(self, dy, i):
        h, part = self.here, self.part(i)
        return send(self.acc.at[h.at(dy, 0), part], self.y_in.at[dy - 1, part], self.y_s.at[dy - 1], self.y_r.at[i, dy - 1],
                    term=h.at(dy, 0))

    def sectors_out(self, slabs, i):
        h = self.here
        for dy, dx in slabs:
            r = h.at(dy, dx)

            @pl.when(h.s + 1 < h.sectors)
            def _():
                self.upward(r, i).start()

            @pl.when(h.s > 0)
            def _():
                self.downward(r, i).start()

    def merge(self, r, i):
        h, part = self.here, self.part(i)
        self.acc[r, part] = self.whole[1, r, part]

        @pl.when(h.s > 0)
        def _():
            self.upward(r, i).wait_recv()
            self.acc[r, part] += self.up_in[r, part]

        @pl.when(h.s + 1 < h.sectors)
        def _():
            self.downward(r, i).wait_recv()
            self.acc[r, part] += self.down_in[r, part]

    def corners(self, i):
        h = self.here
        for dy in range(1, h.gy):
            for dx in range(1, h.gx):
                self.merge(h.at(dy, dx), i)
                self.corner_a(dy, dx, i).start()
                self.corner_b(dy, dx, i).start()

    def sides(self, i):
        h, part = self.here, self.part(i)
        for dy in range(1, h.gy):
            r = h.at(dy, 0)
            self.merge(r, i)
            for dx in range(1, h.gx):
                self.corner_a(dy, dx, i).wait_recv()
                self.acc[r, part, : self.half] += self.da_in[h.corner(dy, dx), part]
            self.along_y(dy, i).start()
        for dx in range(1, h.gx):
            r = h.at(0, dx)
            self.merge(r, i)
            for dy in range(1, h.gy):
                self.corner_b(dy, dx, i).wait_recv()
                self.acc[r, part, self.half :] += self.db_in[h.corner(dy, dx), part]
            self.along_x(dx, i).start()

    def own(self, i):
        h, part = self.here, self.part(i)
        self.merge(h.t, i)
        total = self.acc[h.t, part]
        for dy in range(1, h.gy):
            self.along_y(dy, i).wait_recv()
            total += self.y_in[dy - 1, part]
        for dx in range(1, h.gx):
            self.along_x(dx, i).wait_recv()
            total += self.x_in[dx - 1, part]
        return total

    def drain(self):
        h = self.here

        def sent(source, target, sem):
            send(source, target, sem, self.up_r.at[0, 0], term=h.at(0, 1), sector=h.s).wait_send()

        @pl.when(h.s + 1 < h.sectors)
        def _():
            sent(self.whole.at[2], self.up_in, self.z_s.at[1])

        @pl.when(h.s > 0)
        def _():
            sent(self.whole.at[0], self.down_in, self.z_s.at[0])

        for dy, dx in h.corners:
            c = h.corner(dy, dx)
            sent(self.da_in.at[c], self.da_in.at[c], self.da_s.at[c])
            sent(self.db_in.at[c], self.db_in.at[c], self.db_s.at[c])
        for n in range(h.gx - 1):
            sent(self.x_in.at[n], self.x_in.at[n], self.x_s.at[n])
        for n in range(h.gy - 1):
            sent(self.y_in.at[n], self.y_in.at[n], self.y_s.at[n])


class Gather:
    def __init__(self, here, full, refs, pieces):
        self.here, self.full = here, full
        self.x_s, self.x_r, self.y_s, self.y_r, self.a_s, self.a_r, self.b_s, self.b_r = refs
        self.sub, self.half = full.shape[1] // pieces, full.shape[2] // 2
        self.pieces = pieces

    @staticmethod
    def scratch(terms, pieces):
        gy, gx = grid_of(terms)
        dma = pltpu.SemaphoreType.DMA
        corners = (gy - 1) * (gx - 1)
        return [dma((gx - 1,)), dma((pieces, gx - 1)), dma((gy - 1,)), dma((pieces, gy - 1))] + [
            dma((corners,)), dma((pieces, corners))] * 2

    def part(self, i):
        return pl.ds(pl.multiple_of(i * self.sub, self.sub), self.sub)

    def to_x(self, r, dx, i):
        ref = self.full.at[r, self.part(i)]
        return send(ref, ref, self.x_s.at[dx - 1], self.x_r.at[i, dx - 1], term=self.here.at(0, dx))

    def to_y(self, r, dy, i):
        ref = self.full.at[r, self.part(i)]
        return send(ref, ref, self.y_s.at[dy - 1], self.y_r.at[i, dy - 1], term=self.here.at(dy, 0))

    def relay_a(self, r, dy, dx, i):
        ref, c = self.full.at[r, self.part(i), : self.half], self.here.corner(dy, dx)
        return send(ref, ref, self.a_s.at[c], self.a_r.at[i, c], term=self.here.at(0, dx))

    def relay_b(self, r, dy, dx, i):
        ref, c = self.full.at[r, self.part(i), self.half :], self.here.corner(dy, dx)
        return send(ref, ref, self.b_s.at[c], self.b_r.at[i, c], term=self.here.at(dy, 0))

    def begin(self, i):
        h = self.here
        for dx in range(1, h.gx):
            self.to_x(h.t, dx, i).start()
        for dy in range(1, h.gy):
            self.to_y(h.t, dy, i).start()

    def relay(self, i):
        h = self.here
        for dx in range(1, h.gx):
            r = h.at(0, dx)
            self.to_x(r, h.gx - dx, i).wait_recv()
            for dy in range(1, h.gy):
                self.relay_b(r, dy, dx, i).start()
        for dy in range(1, h.gy):
            r = h.at(dy, 0)
            self.to_y(r, h.gy - dy, i).wait_recv()
            for dx in range(1, h.gx):
                self.relay_a(r, dy, dx, i).start()

    def finish(self, i):
        h = self.here
        for dy in range(1, h.gy):
            for dx in range(1, h.gx):
                self.relay_a(h.at(dy, h.gx - dx), dy, dx, i).wait_recv()
                self.relay_b(h.at(h.gy - dy, dx), dy, dx, i).wait_recv()

    def drain(self):
        h = self.here

        def sent(ref, sem):
            send(ref, ref, sem, self.x_r.at[0, 0], term=h.at(0, 1)).wait_send()

        for n in range(h.gx - 1):
            sent(self.full.at[h.t], self.x_s.at[n])
        for n in range(h.gy - 1):
            sent(self.full.at[h.t], self.y_s.at[n])
        for dy, dx in h.corners:
            sent(self.full.at[h.at(dy, 0), :, : self.half], self.a_s.at[h.corner(dy, dx)])
            sent(self.full.at[h.at(0, dx), :, self.half :], self.b_s.at[h.corner(dy, dx)])


BUFFERS, SEMAPHORES, GATHER_REFS = 8, 11, 8


def kernel(target_hbm, count_hbm, wave_hbm, precond_hbm, left_hbm, right_hbm, first_out, correction_out, second_out, *scratch):
    scratch = list(scratch)

    def take(n):
        refs = scratch[:n]
        del scratch[:n]
        return refs

    here = Place()
    buffers, more, sems = take(BUFFERS), take(BUFFERS), take(SEMAPHORES)
    first, second = Exchange(here, buffers, sems), Exchange(here, more, sems)
    wave, precond, image, left, right, r_high, r_low, v_high, v_low, in_high, in_low, target, count = take(13)
    p_gather, f_gather = Gather(here, precond, take(GATHER_REFS), 1), Gather(here, image, take(GATHER_REFS), SLICES)
    sums, mine, theirs, all_s, all_r, load = take(6)
    terms, sectors, t, s = here.terms, here.sectors, here.t, here.s
    slots, _, rows, width = left.shape
    sub = rows // SLICES
    peers = terms * sectors - 1

    order = here.corners + here.sides
    load_precond = pltpu.make_async_copy(precond_hbm, precond.at[t], load.at[0])
    load_wave = pltpu.make_async_copy(wave_hbm, wave, load.at[1])
    load_target = pltpu.make_async_copy(target_hbm, target, load.at[2])
    load_count = pltpu.make_async_copy(count_hbm, count, load.at[3])
    load_right = [pltpu.make_async_copy(right_hbm.at[j], right.at[j], load.at[4 + j]) for j in range(slots)]
    load_left = [pltpu.make_async_copy(left_hbm.at[:, here.at(*o)], left.at[:, here.at(*o)], load.at[4 + slots + n])
                 for n, o in enumerate(order)]
    corners = len(here.corners)
    arrived = barrier(here)
    for copy in [load_precond, load_wave, load_target, load_count] + load_left[:corners] + load_right + load_left[corners:]:
        copy.start()

    def split_rows(value):
        for r in range(terms):
            v_high[r * rows : (r + 1) * rows], v_low[r * rows : (r + 1) * rows] = split(value(r))

    def inner(slabs, part):
        stack = jnp.concatenate([left[j, here.at(*o), part] for j in range(slots) for o in slabs], axis=0)
        return split(product(*split(stack), v_high[...], v_low[...]))

    def chosen(j, p, tile):
        hit = jnp.logical_and(j < count[0, 0], target[0, j] - s + 1 == p)
        return jnp.where(hit, tile, 0.0)

    def compute(exchange, slabs, part, size):
        high, low = inner(slabs, part)
        m = len(slabs) * size
        tiles = [product(high[j * m : (j + 1) * m], low[j * m : (j + 1) * m], r_high[j], r_low[j]) for j in range(slots)]
        for n, o in enumerate(slabs):
            for p in range(3):
                exchange.whole[p, here.at(*o), part] = sum(
                    chosen(j, p, tiles[j][n * size : (n + 1) * size]) for j in range(slots))

    every = pl.ds(0, rows)

    def corners_first(exchange):
        m = corners * rows
        with jax.named_scope("startv"):
            load_wave.wait()
            split_rows(lambda r: wave[r])
        with jax.named_scope("startl"):
            for copy in load_left[:corners]:
                copy.wait()
            in_high[...], in_low[...] = inner(here.corners, every)
        load_target.wait()
        load_count.wait()
        pairs = [range(j, min(j + 2, slots)) for j in range(0, slots, 2)]
        for pair in pairs:
            with jax.named_scope("startr"):
                for j in pair:
                    load_right[j].wait()
                tiles = {}
                for j in pair:
                    high, low = split(right[j])
                    r_high[j], r_low[j] = high, low
                    tiles[j] = product(in_high[j * m : (j + 1) * m], in_low[j * m : (j + 1) * m], high, low)
                for n, o in enumerate(here.corners):
                    for p in range(3):
                        part = sum(chosen(j, p, tiles[j][n * rows : (n + 1) * rows]) for j in pair)
                        ref = exchange.whole.at[p, here.at(*o)]
                        ref[...] = part if pair == pairs[0] else ref[...] + part

    def apply(exchange, begin, finished, relayed):
        with jax.named_scope("CD"):
            begin()
        for i in range(SLICES):
            exchange.sectors_out(here.corners, i)

        @pl.loop(0, SLICES + 4)
        def _(i):
            @pl.when(i < SLICES)
            def _():
                with jax.named_scope("C"):
                    compute(exchange, here.sides, exchange.part(i), sub)
                with jax.named_scope("S"):
                    exchange.sectors_out(here.sides, i)

            @pl.when(jnp.logical_and(i >= 1, i < 1 + SLICES // 2))
            def _():
                with jax.named_scope("Fd"):
                    exchange.corners(2 * i - 2)
                    exchange.corners(2 * i - 1)

            relayed(i)

            @pl.when(jnp.logical_and(i >= 2, i < SLICES + 2))
            def _():
                with jax.named_scope("Fxy"):
                    exchange.sides(i - 2)

            @pl.when(i >= 4)
            def _():
                with jax.named_scope("Fo"):
                    finished(i - 4, exchange.own(i - 4))

    def fold(x):
        x = jnp.sum(x.reshape(sub // 8, 8, width), axis=0)
        return sum(x[:, c : c + 128] for c in range(0, width, 128))

    def first_begin():
        corners_first(first)
        for copy in load_left[corners:]:
            copy.wait()

    def first_done(i, f):
        part = first.part(i)
        image[t, part] = f

        @pl.when(i == 1)
        def _():
            f_gather.begin(0)

        @pl.when(i >= 1)
        def _():
            f_gather.begin(i)

        first_out[part] = f
        w, p = wave[t, part], precond[t, part]
        wf, ww = w * f, w * w
        for n, x in enumerate((wf, ww, wf * p, ww * p)):
            sums[n] += fold(x)

    def relays(i):
        @pl.when(i == 2)
        def _():
            with jax.named_scope("Gp"):
                p_gather.relay(0)

    with jax.named_scope("enter"):
        load_precond.wait()
        arrived()
        p_gather.begin(0)
    sums[...] = jnp.zeros_like(sums)
    apply(first, first_begin, first_done, relays)

    def to_peer(k):
        return send(mine, theirs.at[k - 1], all_s.at[0], all_r.at[0], **here.peer(k))

    all_peers = send(theirs, theirs, all_s.at[0], all_r.at[0], **here.peer(1))
    with jax.named_scope("sums"):
        shape = (4, 128)
        diagonal = lax.broadcasted_iota(jnp.int32, shape, 0) == lax.broadcasted_iota(jnp.int32, shape, 1)
        line = jnp.sum(jnp.sum(sums[...], axis=1), axis=1, keepdims=True)
        mine[...] = jnp.sum(jnp.where(diagonal, line, 0.0), axis=0, keepdims=True)

        @pl.loop(1, peers + 1)
        def _(k):
            to_peer(k).start()

    with jax.named_scope("relay2"):
        for i in range(SLICES):
            f_gather.relay(i)
        p_gather.finish(0)
    with jax.named_scope("peers"):
        all_peers.wait_recv()

    total = mine[...] + jnp.sum(theirs[...], axis=0)
    cross, norm, a, b = (total[:, n : n + 1] for n in range(4))
    rayleigh = cross / norm
    share = (a - rayleigh * b) / norm
    with jax.named_scope("gfin"):
        for i in range(SLICES):
            f_gather.finish(i)

    def corrected(r):
        return precond[r] * (image[r] - rayleigh * wave[r]) - share * wave[r]

    with jax.named_scope("corr"):
        split_rows(corrected)
        correction_out[...] = corrected(t)

    def second_done(i, total):
        second_out[second.part(i)] = total

    first.drain()
    apply(second, lambda: compute(second, here.corners, every, rows), second_done, lambda i: None)

    with jax.named_scope("drain"):
        second.drain()
        p_gather.drain()
        f_gather.drain()
        all_peers.wait_send()


def publish_kernel(*refs):
    ins, outs, sems = refs[:3], refs[3:6], refs[6]
    copies = [pltpu.make_async_copy(a, b, sems.at[n]) for n, (a, b) in enumerate(zip(ins, outs))]
    for copy in copies:
        copy.start()
    for copy in copies:
        copy.wait()


def per_device(wavefunction, precond, left_ops, right_ops, out_sector, live_counts):
    terms, sectors = lax.axis_size("term"), lax.axis_size("sector")
    width, slots = wavefunction.shape[1], left_ops.shape[1]
    rows = width // terms
    gy, gx = grid_of(terms)
    dma = pltpu.SemaphoreType.DMA
    slab = jax.ShapeDtypeStruct((rows, width), F32)
    block = pltpu.VMEM((terms, rows, width), F32)
    half = pltpu.VMEM((width, width), BF16)
    operators = pltpu.VMEM((slots, terms, rows, width), F32)
    halves = pltpu.VMEM((slots, width, width), BF16)
    inner = pltpu.VMEM((slots * (gy - 1) * (gx - 1) * rows, width), BF16)
    peers = terms * sectors - 1
    outs = pl.pallas_call(
        kernel,
        out_shape=(pltpu.VMEM((rows, width), F32),) * 3,
        in_specs=[HBM] * 6,
        out_specs=(VMEM,) * 3,
        scratch_shapes=Exchange.buffers(width, terms) * 2 + Exchange.semaphores(terms)
        + [block, block, block, operators, pltpu.VMEM((slots, width, width), F32), halves, halves, half, half, inner, inner,
           pltpu.SMEM(out_sector.shape, jnp.int32), pltpu.SMEM(live_counts.shape, jnp.int32)]
        + Gather.scratch(terms, 1) + Gather.scratch(terms, SLICES)
        + [pltpu.VMEM((4, 8, 128), F32), pltpu.VMEM((1, 128), F32), pltpu.VMEM((peers, 1, 128), F32),
           dma((1,)), dma((1,)), dma((4 + slots + terms,))],
        compiler_params=pltpu.CompilerParams(collective_id=0, has_side_effects=True, vmem_limit_bytes=VMEM_BYTES - 3 * 4 * rows * width - (192 << 10)),
    )(out_sector, live_counts, wavefunction.reshape(terms, rows, width), precond[0],
      left_ops.reshape(slots, terms, rows, width), right_ops[0])
    outs = pl.pallas_call(
        publish_kernel,
        out_shape=(slab,) * 3,
        in_specs=[VMEM] * 3,
        out_specs=(HBM,) * 3,
        scratch_shapes=[dma((3,))],
        compiler_params=pltpu.CompilerParams(vmem_limit_bytes=1 << 20),
    )(*outs)
    return tuple(x[None] for x in outs)


def solution(mesh):
    placed = (
        P("sector", None, None),
        P("sector", "term", None),
        P("sector", "term", None, None),
        P("sector", "term", None, None),
        P("sector", "term"),
        P("sector", "term"),
    )
    return jax.shard_map(
        per_device,
        mesh=mesh,
        in_specs=placed,
        out_specs=(P("sector", "term", None), P("sector", "term", None), P("sector", "term", None)),
        check_vma=False,
    )
```

```python
import functools
import math

import jax
import jax.numpy as jnp
from jax import lax
from jax.experimental import pallas as pl
from jax.experimental.pallas import tpu as pltpu
from jax.sharding import PartitionSpec as P

F32, BF16 = jnp.float32, jnp.bfloat16
MESH = pl.DeviceIdType.MESH
VMEM = pl.BlockSpec(memory_space=pltpu.VMEM)
HBM = pl.BlockSpec(memory_space=pltpu.HBM)
SLICES = 4
VMEM_BYTES = 67043328


def split(x):
    high = x.astype(BF16)
    return high, (x - high.astype(F32)).astype(BF16)


def product(a_high, a_low, b_high, b_low):
    dot = functools.partial(jnp.dot, preferred_element_type=F32)
    return dot(a_high, b_high) + dot(a_high, b_low) + dot(a_low, b_high)


def send(source, target, send_sem, recv_sem, **where):
    return pltpu.make_async_remote_copy(
        src_ref=source, dst_ref=target, send_sem=send_sem, recv_sem=recv_sem,
        device_id=where, device_id_type=MESH,
    )


def grid_of(terms):
    columns = max(d for d in range(1, math.isqrt(terms) + 1) if terms % d == 0)
    return terms // columns, columns


class Place:
    def __init__(self):
        self.terms, self.sectors = lax.axis_size("term"), lax.axis_size("sector")
        self.t, self.s = lax.axis_index("term"), lax.axis_index("sector")
        self.gy, self.gx = grid_of(self.terms)
        self.y, self.x = self.t // self.gx, lax.rem(self.t, self.gx)
        self.corners = [(dy, dx) for dy in range(1, self.gy) for dx in range(1, self.gx)]
        self.sides = [(dy, 0) for dy in range(1, self.gy)] + [(0, dx) for dx in range(1, self.gx)]
        self.own = [(0, 0)]

    def at(self, dy, dx):
        return lax.rem(self.y + dy, self.gy) * self.gx + lax.rem(self.x + dx, self.gx)

    def corner(self, dy, dx):
        return (dy - 1) * (self.gx - 1) + dx - 1

    def peer(self, k):
        return {"term": lax.rem(self.t + k // self.sectors, self.terms),
                "sector": lax.rem(self.s + lax.rem(k, self.sectors), self.sectors)}


def barrier(here):
    sem = pltpu.get_barrier_semaphore()
    peers = here.terms * here.sectors - 1

    @pl.loop(1, peers + 1)
    def _(k):
        pl.semaphore_signal(sem, inc=1, device_id=here.peer(k), device_id_type=MESH)

    return lambda: pl.semaphore_wait(sem, peers)


class Exchange:
    def __init__(self, here, refs, sems):
        self.here = here
        self.whole, self.up_in, self.down_in, self.acc, self.da_in, self.db_in, self.x_in, self.y_in = refs
        (self.z_s, self.up_r, self.down_r, self.da_s, self.da_r, self.db_s, self.db_r,
         self.x_s, self.x_r, self.y_s, self.y_r) = sems
        self.rows, self.width = self.acc.shape[1], self.acc.shape[2]
        self.sub, self.half = self.rows // SLICES, self.width // 2

    @staticmethod
    def buffers(width, terms):
        rows, half = width // terms, width // 2
        gy, gx = grid_of(terms)
        whole = pltpu.VMEM((terms, rows, width), F32)
        corner = pltpu.VMEM(((gy - 1) * (gx - 1), rows, half), F32)
        return [pltpu.VMEM((3, terms, rows, width), F32), whole, whole, whole, corner, corner,
                pltpu.VMEM((gx - 1, rows, width), F32), pltpu.VMEM((gy - 1, rows, width), F32)]

    @staticmethod
    def semaphores(terms):
        gy, gx = grid_of(terms)
        dma, corners = pltpu.SemaphoreType.DMA, (gy - 1) * (gx - 1)
        return [dma((2,)), dma((SLICES, terms)), dma((SLICES, terms))] + [dma((corners,)), dma((SLICES, corners))] * 2 + [
            dma((gx - 1,)), dma((SLICES, gx - 1)), dma((gy - 1,)), dma((SLICES, gy - 1))]

    def part(self, i):
        return pl.ds(pl.multiple_of(i * self.sub, self.sub), self.sub)

    def upward(self, r, i):
        h = self.here
        return send(self.whole.at[2, r, self.part(i)], self.up_in.at[r, self.part(i)], self.z_s.at[1],
                    self.up_r.at[i, r], sector=lax.rem(h.s + 1, h.sectors))

    def downward(self, r, i):
        h = self.here
        return send(self.whole.at[0, r, self.part(i)], self.down_in.at[r, self.part(i)], self.z_s.at[0],
                    self.down_r.at[i, r], sector=lax.rem(h.s + h.sectors - 1, h.sectors))

    def corner_a(self, dy, dx, i):
        h, part, c = self.here, self.part(i), self.here.corner(dy, dx)
        return send(self.acc.at[h.at(dy, dx), part, : self.half], self.da_in.at[c, part],
                    self.da_s.at[c], self.da_r.at[i, c], term=h.at(0, dx))

    def corner_b(self, dy, dx, i):
        h, part, c = self.here, self.part(i), self.here.corner(dy, dx)
        return send(self.acc.at[h.at(dy, dx), part, self.half :], self.db_in.at[c, part],
                    self.db_s.at[c], self.db_r.at[i, c], term=h.at(dy, 0))

    def along_x(self, dx, i):
        h, part = self.here, self.part(i)
        return send(self.acc.at[h.at(0, dx), part], self.x_in.at[dx - 1, part], self.x_s.at[dx - 1], self.x_r.at[i, dx - 1],
                    term=h.at(0, dx))

    def along_y(self, dy, i):
        h, part = self.here, self.part(i)
        return send(self.acc.at[h.at(dy, 0), part], self.y_in.at[dy - 1, part], self.y_s.at[dy - 1], self.y_r.at[i, dy - 1],
                    term=h.at(dy, 0))

    def sectors_out(self, slabs, i):
        h = self.here
        for dy, dx in slabs:
            r = h.at(dy, dx)

            @pl.when(h.s + 1 < h.sectors)
            def _():
                self.upward(r, i).start()

            @pl.when(h.s > 0)
            def _():
                self.downward(r, i).start()

    def merge(self, r, i):
        h, part = self.here, self.part(i)
        self.acc[r, part] = self.whole[1, r, part]

        @pl.when(h.s > 0)
        def _():
            self.upward(r, i).wait_recv()
            self.acc[r, part] += self.up_in[r, part]

        @pl.when(h.s + 1 < h.sectors)
        def _():
            self.downward(r, i).wait_recv()
            self.acc[r, part] += self.down_in[r, part]

    def corners(self, i):
        h = self.here
        for dy in range(1, h.gy):
            for dx in range(1, h.gx):
                self.merge(h.at(dy, dx), i)
                self.corner_a(dy, dx, i).start()
                self.corner_b(dy, dx, i).start()

    def sides(self, i):
        h, part = self.here, self.part(i)
        for dy in range(1, h.gy):
            r = h.at(dy, 0)
            self.merge(r, i)
            for dx in range(1, h.gx):
                self.corner_a(dy, dx, i).wait_recv()
                self.acc[r, part, : self.half] += self.da_in[h.corner(dy, dx), part]
            self.along_y(dy, i).start()
        for dx in range(1, h.gx):
            r = h.at(0, dx)
            self.merge(r, i)
            for dy in range(1, h.gy):
                self.corner_b(dy, dx, i).wait_recv()
                self.acc[r, part, self.half :] += self.db_in[h.corner(dy, dx), part]
            self.along_x(dx, i).start()

    def own(self, i):
        h, part = self.here, self.part(i)
        self.merge(h.t, i)
        total = self.acc[h.t, part]
        for dy in range(1, h.gy):
            self.along_y(dy, i).wait_recv()
            total += self.y_in[dy - 1, part]
        for dx in range(1, h.gx):
            self.along_x(dx, i).wait_recv()
            total += self.x_in[dx - 1, part]
        return total

    def drain(self):
        h = self.here

        def sent(source, target, sem):
            send(source, target, sem, self.up_r.at[0, 0], term=h.at(0, 1), sector=h.s).wait_send()

        @pl.when(h.s + 1 < h.sectors)
        def _():
            sent(self.whole.at[2], self.up_in, self.z_s.at[1])

        @pl.when(h.s > 0)
        def _():
            sent(self.whole.at[0], self.down_in, self.z_s.at[0])

        for dy, dx in h.corners:
            c = h.corner(dy, dx)
            sent(self.da_in.at[c], self.da_in.at[c], self.da_s.at[c])
            sent(self.db_in.at[c], self.db_in.at[c], self.db_s.at[c])
        for n in range(h.gx - 1):
            sent(self.x_in.at[n], self.x_in.at[n], self.x_s.at[n])
        for n in range(h.gy - 1):
            sent(self.y_in.at[n], self.y_in.at[n], self.y_s.at[n])


class Gather:
    def __init__(self, here, full, refs, pieces):
        self.here, self.full = here, full
        self.x_s, self.x_r, self.y_s, self.y_r, self.a_s, self.a_r, self.b_s, self.b_r = refs
        self.sub, self.half = full.shape[1] // pieces, full.shape[2] // 2
        self.pieces = pieces

    @staticmethod
    def scratch(terms, pieces):
        gy, gx = grid_of(terms)
        dma = pltpu.SemaphoreType.DMA
        corners = (gy - 1) * (gx - 1)
        return [dma((gx - 1,)), dma((pieces, gx - 1)), dma((gy - 1,)), dma((pieces, gy - 1))] + [
            dma((corners,)), dma((pieces, corners))] * 2

    def part(self, i):
        return pl.ds(pl.multiple_of(i * self.sub, self.sub), self.sub)

    def to_x(self, r, dx, i):
        ref = self.full.at[r, self.part(i)]
        return send(ref, ref, self.x_s.at[dx - 1], self.x_r.at[i, dx - 1], term=self.here.at(0, dx))

    def to_y(self, r, dy, i):
        ref = self.full.at[r, self.part(i)]
        return send(ref, ref, self.y_s.at[dy - 1], self.y_r.at[i, dy - 1], term=self.here.at(dy, 0))

    def relay_a(self, r, dy, dx, i):
        ref, c = self.full.at[r, self.part(i), : self.half], self.here.corner(dy, dx)
        return send(ref, ref, self.a_s.at[c], self.a_r.at[i, c], term=self.here.at(0, dx))

    def relay_b(self, r, dy, dx, i):
        ref, c = self.full.at[r, self.part(i), self.half :], self.here.corner(dy, dx)
        return send(ref, ref, self.b_s.at[c], self.b_r.at[i, c], term=self.here.at(dy, 0))

    def begin(self, i):
        h = self.here
        for dx in range(1, h.gx):
            self.to_x(h.t, dx, i).start()
        for dy in range(1, h.gy):
            self.to_y(h.t, dy, i).start()

    def relay(self, i):
        h = self.here
        for dx in range(1, h.gx):
            r = h.at(0, dx)
            self.to_x(r, h.gx - dx, i).wait_recv()
            for dy in range(1, h.gy):
                self.relay_b(r, dy, dx, i).start()
        for dy in range(1, h.gy):
            r = h.at(dy, 0)
            self.to_y(r, h.gy - dy, i).wait_recv()
            for dx in range(1, h.gx):
                self.relay_a(r, dy, dx, i).start()

    def finish(self, i):
        h = self.here
        for dy in range(1, h.gy):
            for dx in range(1, h.gx):
                self.relay_a(h.at(dy, h.gx - dx), dy, dx, i).wait_recv()
                self.relay_b(h.at(h.gy - dy, dx), dy, dx, i).wait_recv()

    def drain(self):
        h = self.here

        def sent(ref, sem):
            send(ref, ref, sem, self.x_r.at[0, 0], term=h.at(0, 1)).wait_send()

        for n in range(h.gx - 1):
            sent(self.full.at[h.t], self.x_s.at[n])
        for n in range(h.gy - 1):
            sent(self.full.at[h.t], self.y_s.at[n])
        for dy, dx in h.corners:
            sent(self.full.at[h.at(dy, 0), :, : self.half], self.a_s.at[h.corner(dy, dx)])
            sent(self.full.at[h.at(0, dx), :, self.half :], self.b_s.at[h.corner(dy, dx)])


BUFFERS, SEMAPHORES, GATHER_REFS = 8, 11, 8


def kernel(target_hbm, count_hbm, wave_hbm, precond_hbm, left_hbm, right_hbm, first_out, correction_out, second_out, *scratch):
    scratch = list(scratch)

    def take(n):
        refs = scratch[:n]
        del scratch[:n]
        return refs

    here = Place()
    buffers, more, sems = take(BUFFERS), take(BUFFERS), take(SEMAPHORES)
    first, second = Exchange(here, buffers, sems), Exchange(here, more, sems)
    wave, precond, image, left, right, r_high, r_low, v_high, v_low, in_high, in_low, target, count = take(13)
    p_gather, f_gather = Gather(here, precond, take(GATHER_REFS), SLICES), Gather(here, image, take(GATHER_REFS), SLICES)
    sums, mine, theirs, all_s, all_r, load = take(6)
    terms, sectors, t, s = here.terms, here.sectors, here.t, here.s
    slots, _, rows, width = left.shape
    sub = rows // SLICES
    peers = terms * sectors - 1

    order = here.corners + here.sides + here.own
    load_precond = pltpu.make_async_copy(precond_hbm, precond.at[t], load.at[0])
    load_wave = pltpu.make_async_copy(wave_hbm, wave, load.at[1])
    load_target = pltpu.make_async_copy(target_hbm, target, load.at[2])
    load_count = pltpu.make_async_copy(count_hbm, count, load.at[3])
    load_right = [pltpu.make_async_copy(right_hbm.at[j], right.at[j], load.at[4 + j]) for j in range(slots)]
    load_left = [pltpu.make_async_copy(left_hbm.at[:, here.at(*o)], left.at[:, here.at(*o)], load.at[4 + slots + n])
                 for n, o in enumerate(order)]
    corners = len(here.corners)
    arrived = barrier(here)
    for copy in [load_precond, load_wave, load_target, load_count] + load_left[:corners] + load_right + load_left[corners:]:
        copy.start()

    def split_rows(value, start, size):
        for r in range(terms):
            to = pl.ds(r * rows + start, size)
            v_high[to], v_low[to] = split(value(r, pl.ds(start, size)))

    def inner(slabs, part):
        stack = jnp.concatenate([left[j, here.at(*o), part] for j in range(slots) for o in slabs], axis=0)
        return split(product(*split(stack), v_high[...], v_low[...]))

    def chosen(j, p, tile):
        hit = jnp.logical_and(j < count[0, 0], target[0, j] - s + 1 == p)
        return jnp.where(hit, tile, 0.0)

    def compute(exchange, slabs, part, size):
        high, low = inner(slabs, part)
        m = len(slabs) * size
        tiles = [product(high[j * m : (j + 1) * m], low[j * m : (j + 1) * m], r_high[j], r_low[j]) for j in range(slots)]
        for n, o in enumerate(slabs):
            for p in range(3):
                exchange.whole[p, here.at(*o), part] = sum(
                    chosen(j, p, tiles[j][n * size : (n + 1) * size]) for j in range(slots))

    every = pl.ds(0, rows)

    def corners_first(exchange):
        m = corners * rows
        with jax.named_scope("startv"):
            load_wave.wait()
            split_rows(lambda r, part: wave[r, part], 0, rows)
        with jax.named_scope("startl"):
            for copy in load_left[:corners]:
                copy.wait()
            in_high[...], in_low[...] = inner(here.corners, every)
        load_target.wait()
        load_count.wait()
        pairs = [range(j, min(j + 2, slots)) for j in range(0, slots, 2)]
        for pair in pairs:
            with jax.named_scope("startr"):
                for j in pair:
                    load_right[j].wait()
                tiles = {}
                for j in pair:
                    high, low = split(right[j])
                    r_high[j], r_low[j] = high, low
                    tiles[j] = product(in_high[j * m : (j + 1) * m], in_low[j * m : (j + 1) * m], high, low)
                for n, o in enumerate(here.corners):
                    for p in range(3):
                        part = sum(chosen(j, p, tiles[j][n * rows : (n + 1) * rows]) for j in pair)
                        ref = exchange.whole.at[p, here.at(*o)]
                        ref[...] = part if pair == pairs[0] else ref[...] + part

    def apply(exchange, begin, finished, meanwhile):
        with jax.named_scope("CD"):
            begin()
        for i in range(SLICES):
            exchange.sectors_out(here.corners, i)
        meanwhile(0)

        @pl.loop(0, SLICES // 2)
        def _(b):
            with jax.named_scope("C"):
                compute(exchange, here.sides, pl.ds(pl.multiple_of(b * 2 * sub, 2 * sub), 2 * sub), 2 * sub)
            exchange.sectors_out(here.sides, 2 * b)
            exchange.sectors_out(here.sides, 2 * b + 1)
            meanwhile(b + 1)

        with jax.named_scope("Fd"):
            for i in range(SLICES // 2):
                exchange.corners(i)
        with jax.named_scope("CO"):
            compute(exchange, here.own, every, rows)
        for i in range(SLICES):
            exchange.sectors_out(here.own, i)
        with jax.named_scope("Fd"):
            for i in range(SLICES // 2, SLICES):
                exchange.corners(i)
        meanwhile(SLICES - 1)

        @pl.loop(0, SLICES)
        def _(i):
            with jax.named_scope("Fxy"):
                exchange.sides(i)

        @pl.loop(0, SLICES)
        def _(i):
            with jax.named_scope("Fo"):
                finished(i, exchange.own(i))

    def fold(x):
        x = jnp.sum(x.reshape(sub // 8, 8, width), axis=0)
        return sum(x[:, c : c + 128] for c in range(0, width, 128))

    def first_begin():
        corners_first(first)
        for copy in load_left[corners:]:
            copy.wait()

    def first_done(i, f):
        part = first.part(i)
        image[t, part] = f

        @pl.when(i < SLICES - 1)
        def _():
            f_gather.begin(i)

        first_out[part] = f
        w, p = wave[t, part], precond[t, part]
        wf, ww = w * f, w * w
        for n, x in enumerate((wf, ww, wf * p, ww * p)):
            sums[n] += fold(x)

    with jax.named_scope("enter"):
        load_precond.wait()
        arrived()
        for i in range(SLICES):
            p_gather.begin(i)
    sums[...] = jnp.zeros_like(sums)
    apply(first, first_begin, first_done, p_gather.relay)

    def to_peer(k):
        return send(mine, theirs.at[k - 1], all_s.at[0], all_r.at[0], **here.peer(k))

    all_peers = send(theirs, theirs, all_s.at[0], all_r.at[0], **here.peer(1))
    with jax.named_scope("sums"):
        shape = (4, 128)
        diagonal = lax.broadcasted_iota(jnp.int32, shape, 0) == lax.broadcasted_iota(jnp.int32, shape, 1)
        line = jnp.sum(jnp.sum(sums[...], axis=1), axis=1, keepdims=True)
        mine[...] = jnp.sum(jnp.where(diagonal, line, 0.0), axis=0, keepdims=True)

        @pl.loop(1, peers + 1)
        def _(k):
            to_peer(k).start()

    with jax.named_scope("relay2"):
        f_gather.begin(SLICES - 1)
        for i in range(SLICES):
            p_gather.finish(i)
        for i in range(SLICES):
            f_gather.relay(i)
    with jax.named_scope("peers"):
        all_peers.wait_recv()

    total = mine[...] + jnp.sum(theirs[...], axis=0)
    cross, norm, a, b = (total[:, n : n + 1] for n in range(4))
    rayleigh = cross / norm
    share = (a - rayleigh * b) / norm

    def corrected(r, part):
        return precond[r, part] * (image[r, part] - rayleigh * wave[r, part]) - share * wave[r, part]

    correction_out[...] = corrected(t, every)
    for i in range(SLICES):
        with jax.named_scope("gfin"):
            f_gather.finish(i)
        with jax.named_scope("corr"):
            split_rows(corrected, i * sub, sub)

    def second_done(i, total):
        second_out[second.part(i)] = total

    first.drain()
    apply(second, lambda: compute(second, here.corners, every, rows), second_done, lambda i: None)

    with jax.named_scope("drain"):
        second.drain()
        p_gather.drain()
        f_gather.drain()
        all_peers.wait_send()


def publish_kernel(*refs):
    ins, outs, sems = refs[:3], refs[3:6], refs[6]
    copies = [pltpu.make_async_copy(a, b, sems.at[n]) for n, (a, b) in enumerate(zip(ins, outs))]
    for copy in copies:
        copy.start()
    for copy in copies:
        copy.wait()


def per_device(wavefunction, precond, left_ops, right_ops, out_sector, live_counts):
    terms, sectors = lax.axis_size("term"), lax.axis_size("sector")
    width, slots = wavefunction.shape[1], left_ops.shape[1]
    rows = width // terms
    gy, gx = grid_of(terms)
    dma = pltpu.SemaphoreType.DMA
    slab = jax.ShapeDtypeStruct((rows, width), F32)
    block = pltpu.VMEM((terms, rows, width), F32)
    half = pltpu.VMEM((width, width), BF16)
    operators = pltpu.VMEM((slots, terms, rows, width), F32)
    halves = pltpu.VMEM((slots, width, width), BF16)
    inner = pltpu.VMEM((slots * (gy - 1) * (gx - 1) * rows, width), BF16)
    peers = terms * sectors - 1
    outs = pl.pallas_call(
        kernel,
        out_shape=(pltpu.VMEM((rows, width), F32),) * 3,
        in_specs=[HBM] * 6,
        out_specs=(VMEM,) * 3,
        scratch_shapes=Exchange.buffers(width, terms) * 2 + Exchange.semaphores(terms)
        + [block, block, block, operators, pltpu.VMEM((slots, width, width), F32), halves, halves, half, half, inner, inner,
           pltpu.SMEM(out_sector.shape, jnp.int32), pltpu.SMEM(live_counts.shape, jnp.int32)]
        + Gather.scratch(terms, SLICES) * 2
        + [pltpu.VMEM((4, 8, 128), F32), pltpu.VMEM((1, 128), F32), pltpu.VMEM((peers, 1, 128), F32),
           dma((1,)), dma((1,)), dma((4 + slots + terms,))],
        compiler_params=pltpu.CompilerParams(collective_id=0, has_side_effects=True, vmem_limit_bytes=VMEM_BYTES - 3 * 4 * rows * width - (192 << 10)),
    )(out_sector, live_counts, wavefunction.reshape(terms, rows, width), precond[0],
      left_ops.reshape(slots, terms, rows, width), right_ops[0])
    outs = pl.pallas_call(
        publish_kernel,
        out_shape=(slab,) * 3,
        in_specs=[VMEM] * 3,
        out_specs=(HBM,) * 3,
        scratch_shapes=[dma((3,))],
        compiler_params=pltpu.CompilerParams(vmem_limit_bytes=1 << 20),
    )(*outs)
    return tuple(x[None] for x in outs)


def solution(mesh):
    placed = (
        P("sector", None, None),
        P("sector", "term", None),
        P("sector", "term", None, None),
        P("sector", "term", None, None),
        P("sector", "term"),
        P("sector", "term"),
    )
    return jax.shard_map(
        per_device,
        mesh=mesh,
        in_specs=placed,
        out_specs=(P("sector", "term", None), P("sector", "term", None), P("sector", "term", None)),
        check_vma=False,
    )
```

```python
import functools
import math

import jax
import jax.numpy as jnp
from jax import lax
from jax.experimental import pallas as pl
from jax.experimental.pallas import tpu as pltpu
from jax.sharding import PartitionSpec as P

F32, BF16 = jnp.float32, jnp.bfloat16
MESH = pl.DeviceIdType.MESH
VMEM = pl.BlockSpec(memory_space=pltpu.VMEM)
HBM = pl.BlockSpec(memory_space=pltpu.HBM)
SLICES = 4
EARLY = SLICES - 1
VMEM_BYTES = 67043328


def split(x):
    high = x.astype(BF16)
    return high, (x - high.astype(F32)).astype(BF16)


def product(a_high, a_low, b_high, b_low):
    dot = functools.partial(jnp.dot, preferred_element_type=F32)
    return dot(a_high, b_high) + dot(a_high, b_low) + dot(a_low, b_high)


def stacked(a_high, a_low, b_high, b_low):
    dot = functools.partial(jnp.dot, preferred_element_type=F32)
    m = a_high.shape[0]
    both = dot(jnp.concatenate([a_high, a_low], axis=0), b_high)
    return both[:m] + both[m:] + dot(a_high, b_low)


def send(source, target, send_sem, recv_sem, **where):
    return pltpu.make_async_remote_copy(
        src_ref=source, dst_ref=target, send_sem=send_sem, recv_sem=recv_sem,
        device_id=where, device_id_type=MESH,
    )


def grid_of(terms):
    columns = max(d for d in range(1, math.isqrt(terms) + 1) if terms % d == 0)
    return terms // columns, columns


class Place:
    def __init__(self):
        self.terms, self.sectors = lax.axis_size("term"), lax.axis_size("sector")
        self.t, self.s = lax.axis_index("term"), lax.axis_index("sector")
        self.gy, self.gx = grid_of(self.terms)
        self.y, self.x = self.t // self.gx, lax.rem(self.t, self.gx)
        self.corners = [(dy, dx) for dy in range(1, self.gy) for dx in range(1, self.gx)]
        self.sides = [(dy, 0) for dy in range(1, self.gy)] + [(0, dx) for dx in range(1, self.gx)]
        self.own = [(0, 0)]

    def at(self, dy, dx):
        return lax.rem(self.y + dy, self.gy) * self.gx + lax.rem(self.x + dx, self.gx)

    def corner(self, dy, dx):
        return (dy - 1) * (self.gx - 1) + dx - 1

    def peers(self):
        terms = [lax.rem(self.t + k, self.terms) for k in range(self.terms)]
        sectors = [lax.rem(self.s + k, self.sectors) for k in range(self.sectors)]
        pairs = [{"term": t, "sector": s} for t in terms for s in sectors]
        return list(enumerate(pairs[1:]))


def barrier(here):
    sem = pltpu.get_barrier_semaphore()
    peers = here.peers()
    for _, where in peers:
        pl.semaphore_signal(sem, inc=1, device_id=where, device_id_type=MESH)
    return lambda: pl.semaphore_wait(sem, len(peers))


class Total:
    def __init__(self, here, refs):
        self.here = here
        self.sums, self.mine, self.theirs, self.send_sem, self.recv_sem = refs

    @staticmethod
    def scratch(values, peers):
        dma = pltpu.SemaphoreType.DMA
        return [pltpu.VMEM((values, 8, 128), F32), pltpu.VMEM((1, 128), F32), pltpu.VMEM((peers, 1, 128), F32),
                dma((1,)), dma((1,))]

    def all(self):
        return send(self.theirs, self.theirs, self.send_sem.at[0], self.recv_sem.at[0], **self.here.peers()[0][1])

    def begin(self):
        shape = (self.sums.shape[0], 128)
        diagonal = lax.broadcasted_iota(jnp.int32, shape, 0) == lax.broadcasted_iota(jnp.int32, shape, 1)
        line = jnp.sum(jnp.sum(self.sums[...], axis=1), axis=1, keepdims=True)
        self.mine[...] = jnp.sum(jnp.where(diagonal, line, 0.0), axis=0, keepdims=True)
        for k, where in self.here.peers():
            send(self.mine, self.theirs.at[k], self.send_sem.at[0], self.recv_sem.at[0], **where).start()

    def finish(self):
        self.all().wait_recv()
        total = self.mine[...] + jnp.sum(self.theirs[...], axis=0)
        return [total[:, n : n + 1] for n in range(self.sums.shape[0])]

    def drain(self):
        self.all().wait_send()


class Exchange:
    def __init__(self, here, refs, sems, tally=None):
        self.here, self.tally = here, tally
        self.whole, self.up_in, self.down_in, self.acc, self.da_in, self.db_in, self.x_in, self.y_in = refs
        (self.z_s, self.up_r, self.down_r, self.da_s, self.da_r, self.db_s, self.db_r,
         self.x_s, self.x_r, self.y_s, self.y_r) = sems
        self.rows, self.width = self.acc.shape[1], self.acc.shape[2]
        self.sub, self.half = self.rows // SLICES, self.width // 2

    @staticmethod
    def buffers(width, terms):
        rows, half = width // terms, width // 2
        gy, gx = grid_of(terms)
        whole = pltpu.VMEM((terms, rows, width), F32)
        corner = pltpu.VMEM(((gy - 1) * (gx - 1), rows, half), F32)
        return [pltpu.VMEM((3, terms, rows, width), F32), whole, whole, whole, corner, corner,
                pltpu.VMEM((gx - 1, rows, width), F32), pltpu.VMEM((gy - 1, rows, width), F32)]

    @staticmethod
    def semaphores(terms):
        gy, gx = grid_of(terms)
        dma, corners = pltpu.SemaphoreType.DMA, (gy - 1) * (gx - 1)
        return [dma((2,)), dma((SLICES, terms)), dma((SLICES, terms))] + [dma((corners,)), dma((SLICES, corners))] * 2 + [
            dma((gx - 1,)), dma((SLICES, gx - 1)), dma((gy - 1,)), dma((SLICES, gy - 1))]

    def part(self, i):
        return pl.ds(pl.multiple_of(i * self.sub, self.sub), self.sub)

    def upward(self, r, i):
        h = self.here
        return send(self.whole.at[2, r, self.part(i)], self.up_in.at[r, self.part(i)], self.z_s.at[1],
                    self.up_r.at[i, r], sector=lax.rem(h.s + 1, h.sectors))

    def downward(self, r, i):
        h = self.here
        return send(self.whole.at[0, r, self.part(i)], self.down_in.at[r, self.part(i)], self.z_s.at[0],
                    self.down_r.at[i, r], sector=lax.rem(h.s + h.sectors - 1, h.sectors))

    def corner_a(self, dy, dx, i):
        h, part, c = self.here, self.part(i), self.here.corner(dy, dx)
        return send(self.acc.at[h.at(dy, dx), part, : self.half], self.da_in.at[c, part],
                    self.da_s.at[c], self.da_r.at[i, c], term=h.at(0, dx))

    def corner_b(self, dy, dx, i):
        h, part, c = self.here, self.part(i), self.here.corner(dy, dx)
        return send(self.acc.at[h.at(dy, dx), part, self.half :], self.db_in.at[c, part],
                    self.db_s.at[c], self.db_r.at[i, c], term=h.at(dy, 0))

    def along_x(self, dx, i):
        h, part = self.here, self.part(i)
        return send(self.acc.at[h.at(0, dx), part], self.x_in.at[dx - 1, part], self.x_s.at[dx - 1], self.x_r.at[i, dx - 1],
                    term=h.at(0, dx))

    def along_y(self, dy, i):
        h, part = self.here, self.part(i)
        return send(self.acc.at[h.at(dy, 0), part], self.y_in.at[dy - 1, part], self.y_s.at[dy - 1], self.y_r.at[i, dy - 1],
                    term=h.at(dy, 0))

    def sectors_out(self, slabs, i):
        h = self.here
        for dy, dx in slabs:
            r = h.at(dy, dx)

            @pl.when(h.s + 1 < h.sectors)
            def _():
                self.upward(r, i).start()

            @pl.when(h.s > 0)
            def _():
                self.downward(r, i).start()

    def merge(self, r, i):
        h, part = self.here, self.part(i)
        self.acc[r, part] = self.whole[1, r, part]

        @pl.when(h.s > 0)
        def _():
            self.upward(r, i).wait_recv()
            self.acc[r, part] += self.up_in[r, part]

        @pl.when(h.s + 1 < h.sectors)
        def _():
            self.downward(r, i).wait_recv()
            self.acc[r, part] += self.down_in[r, part]

        if self.tally:
            self.tally(r, part, self.acc[r, part])

    def corners(self, i):
        h = self.here
        for dy in range(1, h.gy):
            for dx in range(1, h.gx):
                self.merge(h.at(dy, dx), i)
                self.corner_a(dy, dx, i).start()
                self.corner_b(dy, dx, i).start()

    def sides(self, i):
        h, part = self.here, self.part(i)
        for dy in range(1, h.gy):
            r = h.at(dy, 0)
            self.merge(r, i)
            for dx in range(1, h.gx):
                self.corner_a(dy, dx, i).wait_recv()
                self.acc[r, part, : self.half] += self.da_in[h.corner(dy, dx), part]
            self.along_y(dy, i).start()
        for dx in range(1, h.gx):
            r = h.at(0, dx)
            self.merge(r, i)
            for dy in range(1, h.gy):
                self.corner_b(dy, dx, i).wait_recv()
                self.acc[r, part, self.half :] += self.db_in[h.corner(dy, dx), part]
            self.along_x(dx, i).start()

    def own(self, i):
        h, part = self.here, self.part(i)
        total = self.acc[h.t, part]
        for dy in range(1, h.gy):
            self.along_y(dy, i).wait_recv()
            total += self.y_in[dy - 1, part]
        for dx in range(1, h.gx):
            self.along_x(dx, i).wait_recv()
            total += self.x_in[dx - 1, part]
        return total

    def drain(self):
        h = self.here

        def sent(source, target, sem):
            send(source, target, sem, self.up_r.at[0, 0], term=h.at(0, 1), sector=h.s).wait_send()

        @pl.when(h.s + 1 < h.sectors)
        def _():
            sent(self.whole.at[2], self.up_in, self.z_s.at[1])

        @pl.when(h.s > 0)
        def _():
            sent(self.whole.at[0], self.down_in, self.z_s.at[0])

        for dy, dx in h.corners:
            c = h.corner(dy, dx)
            sent(self.da_in.at[c], self.da_in.at[c], self.da_s.at[c])
            sent(self.db_in.at[c], self.db_in.at[c], self.db_s.at[c])
        for n in range(h.gx - 1):
            sent(self.x_in.at[n], self.x_in.at[n], self.x_s.at[n])
        for n in range(h.gy - 1):
            sent(self.y_in.at[n], self.y_in.at[n], self.y_s.at[n])


class Gather:
    def __init__(self, here, full, refs, pieces):
        self.here, self.full = here, full
        self.x_s, self.x_r, self.y_s, self.y_r, self.a_s, self.a_r, self.b_s, self.b_r = refs
        self.sub, self.half, self.pieces = full.shape[1] // SLICES, full.shape[2] // 2, pieces

    @staticmethod
    def scratch(terms, pieces):
        gy, gx = grid_of(terms)
        dma = pltpu.SemaphoreType.DMA
        corners = (gy - 1) * (gx - 1)
        return [dma((gx - 1,)), dma((pieces, gx - 1)), dma((gy - 1,)), dma((pieces, gy - 1))] + [
            dma((corners,)), dma((pieces, corners))] * 2

    def part(self, i):
        return pl.ds(pl.multiple_of(i * self.sub, self.sub), self.sub)

    def to_x(self, r, dx, i):
        ref = self.full.at[r, self.part(i)]
        return send(ref, ref, self.x_s.at[dx - 1], self.x_r.at[i, dx - 1], term=self.here.at(0, dx))

    def to_y(self, r, dy, i):
        ref = self.full.at[r, self.part(i)]
        return send(ref, ref, self.y_s.at[dy - 1], self.y_r.at[i, dy - 1], term=self.here.at(dy, 0))

    def relay_a(self, r, dy, dx, i):
        ref, c = self.full.at[r, self.part(i), : self.half], self.here.corner(dy, dx)
        return send(ref, ref, self.a_s.at[c], self.a_r.at[i, c], term=self.here.at(0, dx))

    def relay_b(self, r, dy, dx, i):
        ref, c = self.full.at[r, self.part(i), self.half :], self.here.corner(dy, dx)
        return send(ref, ref, self.b_s.at[c], self.b_r.at[i, c], term=self.here.at(dy, 0))

    def begin(self, i):
        h = self.here
        for dx in range(1, h.gx):
            self.to_x(h.t, dx, i).start()
        for dy in range(1, h.gy):
            self.to_y(h.t, dy, i).start()

    def relay(self, i):
        h = self.here
        for dx in range(1, h.gx):
            r = h.at(0, dx)
            self.to_x(r, h.gx - dx, i).wait_recv()
            for dy in range(1, h.gy):
                self.relay_b(r, dy, dx, i).start()
        for dy in range(1, h.gy):
            r = h.at(dy, 0)
            self.to_y(r, h.gy - dy, i).wait_recv()
            for dx in range(1, h.gx):
                self.relay_a(r, dy, dx, i).start()

    def finish(self, i):
        h = self.here
        for dy in range(1, h.gy):
            for dx in range(1, h.gx):
                self.relay_a(h.at(dy, h.gx - dx), dy, dx, i).wait_recv()
                self.relay_b(h.at(h.gy - dy, dx), dy, dx, i).wait_recv()

    def drain(self):
        h, all_rows = self.here, pl.ds(0, self.pieces * self.sub)

        def sent(ref, sem):
            send(ref, ref, sem, self.x_r.at[0, 0], term=h.at(0, 1)).wait_send()

        for n in range(h.gx - 1):
            sent(self.full.at[h.t, all_rows], self.x_s.at[n])
        for n in range(h.gy - 1):
            sent(self.full.at[h.t, all_rows], self.y_s.at[n])
        for dy, dx in h.corners:
            sent(self.full.at[h.at(dy, 0), all_rows, : self.half], self.a_s.at[h.corner(dy, dx)])
            sent(self.full.at[h.at(0, dx), all_rows, self.half :], self.b_s.at[h.corner(dy, dx)])


BUFFERS, SEMAPHORES, GATHER_REFS, TOTAL_REFS = 8, 11, 8, 5


def kernel(target_hbm, count_hbm, wave_hbm, precond_hbm, left_hbm, right_hbm, first_out, correction_out, second_out, *scratch):
    scratch = list(scratch)

    def take(n):
        refs = scratch[:n]
        del scratch[:n]
        return refs

    here = Place()
    buffers, more, sems = take(BUFFERS), take(BUFFERS), take(SEMAPHORES)

    def fold(x):
        x = jnp.sum(x.reshape(x.shape[0] // 8, 8, width), axis=0)
        return sum(x[:, c : c + 128] for c in range(0, width, 128))

    def tally(r, part, value):
        overlap.sums[0] += fold(wave[r, part] * value)

    first, second = Exchange(here, buffers, sems, tally), Exchange(here, more, sems)
    wave, precond, image, left, right, r_high, r_low, v_high, v_low, in_high, in_low, target, count = take(13)
    p_gather, f_gather = Gather(here, precond, take(GATHER_REFS), EARLY), Gather(here, image, take(GATHER_REFS), SLICES)
    overlap, share_total, (load,) = Total(here, take(TOTAL_REFS)), Total(here, take(TOTAL_REFS)), take(1)
    t, s, terms = here.t, here.s, here.terms
    slots, _, rows, width = left.shape
    sub = rows // SLICES

    order = here.corners + here.sides + here.own
    load_precond = pltpu.make_async_copy(precond_hbm, precond.at[t], load.at[0])
    load_wave = pltpu.make_async_copy(wave_hbm, wave, load.at[1])
    load_target = pltpu.make_async_copy(target_hbm, target, load.at[2])
    load_count = pltpu.make_async_copy(count_hbm, count, load.at[3])
    load_right = [pltpu.make_async_copy(right_hbm.at[j], right.at[j], load.at[4 + j]) for j in range(slots)]
    load_left = [pltpu.make_async_copy(left_hbm.at[:, here.at(*o)], left.at[:, here.at(*o)], load.at[4 + slots + n])
                 for n, o in enumerate(order)]
    corners = len(here.corners)
    for copy in [load_precond, load_wave, load_target, load_count] + load_left[:corners] + load_right + load_left[corners:]:
        copy.start()
    arrived = barrier(here)

    def split_rows(value, start, size):
        for r in range(terms):
            to = pl.ds(r * rows + start, size)
            v_high[to], v_low[to] = split(value(r, pl.ds(start, size)))

    def inner(slabs, part):
        stack = jnp.concatenate([left[j, here.at(*o), part] for j in range(slots) for o in slabs], axis=0)
        return split(product(*split(stack), v_high[...], v_low[...]))

    def chosen(j, p, tile):
        hit = jnp.logical_and(j < count[0, 0], target[0, j] - s + 1 == p)
        return jnp.where(hit, tile, 0.0)

    def compute(exchange, slabs, part, size):
        high, low = inner(slabs, part)
        m = len(slabs) * size
        outer = stacked if m < 128 else product
        tiles = [outer(high[j * m : (j + 1) * m], low[j * m : (j + 1) * m], r_high[j], r_low[j]) for j in range(slots)]
        for n, o in enumerate(slabs):
            for p in range(3):
                exchange.whole[p, here.at(*o), part] = sum(
                    chosen(j, p, tiles[j][n * size : (n + 1) * size]) for j in range(slots))

    every = pl.ds(0, rows)

    def corners_first(exchange):
        m = corners * rows
        with jax.named_scope("startv"):
            load_wave.wait()
            split_rows(lambda r, part: wave[r, part], 0, rows)
        with jax.named_scope("startl"):
            for copy in load_left[:corners]:
                copy.wait()
            in_high[...], in_low[...] = inner(here.corners, every)
        load_target.wait()
        load_count.wait()
        pairs = [range(j, min(j + 2, slots)) for j in range(0, slots, 2)]
        for pair in pairs:
            with jax.named_scope("startr"):
                for j in pair:
                    load_right[j].wait()
                tiles = {}
                for j in pair:
                    high, low = split(right[j])
                    r_high[j], r_low[j] = high, low
                    tiles[j] = product(in_high[j * m : (j + 1) * m], in_low[j * m : (j + 1) * m], high, low)
                for n, o in enumerate(here.corners):
                    for p in range(3):
                        part = sum(chosen(j, p, tiles[j][n * rows : (n + 1) * rows]) for j in pair)
                        ref = exchange.whole.at[p, here.at(*o)]
                        ref[...] = part if pair == pairs[0] else ref[...] + part

    def apply(exchange, begin, meanwhile):
        with jax.named_scope("CD"):
            begin()
        for i in range(SLICES):
            exchange.sectors_out(here.corners, i)

        @pl.loop(0, SLICES)
        def _(b):
            with jax.named_scope("C"):
                compute(exchange, here.sides, exchange.part(b), sub)
            exchange.sectors_out(here.sides, b)
            with jax.named_scope("p"):
                meanwhile(b)

            @pl.when(b >= 1)
            def _():
                with jax.named_scope("Fd"):
                    exchange.corners(b - 1)

        with jax.named_scope("Fd"):
            exchange.corners(SLICES - 1)

        @pl.loop(0, 2)
        def _(h):
            with jax.named_scope("Fxy"):
                exchange.sides(h)
            with jax.named_scope("CO"):
                size = rows // 2
                compute(exchange, here.own, pl.ds(pl.multiple_of(h * size, size), size), size)
            for i in range(SLICES // 2):
                exchange.sectors_out(here.own, h * (SLICES // 2) + i)

        @pl.loop(2, SLICES)
        def _(i):
            with jax.named_scope("Fxy"):
                exchange.sides(i)

    def first_begin():
        corners_first(first)
        for copy in load_left[corners:]:
            copy.wait()

    def first_done(i):
        part = first.part(i)
        f = first.own(i)
        first_out[part] = f
        image[t, part] = f

    with jax.named_scope("enter"):
        load_precond.wait()
        arrived()
        for i in range(EARLY):
            p_gather.begin(i)
    overlap.sums[0] = jnp.zeros((8, 128), F32)
    def relays(b):
        @pl.when(b < EARLY)
        def _():
            p_gather.relay(b)

    apply(first, first_begin, relays)

    with jax.named_scope("Fo"):
        for i in range(2):
            first.merge(t, i)
        first_done(0)
        f_gather.begin(0)
    with jax.named_scope("Mo"):
        for i in range(2, SLICES):
            first.merge(t, i)
        overlap.sums[1] = fold(wave[t] * wave[t])
        overlap.begin()
    with jax.named_scope("Fo"):
        for i in range(1, SLICES):
            first_done(i)
            if i < EARLY:
                f_gather.begin(i)
    with jax.named_scope("relay0"):
        for i in range(EARLY):
            p_gather.finish(i)
        f_gather.relay(0)
    with jax.named_scope("ray"):
        cross, norm = overlap.finish()
        rayleigh = cross / norm

    def raw(r, part):
        return precond[r, part] * (image[r, part] - rayleigh * wave[r, part])

    with jax.named_scope("raw"):
        share_total.sums[0] = jnp.zeros((8, 128), F32)
        for i in reversed(range(SLICES)):
            part = first.part(i)
            own = raw(t, part)
            correction_out[part] = own
            share_total.sums[0] += fold(wave[t, part] * own)
            if i >= EARLY:
                image[t, part] = own
        share_total.begin()
        for i in range(EARLY, SLICES):
            f_gather.begin(i)
    with jax.named_scope("relay"):
        for i in range(1, SLICES):
            f_gather.relay(i)
    with jax.named_scope("share"):
        (dot,) = share_total.finish()
        share = dot / norm
    correction_out[...] -= share * wave[t]

    def corrected(r, part):
        return raw(r, part) - share * wave[r, part]

    for i in range(SLICES):
        with jax.named_scope("gfin"):
            f_gather.finish(i)
        with jax.named_scope("corr"):
            split_rows(corrected if i < EARLY else lambda r, part: image[r, part] - share * wave[r, part], i * sub, sub)

    first.drain()
    apply(second, lambda: compute(second, here.corners, every, rows), lambda i: None)

    @pl.loop(0, SLICES)
    def _(i):
        with jax.named_scope("Fo"):
            second.merge(t, i)
            second_out[second.part(i)] = second.own(i)

    with jax.named_scope("drain"):
        for stream in (second, p_gather, f_gather, overlap, share_total):
            stream.drain()


def publish_kernel(*refs):
    ins, outs, sems = refs[:3], refs[3:6], refs[6]
    copies = [pltpu.make_async_copy(a, b, sems.at[n]) for n, (a, b) in enumerate(zip(ins, outs))]
    for copy in copies:
        copy.start()
    for copy in copies:
        copy.wait()


def per_device(wavefunction, precond, left_ops, right_ops, out_sector, live_counts):
    terms, sectors = lax.axis_size("term"), lax.axis_size("sector")
    width, slots = wavefunction.shape[1], left_ops.shape[1]
    rows = width // terms
    gy, gx = grid_of(terms)
    dma = pltpu.SemaphoreType.DMA
    slab = jax.ShapeDtypeStruct((rows, width), F32)
    block = pltpu.VMEM((terms, rows, width), F32)
    half = pltpu.VMEM((width, width), BF16)
    operators = pltpu.VMEM((slots, terms, rows, width), F32)
    halves = pltpu.VMEM((slots, width, width), BF16)
    inner = pltpu.VMEM((slots * (gy - 1) * (gx - 1) * rows, width), BF16)
    peers = terms * sectors - 1
    outs = pl.pallas_call(
        kernel,
        out_shape=(pltpu.VMEM((rows, width), F32),) * 3,
        in_specs=[HBM] * 6,
        out_specs=(VMEM,) * 3,
        scratch_shapes=Exchange.buffers(width, terms) * 2 + Exchange.semaphores(terms)
        + [block, block, block, operators, pltpu.VMEM((slots, width, width), F32), halves, halves, half, half, inner, inner,
           pltpu.SMEM(out_sector.shape, jnp.int32), pltpu.SMEM(live_counts.shape, jnp.int32)]
        + Gather.scratch(terms, EARLY) + Gather.scratch(terms, SLICES)
        + Total.scratch(2, peers) + Total.scratch(1, peers) + [dma((4 + slots + terms,))],
        compiler_params=pltpu.CompilerParams(collective_id=0, has_side_effects=True, vmem_limit_bytes=VMEM_BYTES - 3 * 4 * rows * width - (192 << 10)),
    )(out_sector, live_counts, wavefunction.reshape(terms, rows, width), precond[0],
      left_ops.reshape(slots, terms, rows, width), right_ops[0])
    outs = pl.pallas_call(
        publish_kernel,
        out_shape=(slab,) * 3,
        in_specs=[VMEM] * 3,
        out_specs=(HBM,) * 3,
        scratch_shapes=[dma((3,))],
        compiler_params=pltpu.CompilerParams(vmem_limit_bytes=1 << 20),
    )(*outs)
    return tuple(x[None] for x in outs)


def solution(mesh):
    placed = (
        P("sector", None, None),
        P("sector", "term", None),
        P("sector", "term", None, None),
        P("sector", "term", None, None),
        P("sector", "term"),
        P("sector", "term"),
    )
    return jax.shard_map(
        per_device,
        mesh=mesh,
        in_specs=placed,
        out_specs=(P("sector", "term", None), P("sector", "term", None), P("sector", "term", None)),
        check_vma=False,
    )
```

```python
import functools
import math

import jax
import jax.numpy as jnp
from jax import lax
from jax.experimental import pallas as pl
from jax.experimental.pallas import tpu as pltpu
from jax.sharding import PartitionSpec as P

F32, BF16 = jnp.float32, jnp.bfloat16
MESH = pl.DeviceIdType.MESH
VMEM = pl.BlockSpec(memory_space=pltpu.VMEM)
HBM = pl.BlockSpec(memory_space=pltpu.HBM)
SLICES = 4
EARLY = SLICES - 1
VMEM_BYTES = 67043328


def split(x):
    high = x.astype(BF16)
    return high, (x - high.astype(F32)).astype(BF16)


def product(a_high, a_low, b_high, b_low):
    dot = functools.partial(jnp.dot, preferred_element_type=F32)
    return dot(a_high, b_high) + dot(a_high, b_low) + dot(a_low, b_high)


def stacked(a_high, a_low, b_high, b_low):
    dot = functools.partial(jnp.dot, preferred_element_type=F32)
    m = a_high.shape[0]
    both = dot(jnp.concatenate([a_high, a_low], axis=0), b_high)
    return both[:m] + both[m:] + dot(a_high, b_low)


def send(source, target, send_sem, recv_sem, **where):
    return pltpu.make_async_remote_copy(
        src_ref=source, dst_ref=target, send_sem=send_sem, recv_sem=recv_sem,
        device_id=where, device_id_type=MESH,
    )


def grid_of(terms):
    columns = max(d for d in range(1, math.isqrt(terms) + 1) if terms % d == 0)
    return terms // columns, columns


class Place:
    def __init__(self):
        self.terms, self.sectors = lax.axis_size("term"), lax.axis_size("sector")
        self.t, self.s = lax.axis_index("term"), lax.axis_index("sector")
        self.gy, self.gx = grid_of(self.terms)
        self.y, self.x = self.t // self.gx, lax.rem(self.t, self.gx)
        self.corners = [(dy, dx) for dy in range(1, self.gy) for dx in range(1, self.gx)]
        self.sides = [(dy, 0) for dy in range(1, self.gy)] + [(0, dx) for dx in range(1, self.gx)]
        self.own = [(0, 0)]

    def at(self, dy, dx):
        return lax.rem(self.y + dy, self.gy) * self.gx + lax.rem(self.x + dx, self.gx)

    def corner(self, dy, dx):
        return (dy - 1) * (self.gx - 1) + dx - 1

    def peers(self):
        terms = [lax.rem(self.t + k, self.terms) for k in range(self.terms)]
        sectors = [lax.rem(self.s + k, self.sectors) for k in range(self.sectors)]
        pairs = [{"term": t, "sector": s} for t in terms for s in sectors]
        return list(enumerate(pairs[1:]))


def barrier(here):
    sem = pltpu.get_barrier_semaphore()
    peers = here.peers()
    for _, where in peers:
        pl.semaphore_signal(sem, inc=1, device_id=where, device_id_type=MESH)
    return lambda: pl.semaphore_wait(sem, len(peers))


class Total:
    def __init__(self, here, refs):
        self.here = here
        self.sums, self.mine, self.theirs, self.send_sem, self.recv_sem = refs

    @staticmethod
    def scratch(values, peers):
        dma = pltpu.SemaphoreType.DMA
        return [pltpu.VMEM((values, 8, 128), F32), pltpu.VMEM((1, 128), F32), pltpu.VMEM((peers, 1, 128), F32),
                dma((1,)), dma((1,))]

    def all(self):
        return send(self.theirs, self.theirs, self.send_sem.at[0], self.recv_sem.at[0], **self.here.peers()[0][1])

    def begin(self):
        shape = (self.sums.shape[0], 128)
        diagonal = lax.broadcasted_iota(jnp.int32, shape, 0) == lax.broadcasted_iota(jnp.int32, shape, 1)
        line = jnp.sum(jnp.sum(self.sums[...], axis=1), axis=1, keepdims=True)
        self.mine[...] = jnp.sum(jnp.where(diagonal, line, 0.0), axis=0, keepdims=True)
        for k, where in self.here.peers():
            send(self.mine, self.theirs.at[k], self.send_sem.at[0], self.recv_sem.at[0], **where).start()

    def finish(self):
        self.all().wait_recv()
        total = self.mine[...] + jnp.sum(self.theirs[...], axis=0)
        return [total[:, n : n + 1] for n in range(self.sums.shape[0])]

    def drain(self):
        self.all().wait_send()


class Exchange:
    def __init__(self, here, refs, sems, tally=None):
        self.here, self.tally = here, tally
        self.whole, self.up_in, self.down_in, self.acc, self.da_in, self.db_in, self.x_in, self.y_in = refs
        (self.z_s, self.up_r, self.down_r, self.da_s, self.da_r, self.db_s, self.db_r,
         self.x_s, self.x_r, self.y_s, self.y_r) = sems
        self.rows, self.width = self.acc.shape[1], self.acc.shape[2]
        self.sub, self.half = self.rows // SLICES, self.width // 2

    @staticmethod
    def buffers(width, terms):
        rows, half = width // terms, width // 2
        gy, gx = grid_of(terms)
        whole = pltpu.VMEM((terms, rows, width), F32)
        corner = pltpu.VMEM(((gy - 1) * (gx - 1), rows, half), F32)
        return [pltpu.VMEM((3, terms, rows, width), F32), whole, whole, whole, corner, corner,
                pltpu.VMEM((gx - 1, rows, width), F32), pltpu.VMEM((gy - 1, rows, width), F32)]

    @staticmethod
    def semaphores(terms):
        gy, gx = grid_of(terms)
        dma, corners = pltpu.SemaphoreType.DMA, (gy - 1) * (gx - 1)
        return [dma((2,)), dma((SLICES, terms)), dma((SLICES, terms))] + [dma((corners,)), dma((SLICES, corners))] * 2 + [
            dma((gx - 1,)), dma((SLICES, gx - 1)), dma((gy - 1,)), dma((SLICES, gy - 1))]

    def part(self, i):
        return pl.ds(pl.multiple_of(i * self.sub, self.sub), self.sub)

    def upward(self, r, i):
        h = self.here
        return send(self.whole.at[2, r, self.part(i)], self.up_in.at[r, self.part(i)], self.z_s.at[1],
                    self.up_r.at[i, r], sector=lax.rem(h.s + 1, h.sectors))

    def downward(self, r, i):
        h = self.here
        return send(self.whole.at[0, r, self.part(i)], self.down_in.at[r, self.part(i)], self.z_s.at[0],
                    self.down_r.at[i, r], sector=lax.rem(h.s + h.sectors - 1, h.sectors))

    def corner_a(self, dy, dx, i):
        h, part, c = self.here, self.part(i), self.here.corner(dy, dx)
        return send(self.acc.at[h.at(dy, dx), part, : self.half], self.da_in.at[c, part],
                    self.da_s.at[c], self.da_r.at[i, c], term=h.at(0, dx))

    def corner_b(self, dy, dx, i):
        h, part, c = self.here, self.part(i), self.here.corner(dy, dx)
        return send(self.acc.at[h.at(dy, dx), part, self.half :], self.db_in.at[c, part],
                    self.db_s.at[c], self.db_r.at[i, c], term=h.at(dy, 0))

    def along_x(self, dx, i):
        h, part = self.here, self.part(i)
        return send(self.acc.at[h.at(0, dx), part], self.x_in.at[dx - 1, part], self.x_s.at[dx - 1], self.x_r.at[i, dx - 1],
                    term=h.at(0, dx))

    def along_y(self, dy, i):
        h, part = self.here, self.part(i)
        return send(self.acc.at[h.at(dy, 0), part], self.y_in.at[dy - 1, part], self.y_s.at[dy - 1], self.y_r.at[i, dy - 1],
                    term=h.at(dy, 0))

    def sectors_out(self, slabs, i):
        h = self.here
        for dy, dx in slabs:
            r = h.at(dy, dx)

            @pl.when(h.s + 1 < h.sectors)
            def _():
                self.upward(r, i).start()

            @pl.when(h.s > 0)
            def _():
                self.downward(r, i).start()

    def merge(self, r, i):
        h, part = self.here, self.part(i)
        self.acc[r, part] = self.whole[1, r, part]

        @pl.when(h.s > 0)
        def _():
            self.upward(r, i).wait_recv()
            self.acc[r, part] += self.up_in[r, part]

        @pl.when(h.s + 1 < h.sectors)
        def _():
            self.downward(r, i).wait_recv()
            self.acc[r, part] += self.down_in[r, part]

        if self.tally:
            self.tally(r, part, self.acc[r, part])

    def corners(self, i):
        h = self.here
        for dy in range(1, h.gy):
            for dx in range(1, h.gx):
                self.merge(h.at(dy, dx), i)
                self.corner_a(dy, dx, i).start()
                self.corner_b(dy, dx, i).start()

    def sides(self, i):
        h, part = self.here, self.part(i)
        for dy in range(1, h.gy):
            r = h.at(dy, 0)
            self.merge(r, i)
            for dx in range(1, h.gx):
                self.corner_a(dy, dx, i).wait_recv()
                self.acc[r, part, : self.half] += self.da_in[h.corner(dy, dx), part]
            self.along_y(dy, i).start()
        for dx in range(1, h.gx):
            r = h.at(0, dx)
            self.merge(r, i)
            for dy in range(1, h.gy):
                self.corner_b(dy, dx, i).wait_recv()
                self.acc[r, part, self.half :] += self.db_in[h.corner(dy, dx), part]
            self.along_x(dx, i).start()

    def own(self, i):
        h, part = self.here, self.part(i)
        total = self.acc[h.t, part]
        for dy in range(1, h.gy):
            self.along_y(dy, i).wait_recv()
            total += self.y_in[dy - 1, part]
        for dx in range(1, h.gx):
            self.along_x(dx, i).wait_recv()
            total += self.x_in[dx - 1, part]
        return total

    def drain(self):
        h = self.here

        def sent(source, target, sem):
            send(source, target, sem, self.up_r.at[0, 0], term=h.at(0, 1), sector=h.s).wait_send()

        @pl.when(h.s + 1 < h.sectors)
        def _():
            sent(self.whole.at[2], self.up_in, self.z_s.at[1])

        @pl.when(h.s > 0)
        def _():
            sent(self.whole.at[0], self.down_in, self.z_s.at[0])

        for dy, dx in h.corners:
            c = h.corner(dy, dx)
            sent(self.da_in.at[c], self.da_in.at[c], self.da_s.at[c])
            sent(self.db_in.at[c], self.db_in.at[c], self.db_s.at[c])
        for n in range(h.gx - 1):
            sent(self.x_in.at[n], self.x_in.at[n], self.x_s.at[n])
        for n in range(h.gy - 1):
            sent(self.y_in.at[n], self.y_in.at[n], self.y_s.at[n])


class Gather:
    def __init__(self, here, full, refs, pieces):
        self.here, self.full = here, full
        self.x_s, self.x_r, self.y_s, self.y_r, self.a_s, self.a_r, self.b_s, self.b_r = refs
        self.sub, self.half, self.pieces = full.shape[1] // SLICES, full.shape[2] // 2, pieces

    @staticmethod
    def scratch(terms, pieces):
        gy, gx = grid_of(terms)
        dma = pltpu.SemaphoreType.DMA
        corners = (gy - 1) * (gx - 1)
        return [dma((gx - 1,)), dma((pieces, gx - 1)), dma((gy - 1,)), dma((pieces, gy - 1))] + [
            dma((corners,)), dma((pieces, corners))] * 2

    def part(self, i):
        return pl.ds(pl.multiple_of(i * self.sub, self.sub), self.sub)

    def to_x(self, r, dx, i):
        ref = self.full.at[r, self.part(i)]
        return send(ref, ref, self.x_s.at[dx - 1], self.x_r.at[i, dx - 1], term=self.here.at(0, dx))

    def to_y(self, r, dy, i):
        ref = self.full.at[r, self.part(i)]
        return send(ref, ref, self.y_s.at[dy - 1], self.y_r.at[i, dy - 1], term=self.here.at(dy, 0))

    def relay_a(self, r, dy, dx, i):
        ref, c = self.full.at[r, self.part(i), : self.half], self.here.corner(dy, dx)
        return send(ref, ref, self.a_s.at[c], self.a_r.at[i, c], term=self.here.at(0, dx))

    def relay_b(self, r, dy, dx, i):
        ref, c = self.full.at[r, self.part(i), self.half :], self.here.corner(dy, dx)
        return send(ref, ref, self.b_s.at[c], self.b_r.at[i, c], term=self.here.at(dy, 0))

    def begin(self, i):
        h = self.here
        for dx in range(1, h.gx):
            self.to_x(h.t, dx, i).start()
        for dy in range(1, h.gy):
            self.to_y(h.t, dy, i).start()

    def relay(self, i):
        h = self.here
        for dx in range(1, h.gx):
            r = h.at(0, dx)
            self.to_x(r, h.gx - dx, i).wait_recv()
            for dy in range(1, h.gy):
                self.relay_b(r, dy, dx, i).start()
        for dy in range(1, h.gy):
            r = h.at(dy, 0)
            self.to_y(r, h.gy - dy, i).wait_recv()
            for dx in range(1, h.gx):
                self.relay_a(r, dy, dx, i).start()

    def finish(self, i):
        h = self.here
        for dy in range(1, h.gy):
            for dx in range(1, h.gx):
                self.relay_a(h.at(dy, h.gx - dx), dy, dx, i).wait_recv()
                self.relay_b(h.at(h.gy - dy, dx), dy, dx, i).wait_recv()

    def drain(self):
        h, all_rows = self.here, pl.ds(0, self.pieces * self.sub)

        def sent(ref, sem):
            send(ref, ref, sem, self.x_r.at[0, 0], term=h.at(0, 1)).wait_send()

        for n in range(h.gx - 1):
            sent(self.full.at[h.t, all_rows], self.x_s.at[n])
        for n in range(h.gy - 1):
            sent(self.full.at[h.t, all_rows], self.y_s.at[n])
        for dy, dx in h.corners:
            sent(self.full.at[h.at(dy, 0), all_rows, : self.half], self.a_s.at[h.corner(dy, dx)])
            sent(self.full.at[h.at(0, dx), all_rows, self.half :], self.b_s.at[h.corner(dy, dx)])


BUFFERS, SEMAPHORES, GATHER_REFS, TOTAL_REFS = 8, 11, 8, 5


def kernel(target_hbm, count_hbm, wave_hbm, precond_hbm, left_hbm, right_hbm, first_out, correction_out, second_out, *scratch):
    scratch = list(scratch)

    def take(n):
        refs = scratch[:n]
        del scratch[:n]
        return refs

    here = Place()
    buffers, more, sems = take(BUFFERS), take(BUFFERS), take(SEMAPHORES)

    def fold(x):
        x = jnp.sum(x.reshape(x.shape[0] // 8, 8, width), axis=0)
        return sum(x[:, c : c + 128] for c in range(0, width, 128))

    def tally(r, part, value):
        overlap.sums[0] += fold(wave[r, part] * value)

    first, second = Exchange(here, buffers, sems, tally), Exchange(here, more, sems)
    wave, precond, image, left, right, r_high, r_low, v_high, v_low, in_high, in_low, target, count = take(13)
    p_gather, f_gather = Gather(here, precond, take(GATHER_REFS), EARLY), Gather(here, image, take(GATHER_REFS), SLICES)
    overlap, share_total, (load,) = Total(here, take(TOTAL_REFS)), Total(here, take(TOTAL_REFS)), take(1)
    t, s, terms = here.t, here.s, here.terms
    slots, _, rows, width = left.shape
    sub = rows // SLICES

    order = here.corners + here.sides + here.own
    load_precond = pltpu.make_async_copy(precond_hbm, precond.at[t], load.at[0])
    load_wave = pltpu.make_async_copy(wave_hbm, wave, load.at[1])
    load_target = pltpu.make_async_copy(target_hbm, target, load.at[2])
    load_count = pltpu.make_async_copy(count_hbm, count, load.at[3])
    load_right = [pltpu.make_async_copy(right_hbm.at[j], right.at[j], load.at[4 + j]) for j in range(slots)]
    load_left = [pltpu.make_async_copy(left_hbm.at[:, here.at(*o)], left.at[:, here.at(*o)], load.at[4 + slots + n])
                 for n, o in enumerate(order)]
    corners = len(here.corners)
    for copy in [load_precond, load_wave, load_target, load_count] + load_left[:corners] + load_right + load_left[corners:]:
        copy.start()
    arrived = barrier(here)

    def split_rows(value, start, size):
        for r in range(terms):
            to = pl.ds(r * rows + start, size)
            v_high[to], v_low[to] = split(value(r, pl.ds(start, size)))

    def inner(slabs, part):
        stack = jnp.concatenate([left[j, here.at(*o), part] for j in range(slots) for o in slabs], axis=0)
        return split(product(*split(stack), v_high[...], v_low[...]))

    def chosen(j, p, tile):
        hit = jnp.logical_and(j < count[0, 0], target[0, j] - s + 1 == p)
        return jnp.where(hit, tile, 0.0)

    def outer(m):
        return stacked if m < 128 else product

    def compute(exchange, slabs, part, size):
        high, low = inner(slabs, part)
        m = len(slabs) * size
        tiles = [outer(m)(high[j * m : (j + 1) * m], low[j * m : (j + 1) * m], r_high[j], r_low[j]) for j in range(slots)]
        for n, o in enumerate(slabs):
            for p in range(3):
                exchange.whole[p, here.at(*o), part] = sum(
                    chosen(j, p, tiles[j][n * size : (n + 1) * size]) for j in range(slots))

    every = pl.ds(0, rows)

    def corners_first(exchange):
        part = pl.ds(0, rows // 2)
        m = corners * (rows // 2)
        with jax.named_scope("startv"):
            load_wave.wait()
            split_rows(lambda r, part: wave[r, part], 0, rows)
        with jax.named_scope("startl"):
            for copy in load_left[:corners]:
                copy.wait()
            in_high[...], in_low[...] = inner(here.corners, part)
        load_target.wait()
        load_count.wait()
        pairs = [range(j, min(j + 2, slots)) for j in range(0, slots, 2)]
        for pair in pairs:
            with jax.named_scope("startr"):
                for j in pair:
                    load_right[j].wait()
                tiles = {}
                for j in pair:
                    high, low = split(right[j])
                    r_high[j], r_low[j] = high, low
                    tiles[j] = outer(m)(in_high[j * m : (j + 1) * m], in_low[j * m : (j + 1) * m], high, low)
                for n, o in enumerate(here.corners):
                    for p in range(3):
                        rows_of = slice(n * (rows // 2), (n + 1) * (rows // 2))
                        piece = sum(chosen(j, p, tiles[j][rows_of]) for j in pair)
                        ref = exchange.whole.at[p, here.at(*o), part]
                        ref[...] = piece if pair == pairs[0] else ref[...] + piece

    def apply(exchange, begin, meanwhile):
        def half(h):
            return pl.ds(pl.multiple_of(h * (rows // 2), rows // 2), rows // 2)

        def half_out(slabs, h):
            for i in range(SLICES // 2):
                exchange.sectors_out(slabs, h * (SLICES // 2) + i)

        def corner_block(h):
            with jax.named_scope("CD"):
                compute(exchange, here.corners, half(h), rows // 2)
            half_out(here.corners, h)

        if begin:
            begin()
            half_out(here.corners, 0)
            corner_block(1)
        else:
            pl.loop(0, 2)(corner_block)

        @pl.loop(0, SLICES)
        def _(b):
            with jax.named_scope("C"):
                compute(exchange, here.sides, exchange.part(b), sub)
            exchange.sectors_out(here.sides, b)
            with jax.named_scope("p"):
                meanwhile(b)

            with jax.named_scope("Fd"):
                @pl.when(b < SLICES - 1)
                def _():
                    exchange.corners(b + b // 2)

                @pl.when(b == 1)
                def _():
                    exchange.corners(2)

        @pl.loop(0, 2)
        def _(h):
            with jax.named_scope("Fxy"):
                exchange.sides(h)
            with jax.named_scope("CO"):
                compute(exchange, here.own, half(h), rows // 2)
            half_out(here.own, h)

        @pl.loop(2, SLICES)
        def _(i):
            with jax.named_scope("Fxy"):
                exchange.sides(i)

    def first_begin():
        corners_first(first)
        for copy in load_left[corners:]:
            copy.wait()

    def first_done(i):
        part = first.part(i)
        f = first.own(i)
        first_out[part] = f
        image[t, part] = f

    with jax.named_scope("enter"):
        load_precond.wait()
        arrived()
        for i in range(EARLY):
            p_gather.begin(i)
    overlap.sums[0] = jnp.zeros((8, 128), F32)
    def relays(b):
        @pl.when(b < EARLY)
        def _():
            p_gather.relay(b)

    apply(first, first_begin, relays)

    with jax.named_scope("Fo"):
        for i in range(2):
            first.merge(t, i)
        first_done(0)
        f_gather.begin(0)
    with jax.named_scope("Mo"):
        for i in range(2, SLICES):
            first.merge(t, i)
        overlap.sums[1] = fold(wave[t] * wave[t])
        overlap.begin()
    with jax.named_scope("Fo"):
        for i in range(1, SLICES):
            first_done(i)
            if i < EARLY:
                f_gather.begin(i)
    with jax.named_scope("relay0"):
        for i in range(EARLY):
            p_gather.finish(i)
        f_gather.relay(0)
    with jax.named_scope("ray"):
        cross, norm = overlap.finish()
        rayleigh = cross / norm

    def raw(r, part):
        return precond[r, part] * (image[r, part] - rayleigh * wave[r, part])

    with jax.named_scope("raw"):
        for i in range(EARLY, SLICES):
            image[t, first.part(i)] = raw(t, first.part(i))
            f_gather.begin(i)
        share_total.sums[0] = jnp.zeros((8, 128), F32)
        for i in range(SLICES):
            part = first.part(i)
            own = raw(t, part) if i < EARLY else image[t, part]
            correction_out[part] = own
            share_total.sums[0] += fold(wave[t, part] * own)
        share_total.begin()
    with jax.named_scope("relay"):
        for i in range(1, SLICES):
            f_gather.relay(i)
    with jax.named_scope("share"):
        (dot,) = share_total.finish()
        share = dot / norm
    correction_out[...] -= share * wave[t]

    def corrected(r, part):
        return raw(r, part) - share * wave[r, part]

    for i in range(SLICES):
        with jax.named_scope("gfin"):
            f_gather.finish(i)
        with jax.named_scope("corr"):
            split_rows(corrected if i < EARLY else lambda r, part: image[r, part] - share * wave[r, part], i * sub, sub)

    first.drain()
    apply(second, None, lambda i: None)

    @pl.loop(0, SLICES)
    def _(i):
        with jax.named_scope("Fo"):
            second.merge(t, i)
            second_out[second.part(i)] = second.own(i)

    with jax.named_scope("drain"):
        for stream in (second, p_gather, f_gather, overlap, share_total):
            stream.drain()


def publish_kernel(*refs):
    ins, outs, sems = refs[:3], refs[3:6], refs[6]
    copies = [pltpu.make_async_copy(a, b, sems.at[n]) for n, (a, b) in enumerate(zip(ins, outs))]
    for copy in copies:
        copy.start()
    for copy in copies:
        copy.wait()


def per_device(wavefunction, precond, left_ops, right_ops, out_sector, live_counts):
    terms, sectors = lax.axis_size("term"), lax.axis_size("sector")
    width, slots = wavefunction.shape[1], left_ops.shape[1]
    rows = width // terms
    gy, gx = grid_of(terms)
    dma = pltpu.SemaphoreType.DMA
    slab = jax.ShapeDtypeStruct((rows, width), F32)
    block = pltpu.VMEM((terms, rows, width), F32)
    half = pltpu.VMEM((width, width), BF16)
    operators = pltpu.VMEM((slots, terms, rows, width), F32)
    halves = pltpu.VMEM((slots, width, width), BF16)
    inner = pltpu.VMEM((slots * (gy - 1) * (gx - 1) * (rows // 2), width), BF16)
    peers = terms * sectors - 1
    outs = pl.pallas_call(
        kernel,
        out_shape=(pltpu.VMEM((rows, width), F32),) * 3,
        in_specs=[HBM] * 6,
        out_specs=(VMEM,) * 3,
        scratch_shapes=Exchange.buffers(width, terms) * 2 + Exchange.semaphores(terms)
        + [block, block, block, operators, pltpu.VMEM((slots, width, width), F32), halves, halves, half, half, inner, inner,
           pltpu.SMEM(out_sector.shape, jnp.int32), pltpu.SMEM(live_counts.shape, jnp.int32)]
        + Gather.scratch(terms, EARLY) + Gather.scratch(terms, SLICES)
        + Total.scratch(2, peers) + Total.scratch(1, peers) + [dma((4 + slots + terms,))],
        compiler_params=pltpu.CompilerParams(collective_id=0, has_side_effects=True, vmem_limit_bytes=VMEM_BYTES - 3 * 4 * rows * width - (192 << 10)),
    )(out_sector, live_counts, wavefunction.reshape(terms, rows, width), precond[0],
      left_ops.reshape(slots, terms, rows, width), right_ops[0])
    outs = pl.pallas_call(
        publish_kernel,
        out_shape=(slab,) * 3,
        in_specs=[VMEM] * 3,
        out_specs=(HBM,) * 3,
        scratch_shapes=[dma((3,))],
        compiler_params=pltpu.CompilerParams(vmem_limit_bytes=1 << 20),
    )(*outs)
    return tuple(x[None] for x in outs)


def solution(mesh):
    placed = (
        P("sector", None, None),
        P("sector", "term", None),
        P("sector", "term", None, None),
        P("sector", "term", None, None),
        P("sector", "term"),
        P("sector", "term"),
    )
    return jax.shard_map(
        per_device,
        mesh=mesh,
        in_specs=placed,
        out_specs=(P("sector", "term", None), P("sector", "term", None), P("sector", "term", None)),
        check_vma=False,
    )
```

```python
import functools
import math

import jax
import jax.numpy as jnp
from jax import lax
from jax.experimental import pallas as pl
from jax.experimental.pallas import tpu as pltpu
from jax.sharding import PartitionSpec as P

F32, BF16 = jnp.float32, jnp.bfloat16
MESH = pl.DeviceIdType.MESH
VMEM = pl.BlockSpec(memory_space=pltpu.VMEM)
HBM = pl.BlockSpec(memory_space=pltpu.HBM)
SLICES = 4
EARLY = SLICES - 1
VMEM_BYTES = 67043328


def split(x):
    high = x.astype(BF16)
    return high, (x - high.astype(F32)).astype(BF16)


def product(a_high, a_low, b_high, b_low):
    dot = functools.partial(jnp.dot, preferred_element_type=F32)
    return dot(a_high, b_high) + dot(a_high, b_low) + dot(a_low, b_high)


def stacked(a_high, a_low, b_high, b_low):
    dot = functools.partial(jnp.dot, preferred_element_type=F32)
    m = a_high.shape[0]
    both = dot(jnp.concatenate([a_high, a_low], axis=0), b_high)
    return both[:m] + both[m:] + dot(a_high, b_low)


def send(source, target, send_sem, recv_sem, **where):
    return pltpu.make_async_remote_copy(
        src_ref=source, dst_ref=target, send_sem=send_sem, recv_sem=recv_sem,
        device_id=where, device_id_type=MESH,
    )


def grid_of(terms):
    columns = max(d for d in range(1, math.isqrt(terms) + 1) if terms % d == 0)
    return terms // columns, columns


class Place:
    def __init__(self):
        self.terms, self.sectors = lax.axis_size("term"), lax.axis_size("sector")
        self.t, self.s = lax.axis_index("term"), lax.axis_index("sector")
        self.gy, self.gx = grid_of(self.terms)
        self.y, self.x = self.t // self.gx, lax.rem(self.t, self.gx)
        self.corners = [(dy, dx) for dy in range(1, self.gy) for dx in range(1, self.gx)]
        self.sides = [(dy, 0) for dy in range(1, self.gy)] + [(0, dx) for dx in range(1, self.gx)]
        self.own = [(0, 0)]

    def at(self, dy, dx):
        return lax.rem(self.y + dy, self.gy) * self.gx + lax.rem(self.x + dx, self.gx)

    def corner(self, dy, dx):
        return (dy - 1) * (self.gx - 1) + dx - 1

    def peers(self):
        terms = [lax.rem(self.t + k, self.terms) for k in range(self.terms)]
        sectors = [lax.rem(self.s + k, self.sectors) for k in range(self.sectors)]
        pairs = [{"term": t, "sector": s} for t in terms for s in sectors]
        return list(enumerate(pairs[1:]))


def barrier(here):
    sem = pltpu.get_barrier_semaphore()
    peers = here.peers()
    for _, where in peers:
        pl.semaphore_signal(sem, inc=1, device_id=where, device_id_type=MESH)
    return lambda: pl.semaphore_wait(sem, len(peers))


class Total:
    def __init__(self, here, refs):
        self.here = here
        self.sums, self.mine, self.theirs, self.send_sem, self.recv_sem = refs

    @staticmethod
    def scratch(values, peers):
        dma = pltpu.SemaphoreType.DMA
        return [pltpu.VMEM((values, 8, 128), F32), pltpu.VMEM((1, 128), F32), pltpu.VMEM((peers, 1, 128), F32),
                dma((1,)), dma((1,))]

    def all(self):
        return send(self.theirs, self.theirs, self.send_sem.at[0], self.recv_sem.at[0], **self.here.peers()[0][1])

    def begin(self):
        shape = (self.sums.shape[0], 128)
        diagonal = lax.broadcasted_iota(jnp.int32, shape, 0) == lax.broadcasted_iota(jnp.int32, shape, 1)
        line = jnp.sum(jnp.sum(self.sums[...], axis=1), axis=1, keepdims=True)
        self.mine[...] = jnp.sum(jnp.where(diagonal, line, 0.0), axis=0, keepdims=True)
        for k, where in self.here.peers():
            send(self.mine, self.theirs.at[k], self.send_sem.at[0], self.recv_sem.at[0], **where).start()

    def finish(self):
        self.all().wait_recv()
        total = self.mine[...] + jnp.sum(self.theirs[...], axis=0)
        return [total[:, n : n + 1] for n in range(self.sums.shape[0])]

    def drain(self):
        self.all().wait_send()


class Exchange:
    def __init__(self, here, refs, sems, tally=None):
        self.here, self.tally = here, tally
        self.whole, self.up_in, self.down_in, self.acc, self.da_in, self.db_in, self.x_in, self.y_in = refs
        (self.z_s, self.up_r, self.down_r, self.da_s, self.da_r, self.db_s, self.db_r,
         self.x_s, self.x_r, self.y_s, self.y_r) = sems
        self.rows, self.width = self.acc.shape[1], self.acc.shape[2]
        self.sub, self.half = self.rows // SLICES, self.width // 2

    @staticmethod
    def buffers(width, terms):
        rows, half = width // terms, width // 2
        gy, gx = grid_of(terms)
        whole = pltpu.VMEM((terms, rows, width), F32)
        corner = pltpu.VMEM(((gy - 1) * (gx - 1), rows, half), F32)
        return [pltpu.VMEM((3, terms, rows, width), F32), whole, whole, whole, corner, corner,
                pltpu.VMEM((gx - 1, rows, width), F32), pltpu.VMEM((gy - 1, rows, width), F32)]

    @staticmethod
    def semaphores(terms):
        gy, gx = grid_of(terms)
        dma, corners = pltpu.SemaphoreType.DMA, (gy - 1) * (gx - 1)
        return [dma((2,)), dma((SLICES, terms)), dma((SLICES, terms))] + [dma((corners,)), dma((SLICES, corners))] * 2 + [
            dma((gx - 1,)), dma((SLICES, gx - 1)), dma((gy - 1,)), dma((SLICES, gy - 1))]

    def part(self, i):
        return pl.ds(pl.multiple_of(i * self.sub, self.sub), self.sub)

    def upward(self, r, i):
        h = self.here
        return send(self.whole.at[2, r, self.part(i)], self.up_in.at[r, self.part(i)], self.z_s.at[1],
                    self.up_r.at[i, r], sector=lax.rem(h.s + 1, h.sectors))

    def downward(self, r, i):
        h = self.here
        return send(self.whole.at[0, r, self.part(i)], self.down_in.at[r, self.part(i)], self.z_s.at[0],
                    self.down_r.at[i, r], sector=lax.rem(h.s + h.sectors - 1, h.sectors))

    def corner_a(self, dy, dx, i):
        h, part, c = self.here, self.part(i), self.here.corner(dy, dx)
        return send(self.acc.at[h.at(dy, dx), part, : self.half], self.da_in.at[c, part],
                    self.da_s.at[c], self.da_r.at[i, c], term=h.at(0, dx))

    def corner_b(self, dy, dx, i):
        h, part, c = self.here, self.part(i), self.here.corner(dy, dx)
        return send(self.acc.at[h.at(dy, dx), part, self.half :], self.db_in.at[c, part],
                    self.db_s.at[c], self.db_r.at[i, c], term=h.at(dy, 0))

    def along_x(self, dx, i):
        h, part = self.here, self.part(i)
        return send(self.acc.at[h.at(0, dx), part], self.x_in.at[dx - 1, part], self.x_s.at[dx - 1], self.x_r.at[i, dx - 1],
                    term=h.at(0, dx))

    def along_y(self, dy, i):
        h, part = self.here, self.part(i)
        return send(self.acc.at[h.at(dy, 0), part], self.y_in.at[dy - 1, part], self.y_s.at[dy - 1], self.y_r.at[i, dy - 1],
                    term=h.at(dy, 0))

    def sectors_out(self, slabs, i):
        h = self.here
        for dy, dx in slabs:
            r = h.at(dy, dx)

            @pl.when(h.s + 1 < h.sectors)
            def _():
                self.upward(r, i).start()

            @pl.when(h.s > 0)
            def _():
                self.downward(r, i).start()

    def merge(self, r, i):
        h, part = self.here, self.part(i)
        self.acc[r, part] = self.whole[1, r, part]

        @pl.when(h.s > 0)
        def _():
            self.upward(r, i).wait_recv()
            self.acc[r, part] += self.up_in[r, part]

        @pl.when(h.s + 1 < h.sectors)
        def _():
            self.downward(r, i).wait_recv()
            self.acc[r, part] += self.down_in[r, part]

        if self.tally:
            self.tally(r, part, self.acc[r, part])

    def corners(self, i):
        h = self.here
        for dy in range(1, h.gy):
            for dx in range(1, h.gx):
                self.merge(h.at(dy, dx), i)
                self.corner_a(dy, dx, i).start()
                self.corner_b(dy, dx, i).start()

    def sides(self, i):
        h, part = self.here, self.part(i)
        for dy in range(1, h.gy):
            r = h.at(dy, 0)
            self.merge(r, i)
            for dx in range(1, h.gx):
                self.corner_a(dy, dx, i).wait_recv()
                self.acc[r, part, : self.half] += self.da_in[h.corner(dy, dx), part]
            self.along_y(dy, i).start()
        for dx in range(1, h.gx):
            r = h.at(0, dx)
            self.merge(r, i)
            for dy in range(1, h.gy):
                self.corner_b(dy, dx, i).wait_recv()
                self.acc[r, part, self.half :] += self.db_in[h.corner(dy, dx), part]
            self.along_x(dx, i).start()

    def own(self, i):
        h, part = self.here, self.part(i)
        total = self.acc[h.t, part]
        for dy in range(1, h.gy):
            self.along_y(dy, i).wait_recv()
            total += self.y_in[dy - 1, part]
        for dx in range(1, h.gx):
            self.along_x(dx, i).wait_recv()
            total += self.x_in[dx - 1, part]
        return total

    def drain(self):
        h = self.here

        def sent(source, target, sem):
            send(source, target, sem, self.up_r.at[0, 0], term=h.at(0, 1), sector=h.s).wait_send()

        @pl.when(h.s + 1 < h.sectors)
        def _():
            sent(self.whole.at[2], self.up_in, self.z_s.at[1])

        @pl.when(h.s > 0)
        def _():
            sent(self.whole.at[0], self.down_in, self.z_s.at[0])

        for dy, dx in h.corners:
            c = h.corner(dy, dx)
            sent(self.da_in.at[c], self.da_in.at[c], self.da_s.at[c])
            sent(self.db_in.at[c], self.db_in.at[c], self.db_s.at[c])
        for n in range(h.gx - 1):
            sent(self.x_in.at[n], self.x_in.at[n], self.x_s.at[n])
        for n in range(h.gy - 1):
            sent(self.y_in.at[n], self.y_in.at[n], self.y_s.at[n])


class Gather:
    def __init__(self, here, full, refs, pieces):
        self.here, self.full = here, full
        self.x_s, self.x_r, self.y_s, self.y_r, self.a_s, self.a_r, self.b_s, self.b_r, self.c_s, self.c_r = refs
        self.sub, self.half, self.pieces = full.shape[1] // SLICES, full.shape[2] // 2, pieces

    @staticmethod
    def scratch(terms, pieces):
        gy, gx = grid_of(terms)
        dma = pltpu.SemaphoreType.DMA
        corners = (gy - 1) * (gx - 1)
        return [dma((gx - 1,)), dma((pieces, gx - 1)), dma((gy - 1,)), dma((pieces, gy - 1))] + [
            dma((corners,)), dma((pieces, corners))] * 2 + [dma((corners,)), dma((corners,))]

    def part(self, i):
        return pl.ds(pl.multiple_of(i * self.sub, self.sub), self.sub)

    def to_x(self, r, dx, i):
        ref = self.full.at[r, self.part(i)]
        return send(ref, ref, self.x_s.at[dx - 1], self.x_r.at[i, dx - 1], term=self.here.at(0, dx))

    def to_y(self, r, dy, i):
        ref = self.full.at[r, self.part(i)]
        return send(ref, ref, self.y_s.at[dy - 1], self.y_r.at[i, dy - 1], term=self.here.at(dy, 0))

    def relay_a(self, r, dy, dx, i):
        ref, c = self.full.at[r, self.part(i), : self.half], self.here.corner(dy, dx)
        return send(ref, ref, self.a_s.at[c], self.a_r.at[i, c], term=self.here.at(0, dx))

    def relay_b(self, r, dy, dx, i):
        ref, c = self.full.at[r, self.part(i), self.half :], self.here.corner(dy, dx)
        return send(ref, ref, self.b_s.at[c], self.b_r.at[i, c], term=self.here.at(dy, 0))

    def to_corner(self, r, dy, dx, i):
        ref, c = self.full.at[r, self.part(i)], self.here.corner(dy, dx)
        return send(ref, ref, self.c_s.at[c], self.c_r.at[c], term=self.here.at(dy, dx))

    def begin_direct(self, i):
        for dy, dx in self.here.corners:
            self.to_corner(self.here.t, dy, dx, i).start()
        self.begin(i)

    def finish_direct(self, i):
        h = self.here
        for dx in range(1, h.gx):
            self.to_x(h.at(0, dx), h.gx - dx, i).wait_recv()
        for dy in range(1, h.gy):
            self.to_y(h.at(dy, 0), h.gy - dy, i).wait_recv()
        for dy, dx in h.corners:
            self.to_corner(h.at(h.gy - dy, h.gx - dx), dy, dx, i).wait_recv()

    def drain_direct(self, i):
        for dy, dx in self.here.corners:
            self.to_corner(self.here.t, dy, dx, i).wait_send()

    def begin(self, i):
        h = self.here
        for dx in range(1, h.gx):
            self.to_x(h.t, dx, i).start()
        for dy in range(1, h.gy):
            self.to_y(h.t, dy, i).start()

    def relay(self, i):
        h = self.here
        for dx in range(1, h.gx):
            r = h.at(0, dx)
            self.to_x(r, h.gx - dx, i).wait_recv()
            for dy in range(1, h.gy):
                self.relay_b(r, dy, dx, i).start()
        for dy in range(1, h.gy):
            r = h.at(dy, 0)
            self.to_y(r, h.gy - dy, i).wait_recv()
            for dx in range(1, h.gx):
                self.relay_a(r, dy, dx, i).start()

    def finish(self, i):
        h = self.here
        for dy in range(1, h.gy):
            for dx in range(1, h.gx):
                self.relay_a(h.at(dy, h.gx - dx), dy, dx, i).wait_recv()
                self.relay_b(h.at(h.gy - dy, dx), dy, dx, i).wait_recv()

    def drain(self):
        h, all_rows = self.here, pl.ds(0, self.pieces * self.sub)
        relayed = pl.ds(0, EARLY * self.sub)

        def sent(ref, sem):
            send(ref, ref, sem, self.x_r.at[0, 0], term=h.at(0, 1)).wait_send()

        for n in range(h.gx - 1):
            sent(self.full.at[h.t, all_rows], self.x_s.at[n])
        for n in range(h.gy - 1):
            sent(self.full.at[h.t, all_rows], self.y_s.at[n])
        for dy, dx in h.corners:
            sent(self.full.at[h.at(dy, 0), relayed, : self.half], self.a_s.at[h.corner(dy, dx)])
            sent(self.full.at[h.at(0, dx), relayed, self.half :], self.b_s.at[h.corner(dy, dx)])


BUFFERS, SEMAPHORES, GATHER_REFS, TOTAL_REFS = 8, 11, 10, 5


def kernel(target_hbm, count_hbm, wave_hbm, precond_hbm, left_hbm, right_hbm, first_out, correction_out, second_out, *scratch):
    scratch = list(scratch)

    def take(n):
        refs = scratch[:n]
        del scratch[:n]
        return refs

    here = Place()
    buffers, more, sems = take(BUFFERS), take(BUFFERS), take(SEMAPHORES)

    def fold(x):
        x = jnp.sum(x.reshape(x.shape[0] // 8, 8, width), axis=0)
        return sum(x[:, c : c + 128] for c in range(0, width, 128))

    def tally(r, part, value):
        overlap.sums[0] += fold(wave[r, part] * value)

    first, second = Exchange(here, buffers, sems, tally), Exchange(here, more, sems)
    wave, precond, image, left, right, r_high, r_low, v_high, v_low, in_high, in_low, target, count = take(13)
    p_gather, f_gather = Gather(here, precond, take(GATHER_REFS), EARLY), Gather(here, image, take(GATHER_REFS), SLICES)
    overlap, share_total, (load,) = Total(here, take(TOTAL_REFS)), Total(here, take(TOTAL_REFS)), take(1)
    t, s, terms = here.t, here.s, here.terms
    slots, _, rows, width = left.shape
    sub = rows // SLICES

    order = here.corners + here.sides + here.own
    load_precond = pltpu.make_async_copy(precond_hbm, precond.at[t], load.at[0])
    load_wave = pltpu.make_async_copy(wave_hbm, wave, load.at[1])
    load_target = pltpu.make_async_copy(target_hbm, target, load.at[2])
    load_count = pltpu.make_async_copy(count_hbm, count, load.at[3])
    load_right = [pltpu.make_async_copy(right_hbm.at[j], right.at[j], load.at[4 + j]) for j in range(slots)]
    load_left = [pltpu.make_async_copy(left_hbm.at[:, here.at(*o)], left.at[:, here.at(*o)], load.at[4 + slots + n])
                 for n, o in enumerate(order)]
    corners = len(here.corners)
    for copy in [load_precond, load_wave, load_target, load_count] + load_left[:corners] + load_right + load_left[corners:]:
        copy.start()
    arrived = barrier(here)

    def split_rows(value, start, size):
        for r in range(terms):
            to = pl.ds(r * rows + start, size)
            v_high[to], v_low[to] = split(value(r, pl.ds(start, size)))

    def inner(slabs, part):
        stack = jnp.concatenate([left[j, here.at(*o), part] for j in range(slots) for o in slabs], axis=0)
        return split(product(*split(stack), v_high[...], v_low[...]))

    def chosen(j, p, tile):
        hit = jnp.logical_and(j < count[0, 0], target[0, j] - s + 1 == p)
        return jnp.where(hit, tile, 0.0)

    def outer(m):
        return stacked if m < 128 else product

    def compute(exchange, slabs, part, size):
        high, low = inner(slabs, part)
        m = len(slabs) * size
        tiles = [outer(m)(high[j * m : (j + 1) * m], low[j * m : (j + 1) * m], r_high[j], r_low[j]) for j in range(slots)]
        for n, o in enumerate(slabs):
            for p in range(3):
                exchange.whole[p, here.at(*o), part] = sum(
                    chosen(j, p, tiles[j][n * size : (n + 1) * size]) for j in range(slots))

    every = pl.ds(0, rows)

    def corners_first(exchange):
        part = pl.ds(0, rows // 2)
        m = corners * (rows // 2)
        with jax.named_scope("startv"):
            load_wave.wait()
            split_rows(lambda r, part: wave[r, part], 0, rows)
        with jax.named_scope("startl"):
            for copy in load_left[:corners]:
                copy.wait()
            in_high[...], in_low[...] = inner(here.corners, part)
        load_target.wait()
        load_count.wait()
        pairs = [range(j, min(j + 2, slots)) for j in range(0, slots, 2)]
        for pair in pairs:
            with jax.named_scope("startr"):
                for j in pair:
                    load_right[j].wait()
                tiles = {}
                for j in pair:
                    high, low = split(right[j])
                    r_high[j], r_low[j] = high, low
                    tiles[j] = outer(m)(in_high[j * m : (j + 1) * m], in_low[j * m : (j + 1) * m], high, low)
                for n, o in enumerate(here.corners):
                    for p in range(3):
                        rows_of = slice(n * (rows // 2), (n + 1) * (rows // 2))
                        piece = sum(chosen(j, p, tiles[j][rows_of]) for j in pair)
                        ref = exchange.whole.at[p, here.at(*o), part]
                        ref[...] = piece if pair == pairs[0] else ref[...] + piece

    def apply(exchange, begin, meanwhile):
        def half(h):
            return pl.ds(pl.multiple_of(h * (rows // 2), rows // 2), rows // 2)

        def half_out(slabs, h):
            for i in range(SLICES // 2):
                exchange.sectors_out(slabs, h * (SLICES // 2) + i)

        def corner_block(h):
            with jax.named_scope("CD"):
                compute(exchange, here.corners, half(h), rows // 2)
            half_out(here.corners, h)

        if begin:
            begin()
            half_out(here.corners, 0)
            for i in range(EARLY):
                p_gather.begin(i)
            corner_block(1)
        else:
            pl.loop(0, 2)(corner_block)

        if begin:
            @pl.loop(0, SLICES)
            def _(b):
                with jax.named_scope("C"):
                    compute(exchange, here.sides, exchange.part(b), sub)
                exchange.sectors_out(here.sides, b)
                with jax.named_scope("p"):
                    meanwhile(b)

                with jax.named_scope("Fd"):
                    @pl.when(b < SLICES - 1)
                    def _():
                        exchange.corners(b + b // 2)

                    @pl.when(b == 1)
                    def _():
                        exchange.corners(2)
        else:
            @pl.loop(0, 2)
            def _(h):
                with jax.named_scope("C"):
                    compute(exchange, here.sides, half(h), rows // 2)
                half_out(here.sides, h)
                with jax.named_scope("Fd"):
                    for i in range(SLICES // 2):
                        exchange.corners(h * (SLICES // 2) + i)

        @pl.loop(0, 2)
        def _(h):
            with jax.named_scope("Fxy"):
                exchange.sides(h)
            with jax.named_scope("CO"):
                compute(exchange, here.own, half(h), rows // 2)
            half_out(here.own, h)

        @pl.loop(2, SLICES)
        def _(i):
            with jax.named_scope("Fxy"):
                exchange.sides(i)

    def first_begin():
        corners_first(first)
        with jax.named_scope("enter"):
            load_precond.wait()
            arrived()
        for copy in load_left[corners:]:
            copy.wait()

    def first_done(i):
        part = first.part(i)
        f = first.own(i)
        first_out[part] = f
        image[t, part] = f

    overlap.sums[0] = jnp.zeros((8, 128), F32)
    def relays(b):
        @pl.when(jnp.logical_and(b >= 1, b <= EARLY))
        def _():
            p_gather.relay(b - 1)

    apply(first, first_begin, relays)

    with jax.named_scope("Fo"):
        for i in range(2):
            first.merge(t, i)
        first_done(0)
        f_gather.begin(0)
    with jax.named_scope("Mo"):
        for i in range(2, SLICES):
            first.merge(t, i)
        overlap.sums[1] = fold(wave[t] * wave[t])
        overlap.begin()
    with jax.named_scope("Fo"):
        for i in range(1, SLICES):
            first_done(i)
            if i < EARLY:
                f_gather.begin(i)
    with jax.named_scope("relay0"):
        for i in range(EARLY):
            p_gather.finish(i)
        f_gather.relay(0)
    with jax.named_scope("ray"):
        cross, norm = overlap.finish()
        rayleigh = cross / norm

    def raw(r, part):
        return precond[r, part] * (image[r, part] - rayleigh * wave[r, part])

    with jax.named_scope("raw"):
        for i in range(EARLY, SLICES):
            image[t, first.part(i)] = raw(t, first.part(i))
        share_total.sums[0] = jnp.zeros((8, 128), F32)
        for i in range(SLICES):
            part = first.part(i)
            own = raw(t, part) if i < EARLY else image[t, part]
            correction_out[part] = own
            share_total.sums[0] += fold(wave[t, part] * own)
        share_total.begin()
        for i in range(EARLY, SLICES):
            f_gather.begin_direct(i)
    with jax.named_scope("relay"):
        for i in range(1, EARLY):
            f_gather.relay(i)
    with jax.named_scope("share"):
        (dot,) = share_total.finish()
        share = dot / norm
    correction_out[...] -= share * wave[t]

    def corrected(r, part):
        return raw(r, part) - share * wave[r, part]

    for i in range(SLICES):
        with jax.named_scope("gfin"):
            if i < EARLY:
                f_gather.finish(i)
            else:
                f_gather.finish_direct(i)
        with jax.named_scope("corr"):
            split_rows(corrected if i < EARLY else lambda r, part: image[r, part] - share * wave[r, part], i * sub, sub)

    first.drain()
    apply(second, None, lambda i: None)

    @pl.loop(0, SLICES)
    def _(i):
        with jax.named_scope("Fo"):
            second.merge(t, i)
            second_out[second.part(i)] = second.own(i)

    with jax.named_scope("drain"):
        for stream in (second, p_gather, f_gather, overlap, share_total):
            stream.drain()
        f_gather.drain_direct(EARLY)


def publish_kernel(*refs):
    ins, outs, sems = refs[:3], refs[3:6], refs[6]
    copies = [pltpu.make_async_copy(a, b, sems.at[n]) for n, (a, b) in enumerate(zip(ins, outs))]
    for copy in copies:
        copy.start()
    for copy in copies:
        copy.wait()


def per_device(wavefunction, precond, left_ops, right_ops, out_sector, live_counts):
    terms, sectors = lax.axis_size("term"), lax.axis_size("sector")
    width, slots = wavefunction.shape[1], left_ops.shape[1]
    rows = width // terms
    gy, gx = grid_of(terms)
    dma = pltpu.SemaphoreType.DMA
    slab = jax.ShapeDtypeStruct((rows, width), F32)
    block = pltpu.VMEM((terms, rows, width), F32)
    half = pltpu.VMEM((width, width), BF16)
    operators = pltpu.VMEM((slots, terms, rows, width), F32)
    halves = pltpu.VMEM((slots, width, width), BF16)
    inner = pltpu.VMEM((slots * (gy - 1) * (gx - 1) * (rows // 2), width), BF16)
    peers = terms * sectors - 1
    outs = pl.pallas_call(
        kernel,
        out_shape=(pltpu.VMEM((rows, width), F32),) * 3,
        in_specs=[HBM] * 6,
        out_specs=(VMEM,) * 3,
        scratch_shapes=Exchange.buffers(width, terms) * 2 + Exchange.semaphores(terms)
        + [block, block, block, operators, pltpu.VMEM((slots, width, width), F32), halves, halves, half, half, inner, inner,
           pltpu.SMEM(out_sector.shape, jnp.int32), pltpu.SMEM(live_counts.shape, jnp.int32)]
        + Gather.scratch(terms, EARLY) + Gather.scratch(terms, SLICES)
        + Total.scratch(2, peers) + Total.scratch(1, peers) + [dma((4 + slots + terms,))],
        compiler_params=pltpu.CompilerParams(collective_id=0, has_side_effects=True, vmem_limit_bytes=VMEM_BYTES - 3 * 4 * rows * width - (192 << 10)),
    )(out_sector, live_counts, wavefunction.reshape(terms, rows, width), precond[0],
      left_ops.reshape(slots, terms, rows, width), right_ops[0])
    outs = pl.pallas_call(
        publish_kernel,
        out_shape=(slab,) * 3,
        in_specs=[VMEM] * 3,
        out_specs=(HBM,) * 3,
        scratch_shapes=[dma((3,))],
        compiler_params=pltpu.CompilerParams(vmem_limit_bytes=1 << 20),
    )(*outs)
    return tuple(x[None] for x in outs)


def solution(mesh):
    placed = (
        P("sector", None, None),
        P("sector", "term", None),
        P("sector", "term", None, None),
        P("sector", "term", None, None),
        P("sector", "term"),
        P("sector", "term"),
    )
    return jax.shard_map(
        per_device,
        mesh=mesh,
        in_specs=placed,
        out_specs=(P("sector", "term", None), P("sector", "term", None), P("sector", "term", None)),
        check_vma=False,
    )
```

```python
import functools
import math

import jax
import jax.numpy as jnp
from jax import lax
from jax.experimental import pallas as pl
from jax.experimental.pallas import tpu as pltpu
from jax.sharding import PartitionSpec as P

F32, BF16 = jnp.float32, jnp.bfloat16
MESH = pl.DeviceIdType.MESH
VMEM = pl.BlockSpec(memory_space=pltpu.VMEM)
HBM = pl.BlockSpec(memory_space=pltpu.HBM)
SLICES = 4
EARLY = SLICES - 1
VMEM_BYTES = 67043328


def split(x):
    high = x.astype(BF16)
    return high, (x - high.astype(F32)).astype(BF16)


def product(a_high, a_low, b_high, b_low):
    dot = functools.partial(jnp.dot, preferred_element_type=F32)
    return dot(a_high, b_high) + dot(a_high, b_low) + dot(a_low, b_high)


def stacked(a_high, a_low, b_high, b_low):
    dot = functools.partial(jnp.dot, preferred_element_type=F32)
    m = a_high.shape[0]
    both = dot(jnp.concatenate([a_high, a_low], axis=0), b_high)
    return both[:m] + both[m:] + dot(a_high, b_low)


def send(source, target, send_sem, recv_sem, **where):
    return pltpu.make_async_remote_copy(
        src_ref=source, dst_ref=target, send_sem=send_sem, recv_sem=recv_sem,
        device_id=where, device_id_type=MESH,
    )


def grid_of(terms):
    columns = max(d for d in range(1, math.isqrt(terms) + 1) if terms % d == 0)
    return terms // columns, columns


class Place:
    def __init__(self):
        self.terms, self.sectors = lax.axis_size("term"), lax.axis_size("sector")
        self.t, self.s = lax.axis_index("term"), lax.axis_index("sector")
        self.gy, self.gx = grid_of(self.terms)
        self.y, self.x = self.t // self.gx, lax.rem(self.t, self.gx)
        self.corners = [(dy, dx) for dy in range(1, self.gy) for dx in range(1, self.gx)]
        self.sides = [(dy, 0) for dy in range(1, self.gy)] + [(0, dx) for dx in range(1, self.gx)]
        self.own = [(0, 0)]

    def at(self, dy, dx):
        return lax.rem(self.y + dy, self.gy) * self.gx + lax.rem(self.x + dx, self.gx)

    def corner(self, dy, dx):
        return (dy - 1) * (self.gx - 1) + dx - 1

    def peers(self):
        terms = [lax.rem(self.t + k, self.terms) for k in range(self.terms)]
        sectors = [lax.rem(self.s + k, self.sectors) for k in range(self.sectors)]
        pairs = [{"term": t, "sector": s} for t in terms for s in sectors]
        return list(enumerate(pairs[1:]))


def barrier(here):
    sem = pltpu.get_barrier_semaphore()
    peers = here.peers()
    for _, where in peers:
        pl.semaphore_signal(sem, inc=1, device_id=where, device_id_type=MESH)
    return lambda: pl.semaphore_wait(sem, len(peers))


class Total:
    def __init__(self, here, refs):
        self.here = here
        self.sums, self.mine, self.theirs, self.send_sem, self.recv_sem = refs

    @staticmethod
    def scratch(values, peers):
        dma = pltpu.SemaphoreType.DMA
        return [pltpu.VMEM((values, 8, 128), F32), pltpu.VMEM((1, 128), F32), pltpu.VMEM((peers, 1, 128), F32),
                dma((1,)), dma((1,))]

    def all(self):
        return send(self.theirs, self.theirs, self.send_sem.at[0], self.recv_sem.at[0], **self.here.peers()[0][1])

    def begin(self):
        shape = (self.sums.shape[0], 128)
        diagonal = lax.broadcasted_iota(jnp.int32, shape, 0) == lax.broadcasted_iota(jnp.int32, shape, 1)
        line = jnp.sum(jnp.sum(self.sums[...], axis=1), axis=1, keepdims=True)
        self.mine[...] = jnp.sum(jnp.where(diagonal, line, 0.0), axis=0, keepdims=True)
        for k, where in self.here.peers():
            send(self.mine, self.theirs.at[k], self.send_sem.at[0], self.recv_sem.at[0], **where).start()

    def finish(self):
        self.all().wait_recv()
        total = self.mine[...] + jnp.sum(self.theirs[...], axis=0)
        return [total[:, n : n + 1] for n in range(self.sums.shape[0])]

    def drain(self):
        self.all().wait_send()


class Exchange:
    def __init__(self, here, refs, sems, tally=None):
        self.here, self.tally = here, tally
        self.whole, self.up_in, self.down_in, self.acc, self.da_in, self.db_in, self.x_in, self.y_in = refs
        (self.z_s, self.up_r, self.down_r, self.da_s, self.da_r, self.db_s, self.db_r,
         self.x_s, self.x_r, self.y_s, self.y_r) = sems
        self.rows, self.width = self.acc.shape[1], self.acc.shape[2]
        self.sub, self.half = self.rows // SLICES, self.width // 2

    @staticmethod
    def buffers(width, terms):
        rows, half = width // terms, width // 2
        gy, gx = grid_of(terms)
        whole = pltpu.VMEM((terms, rows, width), F32)
        corner = pltpu.VMEM(((gy - 1) * (gx - 1), rows, half), F32)
        return [pltpu.VMEM((3, terms, rows, width), F32), whole, whole, whole, corner, corner,
                pltpu.VMEM((gx - 1, rows, width), F32), pltpu.VMEM((gy - 1, rows, width), F32)]

    @staticmethod
    def semaphores(terms):
        gy, gx = grid_of(terms)
        dma, corners = pltpu.SemaphoreType.DMA, (gy - 1) * (gx - 1)
        return [dma((2,)), dma((SLICES, terms)), dma((SLICES, terms))] + [dma((corners,)), dma((SLICES, corners))] * 2 + [
            dma((gx - 1,)), dma((SLICES, gx - 1)), dma((gy - 1,)), dma((SLICES, gy - 1))]

    def part(self, i):
        return pl.ds(pl.multiple_of(i * self.sub, self.sub), self.sub)

    def upward(self, r, i):
        h = self.here
        return send(self.whole.at[2, r, self.part(i)], self.up_in.at[r, self.part(i)], self.z_s.at[1],
                    self.up_r.at[i, r], sector=lax.rem(h.s + 1, h.sectors))

    def downward(self, r, i):
        h = self.here
        return send(self.whole.at[0, r, self.part(i)], self.down_in.at[r, self.part(i)], self.z_s.at[0],
                    self.down_r.at[i, r], sector=lax.rem(h.s + h.sectors - 1, h.sectors))

    def corner_a(self, dy, dx, i):
        h, part, c = self.here, self.part(i), self.here.corner(dy, dx)
        return send(self.acc.at[h.at(dy, dx), part, : self.half], self.da_in.at[c, part],
                    self.da_s.at[c], self.da_r.at[i, c], term=h.at(0, dx))

    def corner_b(self, dy, dx, i):
        h, part, c = self.here, self.part(i), self.here.corner(dy, dx)
        return send(self.acc.at[h.at(dy, dx), part, self.half :], self.db_in.at[c, part],
                    self.db_s.at[c], self.db_r.at[i, c], term=h.at(dy, 0))

    def along_x(self, dx, i):
        h, part = self.here, self.part(i)
        return send(self.acc.at[h.at(0, dx), part], self.x_in.at[dx - 1, part], self.x_s.at[dx - 1], self.x_r.at[i, dx - 1],
                    term=h.at(0, dx))

    def along_y(self, dy, i):
        h, part = self.here, self.part(i)
        return send(self.acc.at[h.at(dy, 0), part], self.y_in.at[dy - 1, part], self.y_s.at[dy - 1], self.y_r.at[i, dy - 1],
                    term=h.at(dy, 0))

    def sectors_out(self, slabs, i):
        h = self.here
        for dy, dx in slabs:
            r = h.at(dy, dx)

            @pl.when(h.s + 1 < h.sectors)
            def _():
                self.upward(r, i).start()

            @pl.when(h.s > 0)
            def _():
                self.downward(r, i).start()

    def merge(self, r, i):
        h, part = self.here, self.part(i)
        self.acc[r, part] = self.whole[1, r, part]

        @pl.when(h.s > 0)
        def _():
            self.upward(r, i).wait_recv()
            self.acc[r, part] += self.up_in[r, part]

        @pl.when(h.s + 1 < h.sectors)
        def _():
            self.downward(r, i).wait_recv()
            self.acc[r, part] += self.down_in[r, part]

        if self.tally:
            self.tally(r, part, self.acc[r, part])

    def corners(self, i):
        h = self.here
        for dy in range(1, h.gy):
            for dx in range(1, h.gx):
                self.merge(h.at(dy, dx), i)
                self.corner_a(dy, dx, i).start()
                self.corner_b(dy, dx, i).start()

    def sides(self, i):
        h, part = self.here, self.part(i)
        for dy in range(1, h.gy):
            r = h.at(dy, 0)
            self.merge(r, i)
            for dx in range(1, h.gx):
                self.corner_a(dy, dx, i).wait_recv()
                self.acc[r, part, : self.half] += self.da_in[h.corner(dy, dx), part]
            self.along_y(dy, i).start()
        for dx in range(1, h.gx):
            r = h.at(0, dx)
            self.merge(r, i)
            for dy in range(1, h.gy):
                self.corner_b(dy, dx, i).wait_recv()
                self.acc[r, part, self.half :] += self.db_in[h.corner(dy, dx), part]
            self.along_x(dx, i).start()

    def own(self, i):
        h, part = self.here, self.part(i)
        total = self.acc[h.t, part]
        for dy in range(1, h.gy):
            self.along_y(dy, i).wait_recv()
            total += self.y_in[dy - 1, part]
        for dx in range(1, h.gx):
            self.along_x(dx, i).wait_recv()
            total += self.x_in[dx - 1, part]
        return total

    def drain(self):
        h = self.here

        def sent(source, target, sem):
            send(source, target, sem, self.up_r.at[0, 0], term=h.at(0, 1), sector=h.s).wait_send()

        @pl.when(h.s + 1 < h.sectors)
        def _():
            sent(self.whole.at[2], self.up_in, self.z_s.at[1])

        @pl.when(h.s > 0)
        def _():
            sent(self.whole.at[0], self.down_in, self.z_s.at[0])

        for dy, dx in h.corners:
            c = h.corner(dy, dx)
            sent(self.da_in.at[c], self.da_in.at[c], self.da_s.at[c])
            sent(self.db_in.at[c], self.db_in.at[c], self.db_s.at[c])
        for n in range(h.gx - 1):
            sent(self.x_in.at[n], self.x_in.at[n], self.x_s.at[n])
        for n in range(h.gy - 1):
            sent(self.y_in.at[n], self.y_in.at[n], self.y_s.at[n])


class Gather:
    def __init__(self, here, full, refs, pieces):
        self.here, self.full = here, full
        self.x_s, self.x_r, self.y_s, self.y_r, self.a_s, self.a_r, self.b_s, self.b_r, self.c_s, self.c_r = refs
        self.sub, self.half, self.pieces = full.shape[1] // SLICES, full.shape[2] // 2, pieces

    @staticmethod
    def scratch(terms, pieces):
        gy, gx = grid_of(terms)
        dma = pltpu.SemaphoreType.DMA
        corners = (gy - 1) * (gx - 1)
        return [dma((gx - 1,)), dma((pieces, gx - 1)), dma((gy - 1,)), dma((pieces, gy - 1))] + [
            dma((corners,)), dma((pieces, corners))] * 2 + [dma((corners,)), dma((corners,))]

    def part(self, i):
        return pl.ds(pl.multiple_of(i * self.sub, self.sub), self.sub)

    def to_x(self, r, dx, i):
        ref = self.full.at[r, self.part(i)]
        return send(ref, ref, self.x_s.at[dx - 1], self.x_r.at[i, dx - 1], term=self.here.at(0, dx))

    def to_y(self, r, dy, i):
        ref = self.full.at[r, self.part(i)]
        return send(ref, ref, self.y_s.at[dy - 1], self.y_r.at[i, dy - 1], term=self.here.at(dy, 0))

    def relay_a(self, r, dy, dx, i):
        ref, c = self.full.at[r, self.part(i), : self.half], self.here.corner(dy, dx)
        return send(ref, ref, self.a_s.at[c], self.a_r.at[i, c], term=self.here.at(0, dx))

    def relay_b(self, r, dy, dx, i):
        ref, c = self.full.at[r, self.part(i), self.half :], self.here.corner(dy, dx)
        return send(ref, ref, self.b_s.at[c], self.b_r.at[i, c], term=self.here.at(dy, 0))

    def to_corner(self, r, dy, dx, i):
        ref, c = self.full.at[r, self.part(i)], self.here.corner(dy, dx)
        return send(ref, ref, self.c_s.at[c], self.c_r.at[c], term=self.here.at(dy, dx))

    def begin_direct(self, i):
        for dy, dx in self.here.corners:
            self.to_corner(self.here.t, dy, dx, i).start()
        self.begin(i)

    def finish_direct(self, i):
        h = self.here
        for dx in range(1, h.gx):
            self.to_x(h.at(0, dx), h.gx - dx, i).wait_recv()
        for dy in range(1, h.gy):
            self.to_y(h.at(dy, 0), h.gy - dy, i).wait_recv()
        for dy, dx in h.corners:
            self.to_corner(h.at(h.gy - dy, h.gx - dx), dy, dx, i).wait_recv()

    def drain_direct(self, i):
        for dy, dx in self.here.corners:
            self.to_corner(self.here.t, dy, dx, i).wait_send()

    def begin(self, i):
        h = self.here
        for dx in range(1, h.gx):
            self.to_x(h.t, dx, i).start()
        for dy in range(1, h.gy):
            self.to_y(h.t, dy, i).start()

    def relay(self, i):
        h = self.here
        for dx in range(1, h.gx):
            r = h.at(0, dx)
            self.to_x(r, h.gx - dx, i).wait_recv()
            for dy in range(1, h.gy):
                self.relay_b(r, dy, dx, i).start()
        for dy in range(1, h.gy):
            r = h.at(dy, 0)
            self.to_y(r, h.gy - dy, i).wait_recv()
            for dx in range(1, h.gx):
                self.relay_a(r, dy, dx, i).start()

    def finish(self, i):
        h = self.here
        for dy in range(1, h.gy):
            for dx in range(1, h.gx):
                self.relay_a(h.at(dy, h.gx - dx), dy, dx, i).wait_recv()
                self.relay_b(h.at(h.gy - dy, dx), dy, dx, i).wait_recv()

    def drain(self):
        h, all_rows = self.here, pl.ds(0, self.pieces * self.sub)
        relayed = pl.ds(0, EARLY * self.sub)

        def sent(ref, sem):
            send(ref, ref, sem, self.x_r.at[0, 0], term=h.at(0, 1)).wait_send()

        for n in range(h.gx - 1):
            sent(self.full.at[h.t, all_rows], self.x_s.at[n])
        for n in range(h.gy - 1):
            sent(self.full.at[h.t, all_rows], self.y_s.at[n])
        for dy, dx in h.corners:
            sent(self.full.at[h.at(dy, 0), relayed, : self.half], self.a_s.at[h.corner(dy, dx)])
            sent(self.full.at[h.at(0, dx), relayed, self.half :], self.b_s.at[h.corner(dy, dx)])


BUFFERS, SEMAPHORES, GATHER_REFS, TOTAL_REFS = 8, 11, 10, 5


def kernel(target_hbm, count_hbm, wave_hbm, precond_hbm, left_hbm, right_hbm, first_out, correction_out, second_out, *scratch):
    scratch = list(scratch)

    def take(n):
        refs = scratch[:n]
        del scratch[:n]
        return refs

    here = Place()
    buffers, more, sems = take(BUFFERS), take(BUFFERS), take(SEMAPHORES)

    def fold(x):
        x = jnp.sum(x.reshape(x.shape[0] // 8, 8, width), axis=0)
        return sum(x[:, c : c + 128] for c in range(0, width, 128))

    def tally(r, part, value):
        overlap.sums[0] += fold(wave[r, part] * value)

    first, second = Exchange(here, buffers, sems, tally), Exchange(here, more, sems)
    wave, precond, image, left, right, r_high, r_low, v_high, v_low, in_high, in_low, target, count = take(13)
    p_gather, f_gather = Gather(here, precond, take(GATHER_REFS), EARLY), Gather(here, image, take(GATHER_REFS), SLICES)
    overlap, share_total, (load,) = Total(here, take(TOTAL_REFS)), Total(here, take(TOTAL_REFS)), take(1)
    t, s, terms = here.t, here.s, here.terms
    slots, _, rows, width = left.shape
    sub = rows // SLICES

    load_precond = pltpu.make_async_copy(precond_hbm, precond.at[t], load.at[0])
    load_wave = pltpu.make_async_copy(wave_hbm, wave, load.at[1])
    load_target = pltpu.make_async_copy(target_hbm, target, load.at[2])
    load_count = pltpu.make_async_copy(count_hbm, count, load.at[3])
    load_right = [pltpu.make_async_copy(right_hbm.at[j], right.at[j], load.at[4 + j]) for j in range(slots)]
    def load_rows(o, part, n):
        piece = (slice(None), here.at(*o), part)
        return pltpu.make_async_copy(left_hbm.at[piece], left.at[piece], load.at[4 + slots + n])

    upper, lower = pl.ds(0, rows // 2), pl.ds(rows // 2, rows // 2)
    load_soon = [load_rows(o, upper, n) for n, o in enumerate(here.corners)]
    load_later = [load_rows(o, lower, terms + n) for n, o in enumerate(here.corners)] + [
        load_rows(o, pl.ds(0, rows), len(here.corners) + n) for n, o in enumerate(here.sides + here.own)]
    corners = len(here.corners)
    for copy in [load_wave] + load_soon + [load_target, load_count] + load_right + [load_precond] + load_later:
        copy.start()
    arrived = barrier(here)

    def split_rows(value, start, size):
        for r in range(terms):
            to = pl.ds(r * rows + start, size)
            v_high[to], v_low[to] = split(value(r, pl.ds(start, size)))

    def inner(slabs, part):
        stack = jnp.concatenate([left[j, here.at(*o), part] for j in range(slots) for o in slabs], axis=0)
        return split(product(*split(stack), v_high[...], v_low[...]))

    def chosen(j, p, tile):
        hit = jnp.logical_and(j < count[0, 0], target[0, j] - s + 1 == p)
        return jnp.where(hit, tile, 0.0)

    def outer(m):
        return stacked if m < 128 else product

    def compute(exchange, slabs, part, size):
        high, low = inner(slabs, part)
        m = len(slabs) * size
        tiles = [outer(m)(high[j * m : (j + 1) * m], low[j * m : (j + 1) * m], r_high[j], r_low[j]) for j in range(slots)]
        for n, o in enumerate(slabs):
            for p in range(3):
                exchange.whole[p, here.at(*o), part] = sum(
                    chosen(j, p, tiles[j][n * size : (n + 1) * size]) for j in range(slots))

    every = pl.ds(0, rows)

    def corners_first(exchange):
        part = pl.ds(0, rows // 2)
        m = corners * (rows // 2)
        with jax.named_scope("startv"):
            load_wave.wait()
            split_rows(lambda r, part: wave[r, part], 0, rows)
        with jax.named_scope("startl"):
            for copy in load_soon:
                copy.wait()
            in_high[...], in_low[...] = inner(here.corners, part)
        load_target.wait()
        load_count.wait()
        pairs = [range(j, min(j + 2, slots)) for j in range(0, slots, 2)]
        for pair in pairs:
            with jax.named_scope("startr"):
                for j in pair:
                    load_right[j].wait()
                tiles = {}
                for j in pair:
                    high, low = split(right[j])
                    r_high[j], r_low[j] = high, low
                    tiles[j] = outer(m)(in_high[j * m : (j + 1) * m], in_low[j * m : (j + 1) * m], high, low)
                for n, o in enumerate(here.corners):
                    for p in range(3):
                        rows_of = slice(n * (rows // 2), (n + 1) * (rows // 2))
                        piece = sum(chosen(j, p, tiles[j][rows_of]) for j in pair)
                        ref = exchange.whole.at[p, here.at(*o), part]
                        ref[...] = piece if pair == pairs[0] else ref[...] + piece

    def apply(exchange, begin, meanwhile):
        def half(h):
            return pl.ds(pl.multiple_of(h * (rows // 2), rows // 2), rows // 2)

        def half_out(slabs, h):
            for i in range(SLICES // 2):
                exchange.sectors_out(slabs, h * (SLICES // 2) + i)

        def corner_block(h):
            with jax.named_scope("CD"):
                compute(exchange, here.corners, half(h), rows // 2)
            half_out(here.corners, h)

        if begin:
            begin()
            half_out(here.corners, 0)
            for i in range(EARLY):
                p_gather.begin(i)
            for copy in load_later:
                copy.wait()
            corner_block(1)
        else:
            pl.loop(0, 2)(corner_block)

        if begin:
            @pl.loop(0, SLICES)
            def _(b):
                with jax.named_scope("C"):
                    compute(exchange, here.sides, exchange.part(b), sub)
                exchange.sectors_out(here.sides, b)
                with jax.named_scope("p"):
                    meanwhile(b)

                with jax.named_scope("Fd"):
                    @pl.when(b < SLICES - 1)
                    def _():
                        exchange.corners(b + b // 2)

                    @pl.when(b == 1)
                    def _():
                        exchange.corners(2)
        else:
            with jax.named_scope("C"):
                compute(exchange, here.sides, half(0), rows // 2)
            half_out(here.sides, 0)
            with jax.named_scope("Fd"):
                for i in range(SLICES // 2):
                    exchange.corners(i)

            @pl.loop(SLICES // 2, SLICES)
            def _(i):
                with jax.named_scope("C"):
                    compute(exchange, here.sides, exchange.part(i), sub)
                exchange.sectors_out(here.sides, i)

                @pl.when(i == SLICES // 2)
                def _():
                    with jax.named_scope("Fd"):
                        for k in range(SLICES // 2, SLICES):
                            exchange.corners(k)

        @pl.loop(0, 2)
        def _(h):
            with jax.named_scope("Fxy"):
                exchange.sides(h)
            with jax.named_scope("CO"):
                compute(exchange, here.own, half(h), rows // 2)
            half_out(here.own, h)

        @pl.loop(2, SLICES)
        def _(i):
            with jax.named_scope("Fxy"):
                exchange.sides(i)

    def first_begin():
        corners_first(first)
        with jax.named_scope("enter"):
            load_precond.wait()
            arrived()

    def first_done(i):
        part = first.part(i)
        f = first.own(i)
        first_out[part] = f
        image[t, part] = f

    overlap.sums[0] = jnp.zeros((8, 128), F32)
    def relays(b):
        @pl.when(jnp.logical_and(b >= 1, b <= EARLY))
        def _():
            p_gather.relay(b - 1)

    apply(first, first_begin, relays)

    with jax.named_scope("Fo"):
        for i in range(2):
            first.merge(t, i)
        first_done(0)
        f_gather.begin(0)
    with jax.named_scope("Mo"):
        for i in range(2, SLICES):
            first.merge(t, i)
        overlap.sums[1] = fold(wave[t] * wave[t])
        overlap.begin()
    with jax.named_scope("Fo"):
        for i in range(1, SLICES):
            first_done(i)
            if i < EARLY:
                f_gather.begin(i)
    with jax.named_scope("relay0"):
        for i in range(EARLY):
            p_gather.finish(i)
        f_gather.relay(0)
    with jax.named_scope("ray"):
        cross, norm = overlap.finish()
        rayleigh = cross / norm

    def raw(r, part):
        return precond[r, part] * (image[r, part] - rayleigh * wave[r, part])

    with jax.named_scope("raw"):
        for i in range(EARLY, SLICES):
            image[t, first.part(i)] = raw(t, first.part(i))
        share_total.sums[0] = jnp.zeros((8, 128), F32)
        for i in range(SLICES):
            part = first.part(i)
            own = raw(t, part) if i < EARLY else image[t, part]
            correction_out[part] = own
            share_total.sums[0] += fold(wave[t, part] * own)
        share_total.begin()
        for i in range(EARLY, SLICES):
            f_gather.begin_direct(i)
    with jax.named_scope("relay"):
        for i in range(1, EARLY):
            f_gather.relay(i)
    with jax.named_scope("share"):
        (dot,) = share_total.finish()
        share = dot / norm
    correction_out[...] -= share * wave[t]

    def corrected(r, part):
        return raw(r, part) - share * wave[r, part]

    for i in range(SLICES):
        with jax.named_scope("gfin"):
            if i < EARLY:
                f_gather.finish(i)
            else:
                f_gather.finish_direct(i)
        with jax.named_scope("corr"):
            split_rows(corrected if i < EARLY else lambda r, part: image[r, part] - share * wave[r, part], i * sub, sub)

    first.drain()
    apply(second, None, lambda i: None)

    @pl.loop(0, SLICES)
    def _(i):
        with jax.named_scope("Fo"):
            second.merge(t, i)
            second_out[second.part(i)] = second.own(i)

    with jax.named_scope("drain"):
        for stream in (second, p_gather, f_gather, overlap, share_total):
            stream.drain()
        f_gather.drain_direct(EARLY)


def publish_kernel(*refs):
    ins, outs, sems = refs[:3], refs[3:6], refs[6]
    copies = [pltpu.make_async_copy(a, b, sems.at[n]) for n, (a, b) in enumerate(zip(ins, outs))]
    for copy in copies:
        copy.start()
    for copy in copies:
        copy.wait()


def per_device(wavefunction, precond, left_ops, right_ops, out_sector, live_counts):
    terms, sectors = lax.axis_size("term"), lax.axis_size("sector")
    width, slots = wavefunction.shape[1], left_ops.shape[1]
    rows = width // terms
    gy, gx = grid_of(terms)
    dma = pltpu.SemaphoreType.DMA
    slab = jax.ShapeDtypeStruct((rows, width), F32)
    block = pltpu.VMEM((terms, rows, width), F32)
    half = pltpu.VMEM((width, width), BF16)
    operators = pltpu.VMEM((slots, terms, rows, width), F32)
    halves = pltpu.VMEM((slots, width, width), BF16)
    inner = pltpu.VMEM((slots * (gy - 1) * (gx - 1) * (rows // 2), width), BF16)
    peers = terms * sectors - 1
    outs = pl.pallas_call(
        kernel,
        out_shape=(pltpu.VMEM((rows, width), F32),) * 3,
        in_specs=[HBM] * 6,
        out_specs=(VMEM,) * 3,
        scratch_shapes=Exchange.buffers(width, terms) * 2 + Exchange.semaphores(terms)
        + [block, block, block, operators, pltpu.VMEM((slots, width, width), F32), halves, halves, half, half, inner, inner,
           pltpu.SMEM(out_sector.shape, jnp.int32), pltpu.SMEM(live_counts.shape, jnp.int32)]
        + Gather.scratch(terms, EARLY) + Gather.scratch(terms, SLICES)
        + Total.scratch(2, peers) + Total.scratch(1, peers) + [dma((4 + slots + terms + (gy - 1) * (gx - 1),))],
        compiler_params=pltpu.CompilerParams(collective_id=0, has_side_effects=True, vmem_limit_bytes=VMEM_BYTES - 3 * 4 * rows * width - (192 << 10)),
    )(out_sector, live_counts, wavefunction.reshape(terms, rows, width), precond[0],
      left_ops.reshape(slots, terms, rows, width), right_ops[0])
    outs = pl.pallas_call(
        publish_kernel,
        out_shape=(slab,) * 3,
        in_specs=[VMEM] * 3,
        out_specs=(HBM,) * 3,
        scratch_shapes=[dma((3,))],
        compiler_params=pltpu.CompilerParams(vmem_limit_bytes=1 << 20),
    )(*outs)
    return tuple(x[None] for x in outs)


def solution(mesh):
    placed = (
        P("sector", None, None),
        P("sector", "term", None),
        P("sector", "term", None, None),
        P("sector", "term", None, None),
        P("sector", "term"),
        P("sector", "term"),
    )
    return jax.shard_map(
        per_device,
        mesh=mesh,
        in_specs=placed,
        out_specs=(P("sector", "term", None), P("sector", "term", None), P("sector", "term", None)),
        check_vma=False,
    )
```

```python
import functools
import math

import jax
import jax.numpy as jnp
from jax import lax
from jax.experimental import pallas as pl
from jax.experimental.pallas import tpu as pltpu
from jax.sharding import PartitionSpec as P

F32, BF16 = jnp.float32, jnp.bfloat16
MESH = pl.DeviceIdType.MESH
VMEM = pl.BlockSpec(memory_space=pltpu.VMEM)
HBM = pl.BlockSpec(memory_space=pltpu.HBM)
SLICES = 4
EARLY = SLICES - 1
VMEM_BYTES = 67043328


def split(x):
    high = x.astype(BF16)
    return high, (x - high.astype(F32)).astype(BF16)


def product(a_high, a_low, b_high, b_low):
    dot = functools.partial(jnp.dot, preferred_element_type=F32)
    return dot(a_high, b_high) + dot(a_high, b_low) + dot(a_low, b_high)


def stacked(a_high, a_low, b_high, b_low):
    dot = functools.partial(jnp.dot, preferred_element_type=F32)
    m = a_high.shape[0]
    both = dot(jnp.concatenate([a_high, a_low], axis=0), b_high)
    return both[:m] + both[m:] + dot(a_high, b_low)


def send(source, target, send_sem, recv_sem, **where):
    return pltpu.make_async_remote_copy(
        src_ref=source, dst_ref=target, send_sem=send_sem, recv_sem=recv_sem,
        device_id=where, device_id_type=MESH,
    )


def grid_of(terms):
    columns = max(d for d in range(1, math.isqrt(terms) + 1) if terms % d == 0)
    return terms // columns, columns


class Place:
    def __init__(self):
        self.terms, self.sectors = lax.axis_size("term"), lax.axis_size("sector")
        self.t, self.s = lax.axis_index("term"), lax.axis_index("sector")
        self.gy, self.gx = grid_of(self.terms)
        self.y, self.x = self.t // self.gx, lax.rem(self.t, self.gx)
        self.corners = [(dy, dx) for dy in range(1, self.gy) for dx in range(1, self.gx)]
        self.sides = [(dy, 0) for dy in range(1, self.gy)] + [(0, dx) for dx in range(1, self.gx)]
        self.own = [(0, 0)]

    def at(self, dy, dx):
        return lax.rem(self.y + dy, self.gy) * self.gx + lax.rem(self.x + dx, self.gx)

    def corner(self, dy, dx):
        return (dy - 1) * (self.gx - 1) + dx - 1

    def peers(self):
        terms = [lax.rem(self.t + k, self.terms) for k in range(self.terms)]
        sectors = [lax.rem(self.s + k, self.sectors) for k in range(self.sectors)]
        pairs = [{"term": t, "sector": s} for t in terms for s in sectors]
        return list(enumerate(pairs[1:]))


def barrier(here):
    sem = pltpu.get_barrier_semaphore()
    peers = here.peers()
    for _, where in peers:
        pl.semaphore_signal(sem, inc=1, device_id=where, device_id_type=MESH)
    return lambda: pl.semaphore_wait(sem, len(peers))


class Total:
    def __init__(self, here, refs):
        self.here = here
        self.sums, self.mine, self.theirs, self.send_sem, self.recv_sem = refs

    @staticmethod
    def scratch(values, peers):
        dma = pltpu.SemaphoreType.DMA
        return [pltpu.VMEM((values, 8, 128), F32), pltpu.VMEM((1, 128), F32), pltpu.VMEM((peers, 1, 128), F32),
                dma((1,)), dma((1,))]

    def all(self):
        return send(self.theirs, self.theirs, self.send_sem.at[0], self.recv_sem.at[0], **self.here.peers()[0][1])

    def begin(self):
        shape = (self.sums.shape[0], 128)
        diagonal = lax.broadcasted_iota(jnp.int32, shape, 0) == lax.broadcasted_iota(jnp.int32, shape, 1)
        line = jnp.sum(jnp.sum(self.sums[...], axis=1), axis=1, keepdims=True)
        self.mine[...] = jnp.sum(jnp.where(diagonal, line, 0.0), axis=0, keepdims=True)
        for k, where in self.here.peers():
            send(self.mine, self.theirs.at[k], self.send_sem.at[0], self.recv_sem.at[0], **where).start()

    def finish(self):
        self.all().wait_recv()
        total = self.mine[...] + jnp.sum(self.theirs[...], axis=0)
        return [total[:, n : n + 1] for n in range(self.sums.shape[0])]

    def drain(self):
        self.all().wait_send()


class Exchange:
    def __init__(self, here, refs, sems, tally=None):
        self.here, self.tally = here, tally
        self.whole, self.up_in, self.down_in, self.acc, self.da_in, self.db_in, self.x_in, self.y_in = refs
        (self.z_s, self.up_r, self.down_r, self.da_s, self.da_r, self.db_s, self.db_r,
         self.x_s, self.x_r, self.y_s, self.y_r) = sems
        self.rows, self.width = self.acc.shape[1], self.acc.shape[2]
        self.sub, self.half = self.rows // SLICES, self.width // 2

    @staticmethod
    def buffers(width, terms):
        rows, half = width // terms, width // 2
        gy, gx = grid_of(terms)
        whole = pltpu.VMEM((terms, rows, width), F32)
        corner = pltpu.VMEM(((gy - 1) * (gx - 1), rows, half), F32)
        return [pltpu.VMEM((3, terms, rows, width), F32), whole, whole, whole, corner, corner,
                pltpu.VMEM((gx - 1, rows, width), F32), pltpu.VMEM((gy - 1, rows, width), F32)]

    @staticmethod
    def semaphores(terms):
        gy, gx = grid_of(terms)
        dma, corners = pltpu.SemaphoreType.DMA, (gy - 1) * (gx - 1)
        return [dma((2,)), dma((SLICES, terms)), dma((SLICES, terms))] + [dma((corners,)), dma((SLICES, corners))] * 2 + [
            dma((gx - 1,)), dma((SLICES, gx - 1)), dma((gy - 1,)), dma((SLICES, gy - 1))]

    def part(self, i):
        return pl.ds(pl.multiple_of(i * self.sub, self.sub), self.sub)

    def upward(self, r, i):
        h = self.here
        return send(self.whole.at[2, r, self.part(i)], self.up_in.at[r, self.part(i)], self.z_s.at[1],
                    self.up_r.at[i, r], sector=lax.rem(h.s + 1, h.sectors))

    def downward(self, r, i):
        h = self.here
        return send(self.whole.at[0, r, self.part(i)], self.down_in.at[r, self.part(i)], self.z_s.at[0],
                    self.down_r.at[i, r], sector=lax.rem(h.s + h.sectors - 1, h.sectors))

    def corner_a(self, dy, dx, i):
        h, part, c = self.here, self.part(i), self.here.corner(dy, dx)
        return send(self.acc.at[h.at(dy, dx), part, : self.half], self.da_in.at[c, part],
                    self.da_s.at[c], self.da_r.at[i, c], term=h.at(0, dx))

    def corner_b(self, dy, dx, i):
        h, part, c = self.here, self.part(i), self.here.corner(dy, dx)
        return send(self.acc.at[h.at(dy, dx), part, self.half :], self.db_in.at[c, part],
                    self.db_s.at[c], self.db_r.at[i, c], term=h.at(dy, 0))

    def along_x(self, dx, i):
        h, part = self.here, self.part(i)
        return send(self.acc.at[h.at(0, dx), part], self.x_in.at[dx - 1, part], self.x_s.at[dx - 1], self.x_r.at[i, dx - 1],
                    term=h.at(0, dx))

    def along_y(self, dy, i):
        h, part = self.here, self.part(i)
        return send(self.acc.at[h.at(dy, 0), part], self.y_in.at[dy - 1, part], self.y_s.at[dy - 1], self.y_r.at[i, dy - 1],
                    term=h.at(dy, 0))

    def sectors_out(self, slabs, i):
        h = self.here
        for dy, dx in slabs:
            r = h.at(dy, dx)

            @pl.when(h.s + 1 < h.sectors)
            def _():
                self.upward(r, i).start()

            @pl.when(h.s > 0)
            def _():
                self.downward(r, i).start()

    def merge(self, r, i):
        h, part = self.here, self.part(i)
        self.acc[r, part] = self.whole[1, r, part]

        @pl.when(h.s > 0)
        def _():
            self.upward(r, i).wait_recv()
            self.acc[r, part] += self.up_in[r, part]

        @pl.when(h.s + 1 < h.sectors)
        def _():
            self.downward(r, i).wait_recv()
            self.acc[r, part] += self.down_in[r, part]

        if self.tally:
            self.tally(r, part, self.acc[r, part])

    def corners(self, i):
        h = self.here
        for dy in range(1, h.gy):
            for dx in range(1, h.gx):
                self.merge(h.at(dy, dx), i)
                self.corner_a(dy, dx, i).start()
                self.corner_b(dy, dx, i).start()

    def sides(self, i):
        h, part = self.here, self.part(i)
        for dy in range(1, h.gy):
            r = h.at(dy, 0)
            self.merge(r, i)
            for dx in range(1, h.gx):
                self.corner_a(dy, dx, i).wait_recv()
                self.acc[r, part, : self.half] += self.da_in[h.corner(dy, dx), part]
            self.along_y(dy, i).start()
        for dx in range(1, h.gx):
            r = h.at(0, dx)
            self.merge(r, i)
            for dy in range(1, h.gy):
                self.corner_b(dy, dx, i).wait_recv()
                self.acc[r, part, self.half :] += self.db_in[h.corner(dy, dx), part]
            self.along_x(dx, i).start()

    def own(self, i):
        h, part = self.here, self.part(i)
        total = self.acc[h.t, part]
        for dy in range(1, h.gy):
            self.along_y(dy, i).wait_recv()
            total += self.y_in[dy - 1, part]
        for dx in range(1, h.gx):
            self.along_x(dx, i).wait_recv()
            total += self.x_in[dx - 1, part]
        return total

    def drain(self):
        h = self.here

        def sent(source, target, sem):
            send(source, target, sem, self.up_r.at[0, 0], term=h.at(0, 1), sector=h.s).wait_send()

        @pl.when(h.s + 1 < h.sectors)
        def _():
            sent(self.whole.at[2], self.up_in, self.z_s.at[1])

        @pl.when(h.s > 0)
        def _():
            sent(self.whole.at[0], self.down_in, self.z_s.at[0])

        for dy, dx in h.corners:
            c = h.corner(dy, dx)
            sent(self.da_in.at[c], self.da_in.at[c], self.da_s.at[c])
            sent(self.db_in.at[c], self.db_in.at[c], self.db_s.at[c])
        for n in range(h.gx - 1):
            sent(self.x_in.at[n], self.x_in.at[n], self.x_s.at[n])
        for n in range(h.gy - 1):
            sent(self.y_in.at[n], self.y_in.at[n], self.y_s.at[n])


class Gather:
    def __init__(self, here, full, refs, pieces):
        self.here, self.full = here, full
        self.x_s, self.x_r, self.y_s, self.y_r, self.a_s, self.a_r, self.b_s, self.b_r, self.c_s, self.c_r = refs
        self.sub, self.half, self.pieces = full.shape[1] // SLICES, full.shape[2] // 2, pieces

    @staticmethod
    def scratch(terms, pieces):
        gy, gx = grid_of(terms)
        dma = pltpu.SemaphoreType.DMA
        corners = (gy - 1) * (gx - 1)
        return [dma((gx - 1,)), dma((pieces, gx - 1)), dma((gy - 1,)), dma((pieces, gy - 1))] + [
            dma((corners,)), dma((pieces, corners))] * 2 + [dma((corners,)), dma((corners,))]

    def part(self, i):
        return pl.ds(pl.multiple_of(i * self.sub, self.sub), self.sub)

    def to_x(self, r, dx, i):
        ref = self.full.at[r, self.part(i)]
        return send(ref, ref, self.x_s.at[dx - 1], self.x_r.at[i, dx - 1], term=self.here.at(0, dx))

    def to_y(self, r, dy, i):
        ref = self.full.at[r, self.part(i)]
        return send(ref, ref, self.y_s.at[dy - 1], self.y_r.at[i, dy - 1], term=self.here.at(dy, 0))

    def relay_a(self, r, dy, dx, i):
        ref, c = self.full.at[r, self.part(i), : self.half], self.here.corner(dy, dx)
        return send(ref, ref, self.a_s.at[c], self.a_r.at[i, c], term=self.here.at(0, dx))

    def relay_b(self, r, dy, dx, i):
        ref, c = self.full.at[r, self.part(i), self.half :], self.here.corner(dy, dx)
        return send(ref, ref, self.b_s.at[c], self.b_r.at[i, c], term=self.here.at(dy, 0))

    def to_corner(self, r, dy, dx, i):
        ref, c = self.full.at[r, self.part(i)], self.here.corner(dy, dx)
        return send(ref, ref, self.c_s.at[c], self.c_r.at[c], term=self.here.at(dy, dx))

    def begin_direct(self, i):
        for dy, dx in self.here.corners:
            self.to_corner(self.here.t, dy, dx, i).start()
        self.begin(i)

    def finish_direct(self, i):
        h = self.here
        for dx in range(1, h.gx):
            self.to_x(h.at(0, dx), h.gx - dx, i).wait_recv()
        for dy in range(1, h.gy):
            self.to_y(h.at(dy, 0), h.gy - dy, i).wait_recv()
        for dy, dx in h.corners:
            self.to_corner(h.at(h.gy - dy, h.gx - dx), dy, dx, i).wait_recv()

    def drain_direct(self, i):
        for dy, dx in self.here.corners:
            self.to_corner(self.here.t, dy, dx, i).wait_send()

    def begin(self, i):
        h = self.here
        for dx in range(1, h.gx):
            self.to_x(h.t, dx, i).start()
        for dy in range(1, h.gy):
            self.to_y(h.t, dy, i).start()

    def relay(self, i):
        h = self.here
        for dx in range(1, h.gx):
            r = h.at(0, dx)
            self.to_x(r, h.gx - dx, i).wait_recv()
            for dy in range(1, h.gy):
                self.relay_b(r, dy, dx, i).start()
        for dy in range(1, h.gy):
            r = h.at(dy, 0)
            self.to_y(r, h.gy - dy, i).wait_recv()
            for dx in range(1, h.gx):
                self.relay_a(r, dy, dx, i).start()

    def finish(self, i):
        h = self.here
        for dy in range(1, h.gy):
            for dx in range(1, h.gx):
                self.relay_a(h.at(dy, h.gx - dx), dy, dx, i).wait_recv()
                self.relay_b(h.at(h.gy - dy, dx), dy, dx, i).wait_recv()

    def drain(self):
        h, all_rows = self.here, pl.ds(0, self.pieces * self.sub)
        relayed = pl.ds(0, EARLY * self.sub)

        def sent(ref, sem):
            send(ref, ref, sem, self.x_r.at[0, 0], term=h.at(0, 1)).wait_send()

        for n in range(h.gx - 1):
            sent(self.full.at[h.t, all_rows], self.x_s.at[n])
        for n in range(h.gy - 1):
            sent(self.full.at[h.t, all_rows], self.y_s.at[n])
        for dy, dx in h.corners:
            sent(self.full.at[h.at(dy, 0), relayed, : self.half], self.a_s.at[h.corner(dy, dx)])
            sent(self.full.at[h.at(0, dx), relayed, self.half :], self.b_s.at[h.corner(dy, dx)])


BUFFERS, SEMAPHORES, GATHER_REFS, TOTAL_REFS = 8, 11, 10, 5


def kernel(target_hbm, count_hbm, wave_hbm, precond_hbm, left_hbm, right_hbm, first_out, correction_out, second_out, *scratch):
    scratch = list(scratch)

    def take(n):
        refs = scratch[:n]
        del scratch[:n]
        return refs

    here = Place()
    buffers, more, sems = take(BUFFERS), take(BUFFERS), take(SEMAPHORES)

    def fold(x):
        x = jnp.sum(x.reshape(x.shape[0] // 8, 8, width), axis=0)
        return sum(x[:, c : c + 128] for c in range(0, width, 128))

    def tally(r, part, value):
        overlap.sums[0] += fold(wave[r, part] * value)

    first, second = Exchange(here, buffers, sems, tally), Exchange(here, more, sems)
    wave, precond, image, left, right, r_high, r_low, v_high, v_low, in_high, in_low, target, count = take(13)
    p_gather, f_gather = Gather(here, precond, take(GATHER_REFS), EARLY), Gather(here, image, take(GATHER_REFS), SLICES)
    overlap, share_total, (load,) = Total(here, take(TOTAL_REFS)), Total(here, take(TOTAL_REFS)), take(1)
    t, s, terms = here.t, here.s, here.terms
    slots, _, rows, width = left.shape
    sub = rows // SLICES

    load_precond = pltpu.make_async_copy(precond_hbm, precond.at[t], load.at[0])
    load_wave = pltpu.make_async_copy(wave_hbm, wave, load.at[1])
    load_target = pltpu.make_async_copy(target_hbm, target, load.at[2])
    load_count = pltpu.make_async_copy(count_hbm, count, load.at[3])
    load_right = [pltpu.make_async_copy(right_hbm.at[j], right.at[j], load.at[4 + j]) for j in range(slots)]
    def load_rows(o, part, n):
        piece = (slice(None), here.at(*o), part)
        return pltpu.make_async_copy(left_hbm.at[piece], left.at[piece], load.at[4 + slots + n])

    upper, lower = pl.ds(0, rows // 2), pl.ds(rows // 2, rows // 2)
    load_soon = [load_rows(o, upper, n) for n, o in enumerate(here.corners)]
    load_later = [load_rows(o, lower, terms + n) for n, o in enumerate(here.corners)] + [
        load_rows(o, pl.ds(0, rows), len(here.corners) + n) for n, o in enumerate(here.sides + here.own)]
    corners = len(here.corners)
    for copy in [load_wave] + load_soon + [load_target, load_count, load_precond] + load_right + load_later:
        copy.start()
    arrived = barrier(here)

    def split_rows(value, start, size):
        for r in range(terms):
            to = pl.ds(r * rows + start, size)
            v_high[to], v_low[to] = split(value(r, pl.ds(start, size)))

    def inner(slabs, part):
        stack = jnp.concatenate([left[j, here.at(*o), part] for j in range(slots) for o in slabs], axis=0)
        return split(product(*split(stack), v_high[...], v_low[...]))

    def chosen(j, p, tile):
        hit = jnp.logical_and(j < count[0, 0], target[0, j] - s + 1 == p)
        return jnp.where(hit, tile, 0.0)

    def outer(m):
        return stacked if m < 128 else product

    def compute(exchange, slabs, part, size):
        high, low = inner(slabs, part)
        m = len(slabs) * size
        tiles = [outer(m)(high[j * m : (j + 1) * m], low[j * m : (j + 1) * m], r_high[j], r_low[j]) for j in range(slots)]
        for n, o in enumerate(slabs):
            for p in range(3):
                exchange.whole[p, here.at(*o), part] = sum(
                    chosen(j, p, tiles[j][n * size : (n + 1) * size]) for j in range(slots))

    every = pl.ds(0, rows)

    def corners_first(exchange):
        part = pl.ds(0, rows // 2)
        m = corners * (rows // 2)
        with jax.named_scope("startv"):
            load_wave.wait()
            split_rows(lambda r, part: wave[r, part], 0, rows)
        with jax.named_scope("startl"):
            for copy in load_soon:
                copy.wait()
            in_high[...], in_low[...] = inner(here.corners, part)
        load_target.wait()
        load_count.wait()
        pairs = [range(j, min(j + 2, slots)) for j in range(0, slots, 2)]
        for pair in pairs:
            with jax.named_scope("startr"):
                for j in pair:
                    load_right[j].wait()
                tiles = {}
                for j in pair:
                    high, low = split(right[j])
                    r_high[j], r_low[j] = high, low
                    tiles[j] = outer(m)(in_high[j * m : (j + 1) * m], in_low[j * m : (j + 1) * m], high, low)
                for n, o in enumerate(here.corners):
                    for p in range(3):
                        rows_of = slice(n * (rows // 2), (n + 1) * (rows // 2))
                        piece = sum(chosen(j, p, tiles[j][rows_of]) for j in pair)
                        ref = exchange.whole.at[p, here.at(*o), part]
                        ref[...] = piece if pair == pairs[0] else ref[...] + piece
            if pair == pairs[0]:
                with jax.named_scope("enter"):
                    load_precond.wait()
                    arrived()
                    for i in range(EARLY):
                        p_gather.begin(i)

    def apply(exchange, begin, meanwhile):
        def half(h):
            return pl.ds(pl.multiple_of(h * (rows // 2), rows // 2), rows // 2)

        def half_out(slabs, h):
            for i in range(SLICES // 2):
                exchange.sectors_out(slabs, h * (SLICES // 2) + i)

        def corner_block(h):
            with jax.named_scope("CD"):
                compute(exchange, here.corners, half(h), rows // 2)
            half_out(here.corners, h)

        if begin:
            begin()
            half_out(here.corners, 0)
            for copy in load_later:
                copy.wait()
            corner_block(1)
        else:
            pl.loop(0, 2)(corner_block)

        if begin:
            @pl.loop(0, SLICES)
            def _(b):
                with jax.named_scope("C"):
                    compute(exchange, here.sides, exchange.part(b), sub)
                exchange.sectors_out(here.sides, b)
                with jax.named_scope("p"):
                    meanwhile(b)

                with jax.named_scope("Fd"):
                    @pl.when(b < SLICES - 1)
                    def _():
                        exchange.corners(b + b // 2)

                    @pl.when(b == 1)
                    def _():
                        exchange.corners(2)
        else:
            with jax.named_scope("C"):
                compute(exchange, here.sides, half(0), rows // 2)
            half_out(here.sides, 0)
            with jax.named_scope("Fd"):
                for i in range(SLICES // 2):
                    exchange.corners(i)

            @pl.loop(SLICES // 2, SLICES)
            def _(i):
                with jax.named_scope("C"):
                    compute(exchange, here.sides, exchange.part(i), sub)
                exchange.sectors_out(here.sides, i)

                @pl.when(i == SLICES // 2)
                def _():
                    with jax.named_scope("Fd"):
                        for k in range(SLICES // 2, SLICES):
                            exchange.corners(k)

        @pl.loop(0, 2)
        def _(h):
            with jax.named_scope("Fxy"):
                exchange.sides(h)
            with jax.named_scope("CO"):
                compute(exchange, here.own, half(h), rows // 2)
            half_out(here.own, h)

        @pl.loop(2, SLICES)
        def _(i):
            with jax.named_scope("Fxy"):
                exchange.sides(i)

    def first_begin():
        corners_first(first)

    def first_done(i):
        part = first.part(i)
        f = first.own(i)
        first_out[part] = f
        image[t, part] = f

    overlap.sums[0] = jnp.zeros((8, 128), F32)
    def relays(b):
        @pl.when(jnp.logical_and(b >= 1, b <= EARLY))
        def _():
            p_gather.relay(b - 1)

    apply(first, first_begin, relays)

    with jax.named_scope("Fo"):
        for i in range(2):
            first.merge(t, i)
        first_done(0)
        f_gather.begin(0)
    with jax.named_scope("Mo"):
        for i in range(2, SLICES):
            first.merge(t, i)
        overlap.sums[1] = fold(wave[t] * wave[t])
        overlap.begin()
    with jax.named_scope("Fo"):
        for i in range(1, SLICES):
            first_done(i)
            if i < EARLY:
                f_gather.begin(i)
    with jax.named_scope("relay0"):
        for i in range(EARLY):
            p_gather.finish(i)
        f_gather.relay(0)
    with jax.named_scope("ray"):
        cross, norm = overlap.finish()
        rayleigh = cross / norm

    def raw(r, part):
        return precond[r, part] * (image[r, part] - rayleigh * wave[r, part])

    with jax.named_scope("raw"):
        for i in range(EARLY, SLICES):
            image[t, first.part(i)] = raw(t, first.part(i))
        share_total.sums[0] = jnp.zeros((8, 128), F32)
        for i in range(SLICES):
            part = first.part(i)
            own = raw(t, part) if i < EARLY else image[t, part]
            correction_out[part] = own
            share_total.sums[0] += fold(wave[t, part] * own)
        share_total.begin()
        for i in range(EARLY, SLICES):
            f_gather.begin_direct(i)
    with jax.named_scope("relay"):
        for i in range(1, EARLY):
            f_gather.relay(i)
    with jax.named_scope("share"):
        (dot,) = share_total.finish()
        share = dot / norm
    correction_out[...] -= share * wave[t]

    def corrected(r, part):
        return raw(r, part) - share * wave[r, part]

    for i in range(SLICES):
        with jax.named_scope("gfin"):
            if i < EARLY:
                f_gather.finish(i)
            else:
                f_gather.finish_direct(i)
        with jax.named_scope("corr"):
            split_rows(corrected if i < EARLY else lambda r, part: image[r, part] - share * wave[r, part], i * sub, sub)

    first.drain()
    apply(second, None, lambda i: None)

    @pl.loop(0, SLICES)
    def _(i):
        with jax.named_scope("Fo"):
            second.merge(t, i)
            second_out[second.part(i)] = second.own(i)

    with jax.named_scope("drain"):
        for stream in (second, p_gather, f_gather, overlap, share_total):
            stream.drain()
        f_gather.drain_direct(EARLY)


def publish_kernel(*refs):
    ins, outs, sems = refs[:3], refs[3:6], refs[6]
    copies = [pltpu.make_async_copy(a, b, sems.at[n]) for n, (a, b) in enumerate(zip(ins, outs))]
    for copy in copies:
        copy.start()
    for copy in copies:
        copy.wait()


def per_device(wavefunction, precond, left_ops, right_ops, out_sector, live_counts):
    terms, sectors = lax.axis_size("term"), lax.axis_size("sector")
    width, slots = wavefunction.shape[1], left_ops.shape[1]
    rows = width // terms
    gy, gx = grid_of(terms)
    dma = pltpu.SemaphoreType.DMA
    slab = jax.ShapeDtypeStruct((rows, width), F32)
    block = pltpu.VMEM((terms, rows, width), F32)
    half = pltpu.VMEM((width, width), BF16)
    operators = pltpu.VMEM((slots, terms, rows, width), F32)
    halves = pltpu.VMEM((slots, width, width), BF16)
    inner = pltpu.VMEM((slots * (gy - 1) * (gx - 1) * (rows // 2), width), BF16)
    peers = terms * sectors - 1
    outs = pl.pallas_call(
        kernel,
        out_shape=(pltpu.VMEM((rows, width), F32),) * 3,
        in_specs=[HBM] * 6,
        out_specs=(VMEM,) * 3,
        scratch_shapes=Exchange.buffers(width, terms) * 2 + Exchange.semaphores(terms)
        + [block, block, block, operators, pltpu.VMEM((slots, width, width), F32), halves, halves, half, half, inner, inner,
           pltpu.SMEM(out_sector.shape, jnp.int32), pltpu.SMEM(live_counts.shape, jnp.int32)]
        + Gather.scratch(terms, EARLY) + Gather.scratch(terms, SLICES)
        + Total.scratch(2, peers) + Total.scratch(1, peers) + [dma((4 + slots + terms + (gy - 1) * (gx - 1),))],
        compiler_params=pltpu.CompilerParams(collective_id=0, has_side_effects=True, vmem_limit_bytes=VMEM_BYTES - 3 * 4 * rows * width - (192 << 10)),
    )(out_sector, live_counts, wavefunction.reshape(terms, rows, width), precond[0],
      left_ops.reshape(slots, terms, rows, width), right_ops[0])
    outs = pl.pallas_call(
        publish_kernel,
        out_shape=(slab,) * 3,
        in_specs=[VMEM] * 3,
        out_specs=(HBM,) * 3,
        scratch_shapes=[dma((3,))],
        compiler_params=pltpu.CompilerParams(vmem_limit_bytes=1 << 20),
    )(*outs)
    return tuple(x[None] for x in outs)


def solution(mesh):
    placed = (
        P("sector", None, None),
        P("sector", "term", None),
        P("sector", "term", None, None),
        P("sector", "term", None, None),
        P("sector", "term"),
        P("sector", "term"),
    )
    return jax.shard_map(
        per_device,
        mesh=mesh,
        in_specs=placed,
        out_specs=(P("sector", "term", None), P("sector", "term", None), P("sector", "term", None)),
        check_vma=False,
    )
```

```python
import functools
import math

import jax
import jax.numpy as jnp
from jax import lax
from jax.experimental import pallas as pl
from jax.experimental.pallas import tpu as pltpu
from jax.sharding import PartitionSpec as P

F32, BF16 = jnp.float32, jnp.bfloat16
MESH = pl.DeviceIdType.MESH
VMEM = pl.BlockSpec(memory_space=pltpu.VMEM)
HBM = pl.BlockSpec(memory_space=pltpu.HBM)
SLICES = 4
EARLY = SLICES - 1
VMEM_BYTES = 67043328


def split(x):
    high = x.astype(BF16)
    return high, (x - high.astype(F32)).astype(BF16)


def product(a_high, a_low, b_high, b_low):
    dot = functools.partial(jnp.dot, preferred_element_type=F32)
    return dot(a_high, b_high) + dot(a_high, b_low) + dot(a_low, b_high)


def stacked(a_high, a_low, b_high, b_low):
    dot = functools.partial(jnp.dot, preferred_element_type=F32)
    m = a_high.shape[0]
    both = dot(jnp.concatenate([a_high, a_low], axis=0), b_high)
    return both[:m] + both[m:] + dot(a_high, b_low)


def send(source, target, send_sem, recv_sem, **where):
    return pltpu.make_async_remote_copy(
        src_ref=source, dst_ref=target, send_sem=send_sem, recv_sem=recv_sem,
        device_id=where, device_id_type=MESH,
    )


def grid_of(terms):
    columns = max(d for d in range(1, math.isqrt(terms) + 1) if terms % d == 0)
    return terms // columns, columns


class Place:
    def __init__(self):
        self.terms, self.sectors = lax.axis_size("term"), lax.axis_size("sector")
        self.t, self.s = lax.axis_index("term"), lax.axis_index("sector")
        self.gy, self.gx = grid_of(self.terms)
        self.y, self.x = self.t // self.gx, lax.rem(self.t, self.gx)
        self.corners = [(dy, dx) for dy in range(1, self.gy) for dx in range(1, self.gx)]
        self.sides = [(dy, 0) for dy in range(1, self.gy)] + [(0, dx) for dx in range(1, self.gx)]
        self.own = [(0, 0)]

    def at(self, dy, dx):
        return lax.rem(self.y + dy, self.gy) * self.gx + lax.rem(self.x + dx, self.gx)

    def corner(self, dy, dx):
        return (dy - 1) * (self.gx - 1) + dx - 1

    def peers(self):
        terms = [lax.rem(self.t + k, self.terms) for k in range(self.terms)]
        sectors = [lax.rem(self.s + k, self.sectors) for k in range(self.sectors)]
        pairs = [{"term": t, "sector": s} for t in terms for s in sectors]
        return list(enumerate(pairs[1:]))


def barrier(here):
    sem = pltpu.get_barrier_semaphore()
    peers = here.peers()
    for _, where in peers:
        pl.semaphore_signal(sem, inc=1, device_id=where, device_id_type=MESH)
    return lambda: pl.semaphore_wait(sem, len(peers))


class Total:
    def __init__(self, here, refs):
        self.here = here
        self.sums, self.mine, self.theirs, self.send_sem, self.recv_sem = refs

    @staticmethod
    def scratch(values, peers):
        dma = pltpu.SemaphoreType.DMA
        return [pltpu.VMEM((values, 8, 128), F32), pltpu.VMEM((1, 128), F32), pltpu.VMEM((peers, 1, 128), F32),
                dma((1,)), dma((1,))]

    def all(self):
        return send(self.theirs, self.theirs, self.send_sem.at[0], self.recv_sem.at[0], **self.here.peers()[0][1])

    def begin(self):
        shape = (self.sums.shape[0], 128)
        diagonal = lax.broadcasted_iota(jnp.int32, shape, 0) == lax.broadcasted_iota(jnp.int32, shape, 1)
        line = jnp.sum(jnp.sum(self.sums[...], axis=1), axis=1, keepdims=True)
        self.mine[...] = jnp.sum(jnp.where(diagonal, line, 0.0), axis=0, keepdims=True)
        for k, where in self.here.peers():
            send(self.mine, self.theirs.at[k], self.send_sem.at[0], self.recv_sem.at[0], **where).start()

    def finish(self):
        self.all().wait_recv()
        total = self.mine[...] + jnp.sum(self.theirs[...], axis=0)
        return [total[:, n : n + 1] for n in range(self.sums.shape[0])]

    def drain(self):
        self.all().wait_send()


class Exchange:
    def __init__(self, here, refs, sems, tally=None):
        self.here, self.tally = here, tally
        self.whole, self.up_in, self.down_in, self.acc, self.da_in, self.db_in, self.x_in, self.y_in = refs
        (self.z_s, self.up_r, self.down_r, self.da_s, self.da_r, self.db_s, self.db_r,
         self.x_s, self.x_r, self.y_s, self.y_r) = sems
        self.rows, self.width = self.acc.shape[1], self.acc.shape[2]
        self.sub, self.half = self.rows // SLICES, self.width // 2

    @staticmethod
    def buffers(width, terms):
        rows, half = width // terms, width // 2
        gy, gx = grid_of(terms)
        whole = pltpu.VMEM((terms, rows, width), F32)
        corner = pltpu.VMEM(((gy - 1) * (gx - 1), rows, half), F32)
        return [pltpu.VMEM((3, terms, rows, width), F32), whole, whole, whole, corner, corner,
                pltpu.VMEM((gx - 1, rows, width), F32), pltpu.VMEM((gy - 1, rows, width), F32)]

    @staticmethod
    def semaphores(terms):
        gy, gx = grid_of(terms)
        dma, corners = pltpu.SemaphoreType.DMA, (gy - 1) * (gx - 1)
        return [dma((2,)), dma((SLICES, terms)), dma((SLICES, terms))] + [dma((corners,)), dma((SLICES, corners))] * 2 + [
            dma((gx - 1,)), dma((SLICES, gx - 1)), dma((gy - 1,)), dma((SLICES, gy - 1))]

    def part(self, i):
        return pl.ds(pl.multiple_of(i * self.sub, self.sub), self.sub)

    def upward(self, r, i):
        h = self.here
        return send(self.whole.at[2, r, self.part(i)], self.up_in.at[r, self.part(i)], self.z_s.at[1],
                    self.up_r.at[i, r], sector=lax.rem(h.s + 1, h.sectors))

    def downward(self, r, i):
        h = self.here
        return send(self.whole.at[0, r, self.part(i)], self.down_in.at[r, self.part(i)], self.z_s.at[0],
                    self.down_r.at[i, r], sector=lax.rem(h.s + h.sectors - 1, h.sectors))

    def corner_a(self, dy, dx, i):
        h, part, c = self.here, self.part(i), self.here.corner(dy, dx)
        return send(self.acc.at[h.at(dy, dx), part, : self.half], self.da_in.at[c, part],
                    self.da_s.at[c], self.da_r.at[i, c], term=h.at(0, dx))

    def corner_b(self, dy, dx, i):
        h, part, c = self.here, self.part(i), self.here.corner(dy, dx)
        return send(self.acc.at[h.at(dy, dx), part, self.half :], self.db_in.at[c, part],
                    self.db_s.at[c], self.db_r.at[i, c], term=h.at(dy, 0))

    def along_x(self, dx, i):
        h, part = self.here, self.part(i)
        return send(self.acc.at[h.at(0, dx), part], self.x_in.at[dx - 1, part], self.x_s.at[dx - 1], self.x_r.at[i, dx - 1],
                    term=h.at(0, dx))

    def along_y(self, dy, i):
        h, part = self.here, self.part(i)
        return send(self.acc.at[h.at(dy, 0), part], self.y_in.at[dy - 1, part], self.y_s.at[dy - 1], self.y_r.at[i, dy - 1],
                    term=h.at(dy, 0))

    def sectors_out(self, slabs, i):
        h = self.here
        for dy, dx in slabs:
            r = h.at(dy, dx)

            @pl.when(h.s + 1 < h.sectors)
            def _():
                self.upward(r, i).start()

            @pl.when(h.s > 0)
            def _():
                self.downward(r, i).start()

    def merge(self, r, i):
        h, part = self.here, self.part(i)
        self.acc[r, part] = self.whole[1, r, part]

        @pl.when(h.s > 0)
        def _():
            self.upward(r, i).wait_recv()
            self.acc[r, part] += self.up_in[r, part]

        @pl.when(h.s + 1 < h.sectors)
        def _():
            self.downward(r, i).wait_recv()
            self.acc[r, part] += self.down_in[r, part]

        if self.tally:
            self.tally(r, part, self.acc[r, part])

    def corners(self, i):
        h = self.here
        for dy in range(1, h.gy):
            for dx in range(1, h.gx):
                self.merge(h.at(dy, dx), i)
                self.corner_a(dy, dx, i).start()
                self.corner_b(dy, dx, i).start()

    def sides(self, i):
        h, part = self.here, self.part(i)
        for dy in range(1, h.gy):
            r = h.at(dy, 0)
            self.merge(r, i)
            for dx in range(1, h.gx):
                self.corner_a(dy, dx, i).wait_recv()
                self.acc[r, part, : self.half] += self.da_in[h.corner(dy, dx), part]
            self.along_y(dy, i).start()
        for dx in range(1, h.gx):
            r = h.at(0, dx)
            self.merge(r, i)
            for dy in range(1, h.gy):
                self.corner_b(dy, dx, i).wait_recv()
                self.acc[r, part, self.half :] += self.db_in[h.corner(dy, dx), part]
            self.along_x(dx, i).start()

    def own(self, i):
        h, part = self.here, self.part(i)
        total = self.acc[h.t, part]
        for dy in range(1, h.gy):
            self.along_y(dy, i).wait_recv()
            total += self.y_in[dy - 1, part]
        for dx in range(1, h.gx):
            self.along_x(dx, i).wait_recv()
            total += self.x_in[dx - 1, part]
        return total

    def drain(self):
        h = self.here

        def sent(source, target, sem):
            send(source, target, sem, self.up_r.at[0, 0], term=h.at(0, 1), sector=h.s).wait_send()

        @pl.when(h.s + 1 < h.sectors)
        def _():
            sent(self.whole.at[2], self.up_in, self.z_s.at[1])

        @pl.when(h.s > 0)
        def _():
            sent(self.whole.at[0], self.down_in, self.z_s.at[0])

        for dy, dx in h.corners:
            c = h.corner(dy, dx)
            sent(self.da_in.at[c], self.da_in.at[c], self.da_s.at[c])
            sent(self.db_in.at[c], self.db_in.at[c], self.db_s.at[c])
        for n in range(h.gx - 1):
            sent(self.x_in.at[n], self.x_in.at[n], self.x_s.at[n])
        for n in range(h.gy - 1):
            sent(self.y_in.at[n], self.y_in.at[n], self.y_s.at[n])


class Gather:
    def __init__(self, here, full, refs, pieces):
        self.here, self.full = here, full
        self.x_s, self.x_r, self.y_s, self.y_r, self.a_s, self.a_r, self.b_s, self.b_r, self.c_s, self.c_r = refs
        self.sub, self.half, self.pieces = full.shape[1] // SLICES, full.shape[2] // 2, pieces

    @staticmethod
    def scratch(terms, pieces):
        gy, gx = grid_of(terms)
        dma = pltpu.SemaphoreType.DMA
        corners = (gy - 1) * (gx - 1)
        return [dma((gx - 1,)), dma((pieces, gx - 1)), dma((gy - 1,)), dma((pieces, gy - 1))] + [
            dma((corners,)), dma((pieces, corners))] * 2 + [dma((corners,)), dma((corners,))]

    def part(self, i):
        return pl.ds(pl.multiple_of(i * self.sub, self.sub), self.sub)

    def to_x(self, r, dx, i):
        ref = self.full.at[r, self.part(i)]
        return send(ref, ref, self.x_s.at[dx - 1], self.x_r.at[i, dx - 1], term=self.here.at(0, dx))

    def to_y(self, r, dy, i):
        ref = self.full.at[r, self.part(i)]
        return send(ref, ref, self.y_s.at[dy - 1], self.y_r.at[i, dy - 1], term=self.here.at(dy, 0))

    def relay_a(self, r, dy, dx, i):
        ref, c = self.full.at[r, self.part(i), : self.half], self.here.corner(dy, dx)
        return send(ref, ref, self.a_s.at[c], self.a_r.at[i, c], term=self.here.at(0, dx))

    def relay_b(self, r, dy, dx, i):
        ref, c = self.full.at[r, self.part(i), self.half :], self.here.corner(dy, dx)
        return send(ref, ref, self.b_s.at[c], self.b_r.at[i, c], term=self.here.at(dy, 0))

    def to_corner(self, r, dy, dx, i):
        ref, c = self.full.at[r, self.part(i)], self.here.corner(dy, dx)
        return send(ref, ref, self.c_s.at[c], self.c_r.at[c], term=self.here.at(dy, dx))

    def begin_direct(self, i):
        for dy, dx in self.here.corners:
            self.to_corner(self.here.t, dy, dx, i).start()
        self.begin(i)

    def finish_direct(self, i):
        h = self.here
        for dx in range(1, h.gx):
            self.to_x(h.at(0, dx), h.gx - dx, i).wait_recv()
        for dy in range(1, h.gy):
            self.to_y(h.at(dy, 0), h.gy - dy, i).wait_recv()
        for dy, dx in h.corners:
            self.to_corner(h.at(h.gy - dy, h.gx - dx), dy, dx, i).wait_recv()

    def drain_direct(self, i):
        for dy, dx in self.here.corners:
            self.to_corner(self.here.t, dy, dx, i).wait_send()

    def begin(self, i):
        h = self.here
        for dx in range(1, h.gx):
            self.to_x(h.t, dx, i).start()
        for dy in range(1, h.gy):
            self.to_y(h.t, dy, i).start()

    def relay(self, i):
        h = self.here
        for dx in range(1, h.gx):
            r = h.at(0, dx)
            self.to_x(r, h.gx - dx, i).wait_recv()
            for dy in range(1, h.gy):
                self.relay_b(r, dy, dx, i).start()
        for dy in range(1, h.gy):
            r = h.at(dy, 0)
            self.to_y(r, h.gy - dy, i).wait_recv()
            for dx in range(1, h.gx):
                self.relay_a(r, dy, dx, i).start()

    def finish(self, i):
        h = self.here
        for dy in range(1, h.gy):
            for dx in range(1, h.gx):
                self.relay_a(h.at(dy, h.gx - dx), dy, dx, i).wait_recv()
                self.relay_b(h.at(h.gy - dy, dx), dy, dx, i).wait_recv()

    def drain(self):
        h, all_rows = self.here, pl.ds(0, self.pieces * self.sub)
        relayed = pl.ds(0, EARLY * self.sub)

        def sent(ref, sem):
            send(ref, ref, sem, self.x_r.at[0, 0], term=h.at(0, 1)).wait_send()

        for n in range(h.gx - 1):
            sent(self.full.at[h.t, all_rows], self.x_s.at[n])
        for n in range(h.gy - 1):
            sent(self.full.at[h.t, all_rows], self.y_s.at[n])
        for dy, dx in h.corners:
            sent(self.full.at[h.at(dy, 0), relayed, : self.half], self.a_s.at[h.corner(dy, dx)])
            sent(self.full.at[h.at(0, dx), relayed, self.half :], self.b_s.at[h.corner(dy, dx)])


BUFFERS, SEMAPHORES, GATHER_REFS, TOTAL_REFS = 8, 11, 10, 5


def kernel(target_hbm, count_hbm, wave_hbm, precond_hbm, left_hbm, right_hbm, first_out, correction_out, second_out, *scratch):
    scratch = list(scratch)

    def take(n):
        refs = scratch[:n]
        del scratch[:n]
        return refs

    here = Place()
    buffers, more, sems = take(BUFFERS), take(BUFFERS), take(SEMAPHORES)

    def fold(x):
        x = jnp.sum(x.reshape(x.shape[0] // 8, 8, width), axis=0)
        return sum(x[:, c : c + 128] for c in range(0, width, 128))

    def tally(r, part, value):
        overlap.sums[0] += fold(wave[r, part] * value)

    first, second = Exchange(here, buffers, sems, tally), Exchange(here, more, sems)
    wave, precond, image, left, right, r_high, r_low, v_high, v_low, in_high, in_low, target, count = take(13)
    p_gather, f_gather = Gather(here, precond, take(GATHER_REFS), EARLY), Gather(here, image, take(GATHER_REFS), SLICES)
    overlap, share_total, (load,) = Total(here, take(TOTAL_REFS)), Total(here, take(TOTAL_REFS)), take(1)
    t, s, terms = here.t, here.s, here.terms
    slots, _, rows, width = left.shape
    sub = rows // SLICES

    order = here.corners + here.sides + here.own
    load_precond = pltpu.make_async_copy(precond_hbm, precond.at[t], load.at[0])
    load_wave = pltpu.make_async_copy(wave_hbm, wave, load.at[1])
    load_target = pltpu.make_async_copy(target_hbm, target, load.at[2])
    load_count = pltpu.make_async_copy(count_hbm, count, load.at[3])
    load_right = [pltpu.make_async_copy(right_hbm.at[j], right.at[j], load.at[4 + j]) for j in range(slots)]
    load_left = [pltpu.make_async_copy(left_hbm.at[:, here.at(*o)], left.at[:, here.at(*o)], load.at[4 + slots + n])
                 for n, o in enumerate(order)]
    corners = len(here.corners)
    for copy in [load_precond, load_wave, load_target, load_count] + load_left[:corners] + load_right + load_left[corners:]:
        copy.start()
    arrived = barrier(here)

    def split_rows(value, start, size):
        for r in range(terms):
            to = pl.ds(r * rows + start, size)
            v_high[to], v_low[to] = split(value(r, pl.ds(start, size)))

    def inner(slabs, part):
        stack = jnp.concatenate([left[j, here.at(*o), part] for j in range(slots) for o in slabs], axis=0)
        return split(product(*split(stack), v_high[...], v_low[...]))

    def chosen(j, p, tile):
        hit = jnp.logical_and(j < count[0, 0], target[0, j] - s + 1 == p)
        return jnp.where(hit, tile, 0.0)

    def outer(m):
        return stacked if m < 128 else product

    def compute(exchange, slabs, part, size):
        high, low = inner(slabs, part)
        m = len(slabs) * size
        tiles = [outer(m)(high[j * m : (j + 1) * m], low[j * m : (j + 1) * m], r_high[j], r_low[j]) for j in range(slots)]
        for n, o in enumerate(slabs):
            for p in range(3):
                exchange.whole[p, here.at(*o), part] = sum(
                    chosen(j, p, tiles[j][n * size : (n + 1) * size]) for j in range(slots))

    every = pl.ds(0, rows)

    def corners_first(exchange):
        part = pl.ds(0, rows // 2)
        m = corners * (rows // 2)
        with jax.named_scope("startv"):
            load_wave.wait()
            split_rows(lambda r, part: wave[r, part], 0, rows)
        with jax.named_scope("startl"):
            for copy in load_left[:corners]:
                copy.wait()
            in_high[...], in_low[...] = inner(here.corners, part)
        load_target.wait()
        load_count.wait()
        pairs = [range(j, min(j + 2, slots)) for j in range(0, slots, 2)]
        for pair in pairs:
            with jax.named_scope("startr"):
                for j in pair:
                    load_right[j].wait()
                tiles = {}
                for j in pair:
                    high, low = split(right[j])
                    r_high[j], r_low[j] = high, low
                    tiles[j] = outer(m)(in_high[j * m : (j + 1) * m], in_low[j * m : (j + 1) * m], high, low)
                for n, o in enumerate(here.corners):
                    for p in range(3):
                        rows_of = slice(n * (rows // 2), (n + 1) * (rows // 2))
                        piece = sum(chosen(j, p, tiles[j][rows_of]) for j in pair)
                        ref = exchange.whole.at[p, here.at(*o), part]
                        ref[...] = piece if pair == pairs[0] else ref[...] + piece

    def apply(exchange, begin, meanwhile):
        def half(h):
            return pl.ds(pl.multiple_of(h * (rows // 2), rows // 2), rows // 2)

        def half_out(slabs, h):
            for i in range(SLICES // 2):
                exchange.sectors_out(slabs, h * (SLICES // 2) + i)

        def corner_block(h):
            with jax.named_scope("CD"):
                compute(exchange, here.corners, half(h), rows // 2)
            half_out(here.corners, h)

        if begin:
            begin()
            half_out(here.corners, 0)
            for i in range(EARLY):
                p_gather.begin(i)
            corner_block(1)
        else:
            pl.loop(0, 2)(corner_block)

        @pl.loop(0, 2)
        def _(h):
            with jax.named_scope("C"):
                compute(exchange, here.sides, half(h), rows // 2)
            half_out(here.sides, h)
            with jax.named_scope("Fd"):
                for i in range(SLICES // 2):
                    exchange.corners(h * (SLICES // 2) + i)
            with jax.named_scope("p"):
                meanwhile(h)

        @pl.loop(0, 2)
        def _(h):
            with jax.named_scope("Fxy"):
                exchange.sides(h)
            with jax.named_scope("CO"):
                compute(exchange, here.own, half(h), rows // 2)
            half_out(here.own, h)

        @pl.loop(2, SLICES)
        def _(i):
            with jax.named_scope("Fxy"):
                exchange.sides(i)

    def first_begin():
        corners_first(first)
        with jax.named_scope("enter"):
            load_precond.wait()
            arrived()
        for copy in load_left[corners:]:
            copy.wait()

    def first_done(i):
        part = first.part(i)
        f = first.own(i)
        first_out[part] = f
        image[t, part] = f

    overlap.sums[0] = jnp.zeros((8, 128), F32)
    def relays(h):
        for i in range(EARLY):
            @pl.when(h == (i + 1) // 2)
            def _():
                p_gather.relay(i)

    apply(first, first_begin, relays)

    with jax.named_scope("Fo"):
        for i in range(2):
            first.merge(t, i)
        first_done(0)
        f_gather.begin(0)
    with jax.named_scope("Mo"):
        for i in range(2, SLICES):
            first.merge(t, i)
        overlap.sums[1] = fold(wave[t] * wave[t])
        overlap.begin()
    with jax.named_scope("Fo"):
        for i in range(1, SLICES):
            first_done(i)
            if i < EARLY:
                f_gather.begin(i)
    with jax.named_scope("relay0"):
        for i in range(EARLY):
            p_gather.finish(i)
        f_gather.relay(0)
    with jax.named_scope("ray"):
        cross, norm = overlap.finish()
        rayleigh = cross / norm

    def raw(r, part):
        return precond[r, part] * (image[r, part] - rayleigh * wave[r, part])

    with jax.named_scope("raw"):
        for i in range(EARLY, SLICES):
            image[t, first.part(i)] = raw(t, first.part(i))
        share_total.sums[0] = jnp.zeros((8, 128), F32)
        for i in range(SLICES):
            part = first.part(i)
            own = raw(t, part) if i < EARLY else image[t, part]
            correction_out[part] = own
            share_total.sums[0] += fold(wave[t, part] * own)
        share_total.begin()
        for i in range(EARLY, SLICES):
            f_gather.begin_direct(i)
    with jax.named_scope("relay"):
        for i in range(1, EARLY):
            f_gather.relay(i)
    with jax.named_scope("share"):
        (dot,) = share_total.finish()
        share = dot / norm
    correction_out[...] -= share * wave[t]

    def corrected(r, part):
        return raw(r, part) - share * wave[r, part]

    for i in range(SLICES):
        with jax.named_scope("gfin"):
            if i < EARLY:
                f_gather.finish(i)
            else:
                f_gather.finish_direct(i)
        with jax.named_scope("corr"):
            split_rows(corrected if i < EARLY else lambda r, part: image[r, part] - share * wave[r, part], i * sub, sub)

    first.drain()
    apply(second, None, lambda i: None)

    @pl.loop(0, SLICES)
    def _(i):
        with jax.named_scope("Fo"):
            second.merge(t, i)
            second_out[second.part(i)] = second.own(i)

    with jax.named_scope("drain"):
        for stream in (second, p_gather, f_gather, overlap, share_total):
            stream.drain()
        f_gather.drain_direct(EARLY)


def publish_kernel(*refs):
    ins, outs, sems = refs[:3], refs[3:6], refs[6]
    copies = [pltpu.make_async_copy(a, b, sems.at[n]) for n, (a, b) in enumerate(zip(ins, outs))]
    for copy in copies:
        copy.start()
    for copy in copies:
        copy.wait()


def per_device(wavefunction, precond, left_ops, right_ops, out_sector, live_counts):
    terms, sectors = lax.axis_size("term"), lax.axis_size("sector")
    width, slots = wavefunction.shape[1], left_ops.shape[1]
    rows = width // terms
    gy, gx = grid_of(terms)
    dma = pltpu.SemaphoreType.DMA
    slab = jax.ShapeDtypeStruct((rows, width), F32)
    block = pltpu.VMEM((terms, rows, width), F32)
    half = pltpu.VMEM((width, width), BF16)
    operators = pltpu.VMEM((slots, terms, rows, width), F32)
    halves = pltpu.VMEM((slots, width, width), BF16)
    inner = pltpu.VMEM((slots * (gy - 1) * (gx - 1) * (rows // 2), width), BF16)
    peers = terms * sectors - 1
    outs = pl.pallas_call(
        kernel,
        out_shape=(pltpu.VMEM((rows, width), F32),) * 3,
        in_specs=[HBM] * 6,
        out_specs=(VMEM,) * 3,
        scratch_shapes=Exchange.buffers(width, terms) * 2 + Exchange.semaphores(terms)
        + [block, block, block, operators, pltpu.VMEM((slots, width, width), F32), halves, halves, half, half, inner, inner,
           pltpu.SMEM(out_sector.shape, jnp.int32), pltpu.SMEM(live_counts.shape, jnp.int32)]
        + Gather.scratch(terms, EARLY) + Gather.scratch(terms, SLICES)
        + Total.scratch(2, peers) + Total.scratch(1, peers) + [dma((4 + slots + terms,))],
        compiler_params=pltpu.CompilerParams(collective_id=0, has_side_effects=True, vmem_limit_bytes=VMEM_BYTES - 3 * 4 * rows * width - (192 << 10)),
    )(out_sector, live_counts, wavefunction.reshape(terms, rows, width), precond[0],
      left_ops.reshape(slots, terms, rows, width), right_ops[0])
    outs = pl.pallas_call(
        publish_kernel,
        out_shape=(slab,) * 3,
        in_specs=[VMEM] * 3,
        out_specs=(HBM,) * 3,
        scratch_shapes=[dma((3,))],
        compiler_params=pltpu.CompilerParams(vmem_limit_bytes=1 << 20),
    )(*outs)
    return tuple(x[None] for x in outs)


def solution(mesh):
    placed = (
        P("sector", None, None),
        P("sector", "term", None),
        P("sector", "term", None, None),
        P("sector", "term", None, None),
        P("sector", "term"),
        P("sector", "term"),
    )
    return jax.shard_map(
        per_device,
        mesh=mesh,
        in_specs=placed,
        out_specs=(P("sector", "term", None), P("sector", "term", None), P("sector", "term", None)),
        check_vma=False,
    )
```
